8 devices in a mesh: exam: 1 (over z), cols: 2 (over y), rows: 4 (over x, core).
Axes of the slice: x: 2, y: 2, z: 1, core: 2. Of those that a mesh axis runs over, the one named last changes fastest.
Arguments:
- kspace: float32 [2, 8, 16384], P(None, None, ('exam', 'rows', 'cols'))
- wts_y: float32 [4, 16384], P(None, ('exam', 'rows', 'cols'))
- wts_x: float32 [4, 16384], P(None, ('exam', 'rows', 'cols'))
- idx_y: int32 [16384], P(('exam', 'rows', 'cols'))
- idx_x: int32 [16384], P(('exam', 'rows', 'cols'))
- coil_maps: float32 [2, 8, 368, 368], P(None, ('exam', 'cols'), None, 'rows')
- deapod: float32 [368], replicated
Outputs:
- output: float32 [2, 368, 368], P(None, ('exam', 'cols'), 'rows')
All inputs are finite; a program needn't handle non-finite values.
Results may differ from the reference program's by a relative error of at most 0.001.
Values are sent between devices in bfloat16 or wider.
A program may use at most 1 GiB of HBM per device.

```python
import math
import jax
import jax.numpy as jnp
from jax import lax

IMG_SIZE = 368
NUM_COILS = 8
KERNEL_WIDTH = 4
ROW_BLOCKS = 4
COL_BLOCKS = 2
BLOCK_SLOTS = 2048


def setup_inputs(seed: int = 0, part: int = 0) -> dict:
    root_key = jax.random.key(seed)
    part_key = jax.random.fold_in(root_key, part)
    sub_keys = jax.random.split(part_key, 6)
    grid_size = 2 * IMG_SIZE
    row_blk = grid_size // ROW_BLOCKS
    col_blk = grid_size // COL_BLOCKS
    n_total = ROW_BLOCKS * COL_BLOCKS * BLOCK_SLOTS
    block_id = jnp.arange(n_total) // BLOCK_SLOTS
    idx_y = (block_id // COL_BLOCKS) * row_blk + jax.random.randint(sub_keys[0], (n_total,), 0, row_blk)
    idx_x = (block_id % COL_BLOCKS) * col_blk + jax.random.randint(sub_keys[1], (n_total,), 0, col_blk)
    centre = grid_size // 2
    dist_sq = ((idx_y - centre) ** 2 + (idx_x - centre) ** 2).astype(jnp.float32)
    blob_width = grid_size / 32.0
    envelope = 1.0 + 8.0 * jnp.exp(-dist_sq / (2.0 * blob_width * blob_width))
    samp_scale = grid_size / (KERNEL_WIDTH * math.sqrt(n_total))
    kspace = jax.random.normal(sub_keys[2], (2, NUM_COILS, n_total), jnp.float32) * (envelope * samp_scale)
    wts_y = jax.random.uniform(sub_keys[3], (KERNEL_WIDTH, n_total), jnp.float32, 0.2, 1.0)
    wts_x = jax.random.uniform(sub_keys[4], (KERNEL_WIDTH, n_total), jnp.float32, 0.2, 1.0)
    coil_maps = jax.random.normal(sub_keys[5], (2, NUM_COILS, IMG_SIZE, IMG_SIZE), jnp.float32) / math.sqrt(2.0 * NUM_COILS)
    shared_key = jax.random.key(seed + 99)
    deapod = jax.random.uniform(shared_key, (IMG_SIZE,), jnp.float32, 0.6, 1.4)
    return {'kspace': kspace, 'wts_y': wts_y, 'wts_x': wts_x, 'idx_y': idx_y, 'idx_x': idx_x, 'coil_maps': coil_maps, 'deapod': deapod}


def dft_matrix():
    grid_size = 2 * IMG_SIZE
    freq_idx = jnp.arange(grid_size) - grid_size // 2
    pos_idx = jnp.arange(IMG_SIZE) - IMG_SIZE // 2
    phase_int = (freq_idx[:, None] * pos_idx[None, :]) % grid_size
    phase_ang = phase_int.astype(jnp.float32) * (2.0 * math.pi / grid_size)
    dft_norm = 1.0 / math.sqrt(grid_size)
    cos_t = jnp.cos(phase_ang) * dft_norm
    sin_t = jnp.sin(phase_ang) * dft_norm
    upper_half = jnp.stack([cos_t, sin_t], axis=1)
    lower_half = jnp.stack([-sin_t, cos_t], axis=1)
    return jnp.stack([upper_half, lower_half], axis=0).astype(jnp.bfloat16)


def grid_spread(kspace, wts_y, wts_x, idx_y, idx_x):
    grid_size = 2 * IMG_SIZE
    half_w = KERNEL_WIDTH // 2
    tap_ids = jnp.arange(KERNEL_WIDTH)
    tap_pairs = (jnp.repeat(tap_ids, KERNEL_WIDTH), jnp.tile(tap_ids, KERNEL_WIDTH))

    def add_tap(k_grid, tap_pair):
        tap_a, tap_b = tap_pair
        rows_at = (idx_y + tap_a - half_w) % grid_size
        cols_at = (idx_x + tap_b - half_w) % grid_size
        weight = wts_y[tap_a] * wts_x[tap_b]
        return k_grid.at[:, :, rows_at, cols_at].add(kspace * weight), None

    start_grid = jnp.zeros((2, NUM_COILS, grid_size, grid_size), jnp.float32)
    k_grid, _ = lax.scan(add_tap, start_grid, tap_pairs)
    return k_grid


def reference(kspace, wts_y, wts_x, idx_y, idx_x, coil_maps, deapod):
    k_grid = grid_spread(kspace, wts_y, wts_x, idx_y, idx_x).astype(jnp.bfloat16)
    dft_mat = dft_matrix().astype(jnp.float32)
    half_img = jnp.einsum('scuv,svtq->tcuq', k_grid.astype(jnp.float32), dft_mat).astype(jnp.bfloat16)
    coil_img = jnp.einsum('tcuq,tuop->ocpq', half_img.astype(jnp.float32), dft_mat)
    out_re = jnp.sum(coil_maps[0] * coil_img[0] + coil_maps[1] * coil_img[1], axis=0)
    out_im = jnp.sum(coil_maps[0] * coil_img[1] - coil_maps[1] * coil_img[0], axis=0)
    apod_2d = deapod[:, None] * deapod[None, :]
    return jnp.stack([out_re, out_im]) * apod_2d
```

```python
import functools
import math

import jax
import jax.numpy as jnp
import numpy as np
from jax import lax
from jax.experimental import pallas as pl
from jax.experimental.pallas import tpu as pltpu
from jax.sharding import PartitionSpec as P

F32, BF16 = jnp.float32, jnp.bfloat16
MESH = pl.DeviceIdType.MESH

N_IMG = 368
N_GRID = 736
ROW_BLK = 184
Q_BLK, Q_PAD = 92, 96
P_BLK, P_PAD = 184, 192
N_CH = 8
TILE_U, STRIDE_U, N_SRC = 16, 13, 15
N_TGT = 12
VR = 752
KV = 768
N_CHUNK = 6
N_COPY = 4
CHUNK_TILES = [(1 + 2 * j, 2 + 2 * j) for j in range(5)] + [(0, 11)]


def dft_constants():
    scale = 1.0 / math.sqrt(N_GRID)
    phase = ((np.arange(N_GRID)[:, None] - N_GRID // 2) * (np.arange(N_IMG)[None, :] - N_IMG // 2)) % N_GRID
    ang = phase.astype(np.float64) * (2.0 * math.pi / N_GRID)
    parts = (np.cos(ang) * scale, np.sin(ang) * scale)
    e1 = np.zeros((4, 2, Q_PAD, KV))
    for dest in range(4):
        for cs in range(2):
            e1[dest, cs, :Q_BLK, 6:6 + N_GRID] = parts[cs][:, dest * Q_BLK:(dest + 1) * Q_BLK].T
    e2 = np.zeros((N_CHUNK, 4, 2, TILE_U, 2, 2, P_PAD))
    for j in range(N_CHUNK):
        for src in range(4):
            for tl in range(2):
                base = TILE_U * CHUNK_TILES[j][tl]
                rows = min(TILE_U, ROW_BLK - base)
                u0 = src * ROW_BLK + base
                for cs in range(2):
                    for k in range(2):
                        e2[j, src, tl, :rows, cs, k, :P_BLK] = parts[cs][u0:u0 + rows, k * P_BLK:(k + 1) * P_BLK]
    return (jnp.asarray(e1.reshape(8 * Q_PAD, KV).astype(np.float32)).astype(BF16),
            jnp.asarray(e2.reshape(N_CHUNK * 128, 4 * P_PAD).astype(np.float32)).astype(BF16))


def exchange_kernel(y_ref, wy_ref, wx_ref, iy_ref, ix_ref, y8_ref, wyo_ref, wxo_ref, addr_ref, roff_ref,
                    ysend, asend, rsend, send_sem, recv_sem):
    k = lax.axis_index('cols')
    r = lax.axis_index('rows')
    other = 1 - k
    barrier = pltpu.get_barrier_semaphore()
    pl.semaphore_signal(barrier, inc=1, device_id={'cols': other}, device_id_type=MESH)
    n = y_ref.shape[2]
    y_re, y_im = y_ref[0], y_ref[1]
    low = jnp.concatenate([y_re[0:4], y_im[0:4]], axis=0)
    high = jnp.concatenate([y_re[4:8], y_im[4:8]], axis=0)
    first = k == 0
    y8_ref[:, 0:n] = jnp.where(first, low, high)
    ysend[...] = jnp.where(first, high, low)
    wyo_ref[:, 0:n] = wy_ref[...]
    wxo_ref[0] = wx_ref[...]
    row = iy_ref[...] - r * ROW_BLK
    tile = jnp.zeros_like(row)
    for t in range(1, N_SRC):
        tile = tile + jnp.where(row >= STRIDE_U * t, 1, 0)
    addr = tile * VR + ix_ref[...]
    roff = row - STRIDE_U * tile
    addr_ref[0:16, :] = addr
    roff_ref[0:16, :] = roff
    asend[...] = addr
    rsend[...] = roff
    pl.semaphore_wait(barrier, 1)
    pairs = [(ysend, y8_ref.at[:, n:2 * n]), (wy_ref, wyo_ref.at[:, n:2 * n]), (wx_ref, wxo_ref.at[1]),
             (asend, addr_ref.at[16:32]), (rsend, roff_ref.at[16:32])]
    copies = []
    for i, (src, dst) in enumerate(pairs):
        copies.append(pltpu.make_async_remote_copy(src_ref=src, dst_ref=dst, send_sem=send_sem.at[i], recv_sem=recv_sem.at[i],
                                                   device_id={'cols': other}, device_id_type=MESH))
        copies[-1].start()
    for c in copies:
        c.wait()


def split3(x):
    hi = x.astype(BF16).astype(F32)
    rest = x - hi
    mid = rest.astype(BF16).astype(F32)
    return [hi, mid, rest - mid]


def spread_kernel(addr_ref, y_ref, wy_ref, wx_ref, roff_ref, g_ref, f0_ref, f11_ref, gp_ref, gn_ref, *scr):
    accs = scr[:N_COPY]
    q_scr, raw0 = scr[N_COPY:]
    n = y_ref.shape[1]

    def zero(i, _):
        for a in accs:
            a[pl.ds(pl.multiple_of(i * VR, 8), VR), :] = jnp.zeros((VR, 128), F32)
        return 0
    lax.fori_loop(0, N_SRC, zero, 0)

    r = lax.broadcasted_iota(jnp.int32, (80, 256), 0)
    l = lax.broadcasted_iota(jnp.int32, (80, 256), 1)
    ry = (r < 24) & (l < 128) & ((r & 7) == (l >> 4))
    rw = (r >= 24) & (r < 72) & (l >= 128) & (((r - 24) & 15) == (l & 15))
    expand = jnp.where(ry | rw, 1.0, 0.0).astype(BF16)
    rr = lax.broadcasted_iota(jnp.int32, (16, 512), 0)

    def prep(i, _):
        ds = pl.ds(pl.multiple_of(i * 512, 512), 512)
        y = y_ref[:, ds]
        wy = wy_ref[:, ds]
        ro = jnp.concatenate([roff_ref[pl.ds(4 * i + s, 1), :] for s in range(4)], axis=1)
        d = rr - ro
        w16 = jnp.zeros((16, 512), F32)
        for a in range(4):
            w16 = jnp.where(d == a, wy[a:a + 1], w16)
        lhs = jnp.concatenate(split3(y) + split3(w16) + [jnp.zeros((8, 512), F32)], axis=0).astype(BF16)
        o = lax.dot_general(lhs, expand, (((0,), (0,)), ((), ())), preferred_element_type=F32)
        q_scr[ds, :] = o[:, :128] * o[:, 128:]
        return 0
    lax.fori_loop(0, n // 512, prep, 0)

    sub = lax.broadcasted_iota(jnp.int32, (8, 128), 0)
    top = sub < 4
    half = n // 2

    def block(i, _):
        ds = pl.ds(pl.multiple_of(i * 128, 128), 128)
        wx = jnp.concatenate([wx_ref[0, :, ds], wx_ref[1, :, ds]], axis=0)
        for j in range(128):
            col = jnp.broadcast_to(wx[:, j:j + 1], (8, 128))
            for h in range(2):
                acc = accs[(2 * j + h) % N_COPY]
                base = addr_ref[i + 16 * h, j] + (4 if h == 0 else 0)
                row = jnp.broadcast_to(q_scr[pl.ds(pl.multiple_of(i * 128, 128) + (j + half * h), 1), :], (8, 128))
                s = pl.ds(base, 8)
                c = jnp.where(top, col, 0.0) if h == 0 else jnp.where(top, 0.0, col)
                acc[s, :] = acc[s, :] + c * row
        return 0
    lax.fori_loop(0, half // 128, block, 0)

    for t in range(N_SRC):
        sa, sb = pl.ds(t * VR, 8), pl.ds(t * VR + 736, 8)
        a = accs[0][sa, :]
        b = accs[0][sb, :]
        for acc in accs[1:]:
            a = a + acc[sa, :]
            b = b + acc[sb, :]
            acc[sa, :] = jnp.zeros((8, 128), F32)
            acc[sb, :] = jnp.zeros((8, 128), F32)
        accs[0][sa, :] = a + jnp.where(sub == 6, b, 0.0)
        accs[0][sb, :] = b + jnp.where((sub == 4) | (sub == 5), a, 0.0)

    lane16 = lax.broadcasted_iota(jnp.int32, (16, 128), 1) & 15

    def retile(i, _):
        off = pl.multiple_of(i * 16, 16)
        tiles = []
        for t in range(N_SRC):
            s = pl.ds(t * VR + off, 16)
            v = accs[0][s, :]
            for acc in accs[1:]:
                v = v + acc[s, :]
            tiles.append(v)
        raw0[pl.ds(off, 16), :] = tiles[0]
        for m in range(N_TGT):
            out = None
            for t in range(N_SRC):
                delta = STRIDE_U * t - TILE_U * m - 2
                lo, hi = max(0, delta), min(15, 15 + delta)
                if lo > hi:
                    continue
                v = tiles[t] if delta % 128 == 0 else pltpu.roll(tiles[t], delta % 128, 1)
                if lo > 0 or hi < 15:
                    v = jnp.where((lane16 >= lo) & (lane16 <= hi), v, 0.0)
                out = v if out is None else out + v
            if m == 0:
                f0_ref[pl.ds(off, 16), :] = out
            elif m == N_TGT - 1:
                f11_ref[pl.ds(off, 16), :] = out
            else:
                g_ref[pl.ds(off, 16), (m - 1) * 128:m * 128] = out.astype(BF16)
        return 0
    lax.fori_loop(0, VR // 16, retile, 0)
    g_ref[VR:KV, :] = jnp.zeros((KV - VR, g_ref.shape[1]), BF16)
    for ref in (raw0, f0_ref, f11_ref):
        ref[VR:KV, :] = jnp.zeros((KV - VR, 128), F32)

    la = lax.broadcasted_iota(jnp.int32, (96, 128), 1) & 15
    gp = jnp.zeros((96, 128), F32)
    for c in range(8):
        v = raw0[96 * c:96 * c + 96, :]
        v = pltpu.roll(v, 2 * c, 1) if c else v
        gp = jnp.where((la == 2 * c) | (la == 2 * c + 1), v, gp)
    gp_ref[...] = gp
    lb = lax.broadcasted_iota(jnp.int32, (48, 128), 1) & 15
    gn = jnp.zeros((48, 128), F32)
    for c in range(16):
        v = f11_ref[48 * c:48 * c + 48, :]
        v = pltpu.roll(v, (c - 8) % 128, 1) if c != 8 else v
        gn = jnp.where(lb == c, v, gn)
    gn_ref[...] = gn


def transform_kernel(g_ref, f0_ref, f11_ref, gp_ref, gn_ref, e1_ref, e2_ref, s_ref, out_ref,
                     edge, msg, recv, gpr, gnr, e2f, st, img, psend, precv,
                     msend_sem, mrecv_sem, gsend_sem, grecv_sem, psend_sem, precv_sem):
    k = lax.axis_index('cols')
    r = lax.axis_index('rows')
    chip, core = r // 2, r % 2
    dests = [2 * (1 - chip) + core, 2 * (1 - chip) + (1 - core), 2 * chip + (1 - core)]
    nxt, prv = lax.rem(r + 1, 4), lax.rem(r + 3, 4)
    barrier = pltpu.get_barrier_semaphore()
    for d in dests:
        pl.semaphore_signal(barrier, inc=1, device_id={'rows': d}, device_id_type=MESH)
    pl.semaphore_signal(barrier, inc=1, device_id={'cols': 1 - k}, device_id_type=MESH)

    lane = lax.broadcasted_iota(jnp.int32, (Q_PAD, 256), 1) & 127

    def first_dft(j, g):
        ab = jnp.dot(e1_ref[...], g, preferred_element_type=F32)
        for d in range(4):
            a = ab[192 * d:192 * d + 96]
            b = ab[192 * d + 96:192 * d + 192]
            b = jnp.concatenate([pltpu.roll(b[:, :128], 64, 1), pltpu.roll(b[:, 128:], 64, 1)], axis=1)
            msg[j, d] = jnp.where(lane < 64, a - b, a + b).astype(BF16)

    def message(j, i):
        d = dests[i]
        return pltpu.make_async_remote_copy(src_ref=msg.at[j, d], dst_ref=recv.at[j, r], send_sem=msend_sem.at[j, i],
                                            recv_sem=mrecv_sem.at[j, r], device_id={'rows': d}, device_id_type=MESH)

    def arrival(j, i):
        d = dests[i]
        return pltpu.make_async_remote_copy(src_ref=msg.at[j, d], dst_ref=recv.at[j, d], send_sem=msend_sem.at[j, i],
                                            recv_sem=mrecv_sem.at[j, d], device_id={'rows': d}, device_id_type=MESH)

    def post(j):
        for i in range(3):
            message(j, i).start()
        recv[j, r] = msg[j, r]

    first_dft(0, g_ref[:, 0:256])
    pl.semaphore_wait(barrier, 4)
    to_prv = pltpu.make_async_remote_copy(src_ref=gp_ref, dst_ref=gpr, send_sem=gsend_sem.at[0], recv_sem=grecv_sem.at[0],
                                          device_id={'rows': prv}, device_id_type=MESH)
    to_nxt = pltpu.make_async_remote_copy(src_ref=gn_ref, dst_ref=gnr, send_sem=gsend_sem.at[1], recv_sem=grecv_sem.at[1],
                                          device_id={'rows': nxt}, device_id_type=MESH)
    to_prv.start()
    to_nxt.start()
    post(0)

    def middle(j, _):
        first_dft(j, g_ref[:, pl.ds(pl.multiple_of(j * 256, 256), 256)])
        post(j)
        return 0
    lax.fori_loop(1, 5, middle, 0)

    to_prv.wait()
    to_nxt.wait()
    la = lax.broadcasted_iota(jnp.int32, (96, 128), 1) & 15
    lb = lax.broadcasted_iota(jnp.int32, (48, 128), 1) & 15
    gp, gn = gpr[...], gnr[...]
    for c in range(8):
        s = slice(96 * c, 96 * c + 96)
        add = jnp.where((la == 6) | (la == 7), pltpu.roll(gp, (6 - 2 * c) % 128, 1) if c != 3 else gp, 0.0)
        edge[s, 128:256] = (f11_ref[s, :] + add).astype(BF16)
    for c in range(16):
        s = slice(48 * c, 48 * c + 48)
        add = jnp.where(lb == 0, pltpu.roll(gn, (-c) % 128, 1) if c else gn, 0.0)
        edge[s, 0:128] = (f0_ref[s, :] + add).astype(BF16)
    first_dft(5, edge[...])
    post(5)

    for j in range(N_CHUNK):
        v = e2_ref[128 * j:128 * j + 128, :]
        e2f[j, 0:128, :] = v
        e2f[j, 128:256, 0:384] = -v[:, 384:768]
        e2f[j, 128:256, 384:768] = v[:, 0:384]
    st[...] = jnp.zeros_like(st)
    for s in range(2):
        for c in range(4):
            for h in range(2):
                st[s, c, 0:Q_BLK, P_PAD * h:P_PAD * h + P_BLK] = s_ref[s, c, P_BLK * h:P_BLK * h + P_BLK, :].T

    grp = lax.broadcasted_iota(jnp.int32, (Q_PAD, 128), 1) >> 4

    def regroup(j):
        v = [recv[j, s // 2, :, 128 * (s % 2):128 * (s % 2) + 128].astype(F32) for s in range(8)]
        for b in range(3):
            bit = 1 << b
            m = (grp & bit) == 0
            for s in range(8):
                if s & bit:
                    continue
                x, y = v[s], v[s | bit]
                v[s] = jnp.where(m, x, pltpu.roll(y, 16 * bit, 1))
                v[s | bit] = jnp.where(m, pltpu.roll(x, 128 - 16 * bit, 1), y)
        return [x.astype(BF16) for x in v]

    def second_dft(j):
        for i in range(3):
            arrival(j, i).wait_recv()
        v = regroup(j)
        lhs = jnp.concatenate([jnp.concatenate([v[c], v[4 + c]], axis=1) for c in range(4)], axis=0)
        return jnp.dot(lhs, e2f[j], preferred_element_type=F32)

    img[...] = second_dft(0)

    def accumulate(j, _):
        img[...] += second_dft(j)
        return 0
    lax.fori_loop(1, N_CHUNK, accumulate, 0)

    x_re = jnp.zeros((Q_PAD, 384), F32)
    x_im = jnp.zeros((Q_PAD, 384), F32)
    for c in range(4):
        i_re = img[96 * c:96 * c + 96, 0:384]
        i_im = img[96 * c:96 * c + 96, 384:768]
        x_re = x_re + st[0, c] * i_re + st[1, c] * i_im
        x_im = x_im + st[0, c] * i_im - st[1, c] * i_re
    lo = jnp.concatenate([x_re[:, 0:192], x_im[:, 0:192]], axis=1)
    hi = jnp.concatenate([x_re[:, 192:384], x_im[:, 192:384]], axis=1)
    first = k == 0
    psend[...] = jnp.where(first, hi, lo)
    swap = pltpu.make_async_remote_copy(src_ref=psend, dst_ref=precv, send_sem=psend_sem, recv_sem=precv_sem,
                                        device_id={'cols': 1 - k}, device_id_type=MESH)
    swap.start()
    mine = jnp.where(first, lo, hi)
    for j in range(N_CHUNK):
        for i in range(3):
            message(j, i).wait_send()
    swap.wait()
    total = mine + precv[...]
    out_ref[0] = total[0:Q_BLK, 0:P_BLK].T
    out_ref[1] = total[0:Q_BLK, P_PAD:P_PAD + P_BLK].T


def solution(mesh):
    sample_spec = ('exam', 'rows', 'cols')
    vmem = pl.BlockSpec(memory_space=pltpu.VMEM)
    smem = pl.BlockSpec(memory_space=pltpu.SMEM)
    sds = jax.ShapeDtypeStruct

    def local_fn(kspace, wts_y, wts_x, idx_y, idx_x, coil_maps, deapod):
        n = kspace.shape[2]
        row_id = lax.axis_index('rows')
        col_id = lax.axis_index('cols')
        e1, e2 = dft_constants()
        y8, wy, wx, addr, roff = pl.pallas_call(
            exchange_kernel,
            out_shape=[sds((8, 2 * n), F32), sds((4, 2 * n), F32), sds((2, 4, n), F32), sds((32, 128), jnp.int32), sds((32, 128), jnp.int32)],
            in_specs=[vmem] * 5,
            out_specs=[vmem] * 5,
            scratch_shapes=[pltpu.VMEM((8, n), F32), pltpu.VMEM((16, 128), jnp.int32), pltpu.VMEM((16, 128), jnp.int32),
                            pltpu.SemaphoreType.DMA((5,)), pltpu.SemaphoreType.DMA((5,))],
            compiler_params=pltpu.CompilerParams(collective_id=0, has_side_effects=True),
            name='exchange',
        )(kspace, wts_y, wts_x, idx_y.reshape(16, 128), idx_x.reshape(16, 128))
        g, f0, f11, gp, gn = pl.pallas_call(
            spread_kernel,
            out_shape=[sds((KV, 1280), BF16), sds((KV, 128), F32), sds((KV, 128), F32), sds((96, 128), F32), sds((48, 128), F32)],
            in_specs=[smem] + [vmem] * 4,
            out_specs=[vmem] * 5,
            scratch_shapes=[pltpu.VMEM((N_SRC * VR, 128), F32)] * N_COPY + [pltpu.VMEM((2 * n, 128), F32), pltpu.VMEM((KV, 128), F32)],
            compiler_params=pltpu.CompilerParams(vmem_limit_bytes=50 * 2**20),
            name='spread',
        )(addr, y8, wy, wx, roff)
        part = pl.pallas_call(
            transform_kernel,
            out_shape=sds((2, P_BLK, Q_BLK), F32),
            in_specs=[vmem] * 8,
            out_specs=vmem,
            scratch_shapes=[
                pltpu.VMEM((KV, 256), BF16),
                pltpu.VMEM((N_CHUNK, 4, Q_PAD, 256), BF16),
                pltpu.VMEM((N_CHUNK, 4, Q_PAD, 256), BF16),
                pltpu.VMEM((96, 128), F32),
                pltpu.VMEM((48, 128), F32),
                pltpu.VMEM((N_CHUNK, 256, 768), BF16),
                pltpu.VMEM((2, 4, Q_PAD, 384), F32),
                pltpu.VMEM((4 * Q_PAD, 768), F32),
                pltpu.VMEM((Q_PAD, 384), F32),
                pltpu.VMEM((Q_PAD, 384), F32),
                pltpu.SemaphoreType.DMA((N_CHUNK, 3)),
                pltpu.SemaphoreType.DMA((N_CHUNK, 4)),
                pltpu.SemaphoreType.DMA((2,)),
                pltpu.SemaphoreType.DMA((2,)),
                pltpu.SemaphoreType.DMA,
                pltpu.SemaphoreType.DMA,
            ],
            compiler_params=pltpu.CompilerParams(collective_id=1, has_side_effects=True, vmem_limit_bytes=50 * 2**20),
            name='transform',
        )(g, f0, f11, gp, gn, e1, e2, coil_maps)
        d_rows = lax.dynamic_slice(deapod, (col_id * P_BLK,), (P_BLK,))
        d_cols = lax.dynamic_slice(deapod, (row_id * Q_BLK,), (Q_BLK,))
        return part * (d_rows[:, None] * d_cols[None, :])

    return jax.shard_map(
        local_fn,
        mesh=mesh,
        in_specs=(P(None, None, sample_spec), P(None, sample_spec), P(None, sample_spec), P(sample_spec), P(sample_spec), P(None, ('exam', 'cols'), None, 'rows'), P()),
        out_specs=P(None, ('exam', 'cols'), 'rows'),
        check_vma=False,
    )
```

```python
import functools
import functools
import math

import jax
import jax.numpy as jnp
import numpy as np
from jax import lax
from jax.experimental import pallas as pl
from jax.experimental.pallas import tpu as pltpu
from jax.sharding import PartitionSpec as P

F32, BF16 = jnp.float32, jnp.bfloat16
MESH = pl.DeviceIdType.MESH

N_IMG = 368
N_GRID = 736
ROW_BLK = 184
Q_BLK, Q_PAD = 92, 96
P_BLK, P_PAD, P_ALL = 184, 192, 384
N_CH = 8
TILE_U, STRIDE_U, N_SRC = 16, 13, 15
N_TGT = 12
COL_BLK = 368
VR = 384
KV = 2 * VR
LANES, ROWS = 128, 16
EDGE = 6
N_CHUNK = 6
N_COPY = 4
CHUNK_TILES = [(1 + 2 * j, 2 + 2 * j) for j in range(5)] + [(0, 11)]


def dft_constants():
    scale = 1.0 / math.sqrt(N_GRID)
    phase = ((np.arange(N_GRID)[:, None] - N_GRID // 2) * (np.arange(N_IMG)[None, :] - N_IMG // 2)) % N_GRID
    ang = phase.astype(np.float64) * (2.0 * math.pi / N_GRID)
    parts = (np.cos(ang) * scale, np.sin(ang) * scale)
    e1 = np.zeros((4, 2, Q_PAD, 2, VR))
    for dest in range(4):
        for cs in range(2):
            for half in range(2):
                    part = parts[cs][half * COL_BLK:(half + 1) * COL_BLK, dest * Q_BLK:(dest + 1) * Q_BLK]
                    e1[dest, cs, :Q_BLK, half, EDGE:EDGE + COL_BLK] = part.T
    e2 = np.zeros((N_CHUNK, 4, 2, TILE_U, 2, P_ALL))
    for j in range(N_CHUNK):
        for src in range(4):
            for tl in range(2):
                base = TILE_U * CHUNK_TILES[j][tl]
                rows = min(TILE_U, ROW_BLK - base)
                u0 = src * ROW_BLK + base
                for cs in range(2):
                    e2[j, src, tl, :rows, cs, :N_IMG] = parts[cs][u0:u0 + rows]
    return (jnp.asarray(e1.reshape(8 * Q_PAD, KV).astype(np.float32)).astype(BF16),
            jnp.asarray(e2.reshape(N_CHUNK * LANES, 2 * P_ALL).astype(np.float32)).astype(BF16))


def split3(x):
    hi = x.astype(BF16).astype(F32)
    rest = x - hi
    mid = rest.astype(BF16).astype(F32)
    return [hi, mid, rest - mid]


def spread_kernel(received, y_ref, wy_ref, wx_ref, iy_ref, ix_ref, *refs):
    accs = refs[:N_COPY]
    qa, qb, y_sel, roff, addr_v, addr, sem = refs[N_COPY:]
    k = lax.axis_index('cols')
    r = lax.axis_index('rows')
    half = 1 - k if received else k
    n = y_ref.shape[2]

    row = iy_ref[...] - r * ROW_BLK
    tile = jnp.zeros_like(row)
    for t in range(1, N_SRC):
        tile = tile + jnp.where(row >= STRIDE_U * t, 1, 0)
    addr_v[...] = tile * VR + (ix_ref[...] - half * COL_BLK)
    roff[...] = row - STRIDE_U * tile
    to_smem = pltpu.make_async_copy(addr_v, addr, sem)
    to_smem.start()
    y_re, y_im = y_ref[0], y_ref[1]
    low = jnp.concatenate([y_re[0:4], y_im[0:4]], axis=0)
    high = jnp.concatenate([y_re[4:8], y_im[4:8]], axis=0)
    y_sel[...] = jnp.where(k == 0, low, high)

    def zero(i, _):
        for a in accs:
            a[pl.ds(pl.multiple_of(i * VR, 8), VR), :] = jnp.zeros((VR, LANES), F32)
        return 0
    lax.fori_loop(0, N_SRC, zero, 0)

    r0 = lax.broadcasted_iota(jnp.int32, (80, 256), 0)
    l0 = lax.broadcasted_iota(jnp.int32, (80, 256), 1)
    ry = (r0 < 24) & (l0 < LANES) & ((r0 & 7) == (l0 >> 4))
    rw = (r0 >= 24) & (r0 < 72) & (l0 >= LANES) & (((r0 - 24) & 15) == (l0 & 15))
    expand = jnp.where(ry | rw, 1.0, 0.0).astype(BF16)
    rr = lax.broadcasted_iota(jnp.int32, (ROWS, 256), 0)
    n_blk = n // 256

    def prep(i, q_ref):
        ds = [pl.ds(pl.multiple_of((i + n_blk * h) * LANES, LANES), LANES) for h in range(2)]
        y = jnp.concatenate([y_sel[:, s] for s in ds], axis=1)
        wy = jnp.concatenate([wy_ref[:, s] for s in ds], axis=1)
        d = rr - jnp.concatenate([roff[pl.ds(i + n_blk * h, 1), :] for h in range(2)], axis=1)
        w16 = jnp.zeros((ROWS, 256), F32)
        for a in range(4):
            w16 = jnp.where(d == a, wy[a:a + 1], w16)
        lhs = jnp.concatenate(split3(y) + split3(w16) + [jnp.zeros((8, 256), F32)], axis=0).astype(BF16)
        o = lax.dot_general(lhs, expand, (((0,), (0,)), ((), ())), preferred_element_type=F32)
        q_ref[...] = o[:, :LANES] * o[:, LANES:]

    top = lax.broadcasted_iota(jnp.int32, (8, LANES), 0) < 4

    def scatter(i, q_ref):
        wx = jnp.concatenate([wx_ref[:, pl.ds(pl.multiple_of((i + n_blk * h) * LANES, LANES), LANES)] for h in range(2)], axis=0)
        for j in range(LANES):
            col = jnp.broadcast_to(wx[:, j:j + 1], (8, LANES))
            for h in range(2):
                acc = accs[(2 * j + h) % N_COPY]
                base = addr[i + n_blk * h, j] + (0 if h else 4)
                q = jnp.broadcast_to(q_ref[j + LANES * h:j + LANES * h + 1, :], (8, LANES))
                s = pl.ds(base, 8)
                c = jnp.where(top, 0.0, col) if h else jnp.where(top, col, 0.0)
                acc[s, :] = acc[s, :] + c * q

    prep(0, qa)
    to_smem.wait()

    def two_blocks(i, _):
        prep(2 * i + 1, qb)
        scatter(2 * i, qa)
        prep(lax.rem(2 * i + 2, n_blk), qa)
        scatter(2 * i + 1, qb)
        return 0
    lax.fori_loop(0, n_blk // 2, two_blocks, 0)


def transform_kernel(*refs):
    own, nbr = refs[:N_COPY], refs[N_COPY:2 * N_COPY]
    (e1_ref, e2_ref, s_ref, out_ref, gch, raw0, f0, f11, gps, gns, msg, recv, gpr, gnr, e2f, st, img, psend, precv,
     msend_sem, mrecv_sem, gsend_sem, grecv_sem, psend_sem, precv_sem) = refs[2 * N_COPY:]
    k = lax.axis_index('cols')
    r = lax.axis_index('rows')
    chip, core = r // 2, r % 2
    dests = [2 * (1 - chip) + core, 2 * (1 - chip) + (1 - core), 2 * chip + (1 - core)]
    nxt, prv = lax.rem(r + 1, 4), lax.rem(r + 3, 4)
    barrier = pltpu.get_barrier_semaphore()
    for d in dests:
        pl.semaphore_signal(barrier, inc=1, device_id={'rows': d}, device_id_type=MESH)
    pl.semaphore_signal(barrier, inc=1, device_id={'cols': 1 - k}, device_id_type=MESH)

    slots = ((own, k), (nbr, 1 - k))
    lane16 = lax.broadcasted_iota(jnp.int32, (ROWS, LANES), 1) & 15
    sub16 = lax.broadcasted_iota(jnp.int32, (ROWS, LANES), 0)

    def merged(accs, off, targets):
        wanted = {}
        for m in targets:
            deltas = {0: 0} if m is None else {t: STRIDE_U * t - TILE_U * m - 2 for t in range(N_SRC)}
            wanted[m] = {t: d for t, d in deltas.items() if abs(d) < ROWS}
        loaded = {}
        for t in sorted({t for w in wanted.values() for t in w}):
            s = pl.ds(t * VR + off, ROWS)
            v = accs[0][s, :]
            for acc in accs[1:]:
                v = v + acc[s, :]
            loaded[t] = v
        outs = []
        for m in targets:
            out = None
            for t, d in wanted[m].items():
                lo, hi = max(0, d), min(15, 15 + d)
                v = pltpu.roll(loaded[t], d % LANES, 1) if d else loaded[t]
                if lo > 0 or hi < 15:
                    v = jnp.where((lane16 >= lo) & (lane16 <= hi), v, 0.0)
                out = v if out is None else out + v
            outs.append(out)
        return outs

    def merge_all(targets, put):
        def rows(i, _):
            for accs, half in slots:
                off = pl.multiple_of(i * ROWS, ROWS)
                put(pl.multiple_of(half * VR + off, ROWS), merged(accs, off, targets))
            return 0
        lax.fori_loop(1, VR // ROWS - 1, rows, 0)
        last = VR - ROWS
        a = [merged(accs, 0, targets) for accs, _ in slots]
        b = [merged(accs, last, targets) for accs, _ in slots]
        for i, (_, half) in enumerate(slots):
            fix_a = [x + jnp.where(sub16 == 6, y, 0.0) for x, y in zip(a[i], b[1 - i])]
            fix_b = [y + jnp.where((sub16 == 4) | (sub16 == 5), x, 0.0) for x, y in zip(a[1 - i], b[i])]
            put(pl.multiple_of(half * VR, ROWS), fix_a)
            put(pl.multiple_of(half * VR + last, ROWS), fix_b)

    def put_chunk(off, vals):
        for i, v in enumerate(vals):
            gch[pl.ds(off, ROWS), LANES * i:LANES * (i + 1)] = v.astype(BF16)

    def put_edges(off, vals):
        for ref, v in zip((raw0, f0, f11), vals):
            ref[pl.ds(off, ROWS), :] = v

    lane = lax.broadcasted_iota(jnp.int32, (Q_PAD, 256), 1) & 127

    def first_dft(j, g):
        ab = jnp.dot(e1_ref[...], g, preferred_element_type=F32)
        for d in range(4):
            a = ab[192 * d:192 * d + 96]
            b = ab[192 * d + 96:192 * d + 192]
            b = jnp.concatenate([pltpu.roll(b[:, :128], 64, 1), pltpu.roll(b[:, 128:], 64, 1)], axis=1)
            msg[j, d] = jnp.where(lane < 64, a - b, a + b).astype(BF16)

    def message(j, i):
        d = dests[i]
        return pltpu.make_async_remote_copy(src_ref=msg.at[j, d], dst_ref=recv.at[j, r], send_sem=msend_sem.at[j, i],
                                            recv_sem=mrecv_sem.at[j, r], device_id={'rows': d}, device_id_type=MESH)

    def arrival(j, i):
        d = dests[i]
        return pltpu.make_async_remote_copy(src_ref=msg.at[j, d], dst_ref=recv.at[j, d], send_sem=msend_sem.at[j, i],
                                            recv_sem=mrecv_sem.at[j, d], device_id={'rows': d}, device_id_type=MESH)

    def post(j):
        for i in range(3):
            message(j, i).start()
        recv[j, r] = msg[j, r]

    merge_all(CHUNK_TILES[0], put_chunk)
    first_dft(0, gch[...])
    pl.semaphore_wait(barrier, 4)
    post(0)

    merge_all((None, 0, N_TGT - 1), put_edges)
    la = lax.broadcasted_iota(jnp.int32, (96, LANES), 1) & 15
    lb = lax.broadcasted_iota(jnp.int32, (48, LANES), 1) & 15

    def shifted(v, by):
        return pltpu.roll(v, by % LANES, 1) if by else v

    gp = jnp.zeros((96, LANES), F32)
    for c in range(8):
        gp = jnp.where((la >> 1) == c, shifted(raw0[96 * c:96 * c + 96, :], 2 * c), gp)
    gps[...] = gp
    gn = jnp.zeros((48, LANES), F32)
    for c in range(16):
        gn = jnp.where(lb == c, shifted(f11[48 * c:48 * c + 48, :], c - 8), gn)
    gns[...] = gn
    to_prv = pltpu.make_async_remote_copy(src_ref=gps, dst_ref=gpr, send_sem=gsend_sem.at[0], recv_sem=grecv_sem.at[0],
                                          device_id={'rows': prv}, device_id_type=MESH)
    to_nxt = pltpu.make_async_remote_copy(src_ref=gns, dst_ref=gnr, send_sem=gsend_sem.at[1], recv_sem=grecv_sem.at[1],
                                          device_id={'rows': nxt}, device_id_type=MESH)
    to_prv.start()
    to_nxt.start()

    for j in range(1, N_CHUNK - 1):
        merge_all(CHUNK_TILES[j], put_chunk)
        first_dft(j, gch[...])
        post(j)

    to_prv.wait()
    to_nxt.wait()
    gp, gn = gpr[...], gnr[...]
    for c in range(8):
        s = slice(96 * c, 96 * c + 96)
        gch[s, LANES:2 * LANES] = (f11[s, :] + jnp.where((la >> 1) == 3, shifted(gp, 6 - 2 * c), 0.0)).astype(BF16)
    for c in range(16):
        s = slice(48 * c, 48 * c + 48)
        gch[s, 0:LANES] = (f0[s, :] + jnp.where(lb == 0, shifted(gn, -c), 0.0)).astype(BF16)
    first_dft(N_CHUNK - 1, gch[...])
    post(N_CHUNK - 1)

    for j in range(N_CHUNK):
        v = e2_ref[128 * j:128 * j + 128, :]
        e2f[j, 0:128, :] = v
        e2f[j, 128:256, 0:P_ALL] = -v[:, P_ALL:2 * P_ALL]
        e2f[j, 128:256, P_ALL:2 * P_ALL] = v[:, 0:P_ALL]
    st[...] = jnp.zeros_like(st)
    for s in range(2):
        for c in range(4):
            st[s, c, 0:Q_BLK, 0:N_IMG] = s_ref[s, :, c, :]

    grp = lax.broadcasted_iota(jnp.int32, (Q_PAD, 128), 1) >> 4

    def regroup(j):
        v = [recv[j, s // 2, :, 128 * (s % 2):128 * (s % 2) + 128].astype(F32) for s in range(8)]
        for b in range(3):
            bit = 1 << b
            m = (grp & bit) == 0
            for s in range(8):
                if s & bit:
                    continue
                x, y = v[s], v[s | bit]
                v[s] = jnp.where(m, x, pltpu.roll(y, 16 * bit, 1))
                v[s | bit] = jnp.where(m, pltpu.roll(x, 128 - 16 * bit, 1), y)
        return [x.astype(BF16) for x in v]

    def second_dft(j):
        for i in range(3):
            arrival(j, i).wait_recv()
        v = regroup(j)
        lhs = jnp.concatenate([jnp.concatenate([v[c], v[4 + c]], axis=1) for c in range(4)], axis=0)
        return jnp.dot(lhs, e2f[j], preferred_element_type=F32)

    img[...] = second_dft(0)

    def accumulate(j, _):
        img[...] += second_dft(j)
        return 0
    lax.fori_loop(1, N_CHUNK, accumulate, 0)

    x_re = jnp.zeros((Q_PAD, P_ALL), F32)
    x_im = jnp.zeros((Q_PAD, P_ALL), F32)
    for c in range(4):
        i_re = img[96 * c:96 * c + 96, 0:P_ALL]
        i_im = img[96 * c:96 * c + 96, P_ALL:2 * P_ALL]
        x_re = x_re + st[0, c] * i_re + st[1, c] * i_im
        x_im = x_im + st[0, c] * i_im - st[1, c] * i_re
    lo = jnp.concatenate([x_re[:, 0:P_PAD], x_im[:, 0:P_PAD]], axis=1)
    hi = jnp.concatenate([x_re[:, P_BLK:P_BLK + P_PAD], x_im[:, P_BLK:P_BLK + P_PAD]], axis=1)
    first = k == 0
    psend[...] = jnp.where(first, hi, lo)
    swap = pltpu.make_async_remote_copy(src_ref=psend, dst_ref=precv, send_sem=psend_sem, recv_sem=precv_sem,
                                        device_id={'cols': 1 - k}, device_id_type=MESH)
    swap.start()
    mine = jnp.where(first, lo, hi)
    for j in range(N_CHUNK):
        for i in range(3):
            message(j, i).wait_send()
    swap.wait()
    total = mine + precv[...]
    out_ref[0] = total[0:Q_BLK, 0:P_BLK].T
    out_ref[1] = total[0:Q_BLK, P_PAD:P_PAD + P_BLK].T


def solution(mesh):
    sample_spec = ('exam', 'rows', 'cols')
    vmem = pl.BlockSpec(memory_space=pltpu.VMEM)
    sds = jax.ShapeDtypeStruct

    def local_fn(kspace, wts_y, wts_x, idx_y, idx_x, coil_maps, deapod):
        n = kspace.shape[2]
        row_id = lax.axis_index('rows')
        col_id = lax.axis_index('cols')
        e1, e2 = dft_constants()
        samples = (kspace, wts_y, wts_x, idx_y.reshape(16, LANES), idx_x.reshape(16, LANES))
        moved = [lax.ppermute(x, 'cols', [(0, 1), (1, 0)]) for x in samples]

        def spread(received, args):
            return pl.pallas_call(
                functools.partial(spread_kernel, received),
                out_shape=[sds((N_SRC * VR, LANES), F32)] * N_COPY,
                in_specs=[vmem] * 5,
                out_specs=[vmem] * N_COPY,
                scratch_shapes=[pltpu.VMEM((256, LANES), F32), pltpu.VMEM((256, LANES), F32), pltpu.VMEM((8, n), F32),
                                pltpu.VMEM((16, LANES), jnp.int32), pltpu.VMEM((16, LANES), jnp.int32),
                                pltpu.SMEM((16, LANES), jnp.int32), pltpu.SemaphoreType.DMA],
                compiler_params=pltpu.CompilerParams(vmem_limit_bytes=16 * 2**20),
                cost_estimate=pl.CostEstimate(flops=10**8, bytes_accessed=10**7, transcendentals=0),
                name='spread_received' if received else 'spread_own',
            )(*args)

        accs = spread(False, samples)
        accs += spread(True, moved)
        maps = jnp.transpose(coil_maps, (0, 3, 1, 2))
        part = pl.pallas_call(
            transform_kernel,
            out_shape=sds((2, P_BLK, Q_BLK), F32),
            in_specs=[vmem] * (2 * N_COPY + 3),
            out_specs=vmem,
            scratch_shapes=[pltpu.VMEM((KV, 256), BF16)] + [pltpu.VMEM((KV, LANES), F32)] * 3 + [
                pltpu.VMEM((96, LANES), F32),
                pltpu.VMEM((48, LANES), F32),
                pltpu.VMEM((N_CHUNK, 4, Q_PAD, 256), BF16),
                pltpu.VMEM((N_CHUNK, 4, Q_PAD, 256), BF16),
                pltpu.VMEM((96, LANES), F32),
                pltpu.VMEM((48, LANES), F32),
                pltpu.VMEM((N_CHUNK, 256, 2 * P_ALL), BF16),
                pltpu.VMEM((2, 4, Q_PAD, P_ALL), F32),
                pltpu.VMEM((4 * Q_PAD, 2 * P_ALL), F32),
                pltpu.VMEM((Q_PAD, P_ALL), F32),
                pltpu.VMEM((Q_PAD, P_ALL), F32),
                pltpu.SemaphoreType.DMA((N_CHUNK, 3)),
                pltpu.SemaphoreType.DMA((N_CHUNK, 4)),
                pltpu.SemaphoreType.DMA((2,)),
                pltpu.SemaphoreType.DMA((2,)),
                pltpu.SemaphoreType.DMA,
                pltpu.SemaphoreType.DMA,
            ],
            compiler_params=pltpu.CompilerParams(collective_id=1, has_side_effects=True, vmem_limit_bytes=24 * 2**20),
            name='transform',
        )(*accs, e1, e2, maps)
        d_rows = lax.dynamic_slice(deapod, (col_id * P_BLK,), (P_BLK,))
        d_cols = lax.dynamic_slice(deapod, (row_id * Q_BLK,), (Q_BLK,))
        return part * (d_rows[:, None] * d_cols[None, :])

    return jax.shard_map(
        local_fn,
        mesh=mesh,
        in_specs=(P(None, None, sample_spec), P(None, sample_spec), P(None, sample_spec), P(sample_spec), P(sample_spec), P(None, ('exam', 'cols'), None, 'rows'), P()),
        out_specs=P(None, ('exam', 'cols'), 'rows'),
        check_vma=False,
    )
```

```python
import functools
import math

import jax
import jax.numpy as jnp
import numpy as np
from jax import lax
from jax.experimental import pallas as pl
from jax.experimental.pallas import tpu as pltpu
from jax.sharding import PartitionSpec as P

F32, BF16 = jnp.float32, jnp.bfloat16
MESH = pl.DeviceIdType.MESH

N_IMG = 368
N_GRID = 736
ROW_BLK = 184
Q_BLK, Q_PAD = 92, 96
P_BLK, P_PAD, P_ALL = 184, 192, 384
N_CH = 8
TILE_U, STRIDE_U, N_SRC = 16, 13, 15
N_TGT = 12
COL_BLK = 368
VR = 384
VS = 392
KV = 2 * VR
LANES, ROWS = 128, 16
EDGE = 6
N_CHUNK = 6
N_COPY = 3
CHUNK_TILES = [(1 + 2 * j, 2 + 2 * j) for j in range(5)] + [(0, 11)]


def dft_constants():
    scale = 1.0 / math.sqrt(N_GRID)
    phase = ((np.arange(N_GRID)[:, None] - N_GRID // 2) * (np.arange(N_IMG)[None, :] - N_IMG // 2)) % N_GRID
    ang = phase.astype(np.float64) * (2.0 * math.pi / N_GRID)
    parts = (np.cos(ang) * scale, np.sin(ang) * scale)
    e1 = np.zeros((4, 2, Q_PAD, 2, VR))
    for dest in range(4):
        for cs in range(2):
            for half in range(2):
                    part = parts[cs][half * COL_BLK:(half + 1) * COL_BLK, dest * Q_BLK:(dest + 1) * Q_BLK]
                    e1[dest, cs, :Q_BLK, half, EDGE:EDGE + COL_BLK] = part.T
    e2 = np.zeros((N_CHUNK, 4, 2, TILE_U, 2, P_ALL))
    for j in range(N_CHUNK):
        for src in range(4):
            for tl in range(2):
                base = TILE_U * CHUNK_TILES[j][tl]
                rows = min(TILE_U, ROW_BLK - base)
                u0 = src * ROW_BLK + base
                for cs in range(2):
                    e2[j, src, tl, :rows, cs, :N_IMG] = parts[cs][u0:u0 + rows]
    return (jnp.asarray(e1.reshape(8 * Q_PAD, KV).astype(np.float32)).astype(BF16),
            jnp.asarray(e2.reshape(N_CHUNK * LANES, 2 * P_ALL).astype(np.float32)).astype(BF16))


def exchange_kernel(y_hbm, wy_hbm, wx_hbm, iy_hbm, ix_hbm, y_ref, wy_ref, wx_ref, addr_ref, roff_ref, *refs):
    accs = refs[:2 * N_COPY]
    y_in, iy, ix, y_send, in_sem, send_sem, recv_sem = refs[2 * N_COPY:]
    k = lax.axis_index('cols')
    r = lax.axis_index('rows')
    other = {'cols': 1 - k}
    barrier = pltpu.get_barrier_semaphore()
    pl.semaphore_signal(barrier, inc=1, device_id=other, device_id_type=MESH)
    loads = [(iy_hbm, iy), (ix_hbm, ix), (y_hbm, y_in), (wy_hbm, wy_ref.at[0]), (wx_hbm, wx_ref.at[0])]
    loads = [pltpu.make_async_copy(a, b, in_sem.at[i]) for i, (a, b) in enumerate(loads)]
    for c in loads:
        c.start()

    def send(i, src, dst):
        c = pltpu.make_async_remote_copy(src_ref=src, dst_ref=dst, send_sem=send_sem.at[i], recv_sem=recv_sem.at[i],
                                         device_id=other, device_id_type=MESH)
        c.start()
        return c

    loads[0].wait()
    loads[1].wait()
    row = iy[...] - r * ROW_BLK
    tile = jnp.zeros_like(row)
    for t in range(1, N_SRC):
        tile = tile + jnp.where(row >= STRIDE_U * t, 1, 0)
    addr_ref[0] = tile * VS + (ix[...] - k * COL_BLK)
    roff_ref[0] = row - STRIDE_U * tile
    loads[2].wait()
    y_re, y_im = y_in[0], y_in[1]
    low = jnp.concatenate([y_re[0:4], y_im[0:4]], axis=0)
    high = jnp.concatenate([y_re[4:8], y_im[4:8]], axis=0)
    y_ref[0] = jnp.where(k == 0, low, high)
    y_send[...] = jnp.where(k == 0, high, low)
    loads[3].wait()
    loads[4].wait()
    pl.semaphore_wait(barrier, 1)
    copies = [send(0, wy_ref.at[0], wy_ref.at[1]), send(1, wx_ref.at[0], wx_ref.at[1]), send(2, addr_ref.at[0], addr_ref.at[1]),
              send(3, roff_ref.at[0], roff_ref.at[1]), send(4, y_send, y_ref.at[1])]

    def zero(i, _):
        for a in accs:
            a[pl.ds(pl.multiple_of(i * VS, 8), VS), :] = jnp.zeros((VS, LANES), F32)
        return 0
    lax.fori_loop(0, N_SRC, zero, 0)
    for c in copies:
        c.wait()


def split3(x):
    hi = x.astype(BF16).astype(F32)
    rest = x - hi
    mid = rest.astype(BF16).astype(F32)
    return [hi, mid, rest - mid]


def spread_kernel(addr_ref, y_ref, wy_ref, wx_ref, roff_ref, *refs):
    accs = refs[2 * N_COPY:4 * N_COPY]
    addr, sem = refs[4 * N_COPY], refs[-1]
    q_refs = refs[4 * N_COPY + 1:-1]
    to_smem = pltpu.make_async_copy(addr_ref, addr, sem)
    to_smem.start()
    n = y_ref.shape[2]

    r0 = lax.broadcasted_iota(jnp.int32, (80, 256), 0)
    l0 = lax.broadcasted_iota(jnp.int32, (80, 256), 1)
    ry = (r0 < 24) & (l0 < LANES) & ((r0 & 7) == (l0 >> 4))
    rw = (r0 >= 24) & (r0 < 72) & (l0 >= LANES) & (((r0 - 24) & 15) == (l0 & 15))
    expand = jnp.where(ry | rw, 1.0, 0.0).astype(BF16)
    rr = lax.broadcasted_iota(jnp.int32, (ROWS, 256), 0)
    n_blk = n // 256

    def prep(i, slot, q_ref):
        ds = [pl.ds(pl.multiple_of((i + n_blk * h) * LANES, LANES), LANES) for h in range(2)]
        y = jnp.concatenate([y_ref[slot, :, s] for s in ds], axis=1)
        wy = jnp.concatenate([wy_ref[slot, :, s] for s in ds], axis=1)
        d = rr - jnp.concatenate([roff_ref[slot, pl.ds(i + n_blk * h, 1), :] for h in range(2)], axis=1)
        w16 = jnp.zeros((ROWS, 256), F32)
        for a in range(4):
            w16 = jnp.where(d == a, wy[a:a + 1], w16)
        lhs = jnp.concatenate(split3(y) + split3(w16) + [jnp.zeros((8, 256), F32)], axis=0).astype(BF16)
        o = lax.dot_general(lhs, expand, (((0,), (0,)), ((), ())), preferred_element_type=F32)
        q_ref[...] = o[:, :LANES] * o[:, LANES:]

    top = lax.broadcasted_iota(jnp.int32, (8, LANES), 0) < 4

    def scatter(i, qs):
        ds = [pl.ds(pl.multiple_of((i + n_blk * h) * LANES, LANES), LANES) for h in range(2)]
        wx = [jnp.concatenate([wx_ref[slot, :, s] for s in ds], axis=0) for slot in range(2)]
        for j in range(LANES):
            cols = [jnp.broadcast_to(wx[slot][:, j:j + 1], (8, LANES)) for slot in range(2)]
            for h in range(2):
                for slot in range(2):
                    acc = accs[slot * N_COPY + (2 * j + h) % N_COPY]
                    base = addr[slot, i + n_blk * h, j] + (0 if h else 4)
                    q = jnp.broadcast_to(qs[slot][j + LANES * h:j + LANES * h + 1, :], (8, LANES))
                    s = pl.ds(base, 8)
                    c = jnp.where(top, 0.0, cols[slot]) if h else jnp.where(top, cols[slot], 0.0)
                    acc[s, :] = acc[s, :] + c * q

    qa, qb = q_refs[:2], q_refs[2:]
    for slot in range(2):
        prep(0, slot, qa[slot])
    to_smem.wait()

    def two_blocks(i, _):
        for step, now, then in ((0, qa, qb), (1, qb, qa)):
            for slot in range(2):
                prep(lax.rem(2 * i + step + 1, n_blk), slot, then[slot])
            scatter(2 * i + step, now)
        return 0
    lax.fori_loop(0, n_blk // 2, two_blocks, 0)


def transform_kernel(*refs):
    own, nbr = refs[:N_COPY], refs[N_COPY:2 * N_COPY]
    (e1_hbm, e2_hbm, s_hbm, d_hbm, out_ref, e1_ref, e2_ref, s_ref, d_ref, dd, gch, raw0, f0, f11, gps, gns, msg, recv, gpr, gnr, e2f, st, img, psend, precv,
     msend_sem, mrecv_sem, gsend_sem, grecv_sem, psend_sem, precv_sem, in_sem) = refs[2 * N_COPY:]
    k = lax.axis_index('cols')
    r = lax.axis_index('rows')
    chip, core = r // 2, r % 2
    dests = [2 * (1 - chip) + core, 2 * (1 - chip) + (1 - core), 2 * chip + (1 - core)]
    nxt, prv = lax.rem(r + 1, 4), lax.rem(r + 3, 4)
    barrier = pltpu.get_barrier_semaphore()
    for d in dests:
        pl.semaphore_signal(barrier, inc=1, device_id={'rows': d}, device_id_type=MESH)
    pl.semaphore_signal(barrier, inc=1, device_id={'cols': 1 - k}, device_id_type=MESH)

    loads = [pltpu.make_async_copy(a, b, in_sem.at[i]) for i, (a, b) in
             enumerate(((e1_hbm, e1_ref), (e2_hbm, e2_ref), (s_hbm, s_ref), (d_hbm, d_ref)))]
    for c in loads:
        c.start()
    slots = ((own, k), (nbr, 1 - k))
    lane16 = lax.broadcasted_iota(jnp.int32, (ROWS, LANES), 1) & 15
    sub16 = lax.broadcasted_iota(jnp.int32, (ROWS, LANES), 0)

    def merged(accs, off, targets):
        wanted = {}
        for m in targets:
            deltas = {0: 0} if m is None else {t: STRIDE_U * t - TILE_U * m - 2 for t in range(N_SRC)}
            wanted[m] = {t: d for t, d in deltas.items() if abs(d) < ROWS}
        loaded = {}
        for t in sorted({t for w in wanted.values() for t in w}):
            s = pl.ds(t * VS + off, ROWS)
            v = accs[0][s, :]
            for acc in accs[1:]:
                v = v + acc[s, :]
            loaded[t] = v
        outs = []
        for m in targets:
            out = None
            for t, d in wanted[m].items():
                lo, hi = max(0, d), min(15, 15 + d)
                v = pltpu.roll(loaded[t], d % LANES, 1) if d else loaded[t]
                if lo > 0 or hi < 15:
                    v = jnp.where((lane16 >= lo) & (lane16 <= hi), v, 0.0)
                out = v if out is None else out + v
            outs.append(out)
        return outs

    def merge_all(targets, put):
        def rows(i, _):
            for step in range(2):
                for accs, half in slots:
                    off = pl.multiple_of((2 * i + 1 + step) * ROWS, ROWS)
                    put(pl.multiple_of(half * VR + off, ROWS), merged(accs, off, targets))
            return 0
        lax.fori_loop(0, VR // (2 * ROWS) - 1, rows, 0)
        last = VR - ROWS
        a = [merged(accs, 0, targets) for accs, _ in slots]
        b = [merged(accs, last, targets) for accs, _ in slots]
        for i, (_, half) in enumerate(slots):
            fix_a = [x + jnp.where(sub16 == 6, y, 0.0) for x, y in zip(a[i], b[1 - i])]
            fix_b = [y + jnp.where((sub16 == 4) | (sub16 == 5), x, 0.0) for x, y in zip(a[1 - i], b[i])]
            put(pl.multiple_of(half * VR, ROWS), fix_a)
            put(pl.multiple_of(half * VR + last, ROWS), fix_b)

    def put_chunk(off, vals):
        for i, v in enumerate(vals):
            gch[pl.ds(off, ROWS), LANES * i:LANES * (i + 1)] = v.astype(BF16)

    def put_edges(off, vals):
        for ref, v in zip((raw0, f0, f11), vals):
            ref[pl.ds(off, ROWS), :] = v

    lane = lax.broadcasted_iota(jnp.int32, (Q_PAD, 256), 1) & 127

    def first_dft(j, g):
        ab = jnp.dot(e1_ref[...], g, preferred_element_type=F32)
        for d in range(4):
            a = ab[192 * d:192 * d + 96]
            b = ab[192 * d + 96:192 * d + 192]
            b = jnp.concatenate([pltpu.roll(b[:, :128], 64, 1), pltpu.roll(b[:, 128:], 64, 1)], axis=1)
            msg[j, d] = jnp.where(lane < 64, a - b, a + b).astype(BF16)

    def message(j, i):
        d = dests[i]
        return pltpu.make_async_remote_copy(src_ref=msg.at[j, d], dst_ref=recv.at[j, r], send_sem=msend_sem.at[j, i],
                                            recv_sem=mrecv_sem.at[j, r], device_id={'rows': d}, device_id_type=MESH)

    def arrival(j, i):
        d = dests[i]
        return pltpu.make_async_remote_copy(src_ref=msg.at[j, d], dst_ref=recv.at[j, d], send_sem=msend_sem.at[j, i],
                                            recv_sem=mrecv_sem.at[j, d], device_id={'rows': d}, device_id_type=MESH)

    def post(j):
        for i in range(3):
            message(j, i).start()
        recv[j, r] = msg[j, r]

    merge_all(CHUNK_TILES[0], put_chunk)
    loads[0].wait()
    first_dft(0, gch[...])
    pl.semaphore_wait(barrier, 4)
    post(0)

    merge_all((None, 0, N_TGT - 1), put_edges)
    la = lax.broadcasted_iota(jnp.int32, (96, LANES), 1) & 15
    lb = lax.broadcasted_iota(jnp.int32, (48, LANES), 1) & 15

    def shifted(v, by):
        return pltpu.roll(v, by % LANES, 1) if by else v

    gp = jnp.zeros((96, LANES), F32)
    for c in range(8):
        gp = jnp.where((la >> 1) == c, shifted(raw0[96 * c:96 * c + 96, :], 2 * c), gp)
    gps[...] = gp
    gn = jnp.zeros((48, LANES), F32)
    for c in range(16):
        gn = jnp.where(lb == c, shifted(f11[48 * c:48 * c + 48, :], c - 8), gn)
    gns[...] = gn
    to_prv = pltpu.make_async_remote_copy(src_ref=gps, dst_ref=gpr, send_sem=gsend_sem.at[0], recv_sem=grecv_sem.at[0],
                                          device_id={'rows': prv}, device_id_type=MESH)
    to_nxt = pltpu.make_async_remote_copy(src_ref=gns, dst_ref=gnr, send_sem=gsend_sem.at[1], recv_sem=grecv_sem.at[1],
                                          device_id={'rows': nxt}, device_id_type=MESH)
    to_prv.start()
    to_nxt.start()

    for j in range(1, N_CHUNK - 1):
        merge_all(CHUNK_TILES[j], put_chunk)
        first_dft(j, gch[...])
        post(j)

    to_prv.wait()
    to_nxt.wait()
    gp, gn = gpr[...], gnr[...]
    for c in range(8):
        s = slice(96 * c, 96 * c + 96)
        gch[s, LANES:2 * LANES] = (f11[s, :] + jnp.where((la >> 1) == 3, shifted(gp, 6 - 2 * c), 0.0)).astype(BF16)
    for c in range(16):
        s = slice(48 * c, 48 * c + 48)
        gch[s, 0:LANES] = (f0[s, :] + jnp.where(lb == 0, shifted(gn, -c), 0.0)).astype(BF16)
    first_dft(N_CHUNK - 1, gch[...])
    post(N_CHUNK - 1)

    for c in loads[1:]:
        c.wait()
    for j in range(N_CHUNK):
        v = e2_ref[128 * j:128 * j + 128, :]
        e2f[j, 0:128, :] = v
        e2f[j, 128:256, 0:P_ALL] = -v[:, P_ALL:2 * P_ALL]
        e2f[j, 128:256, P_ALL:2 * P_ALL] = v[:, 0:P_ALL]
    st[...] = jnp.zeros_like(st)
    for s in range(2):
        for c in range(4):
            st[s, c, 0:Q_BLK, 0:N_IMG] = s_ref[s, :, c, :]

    half_p = jnp.where(k == 0, d_ref[:, 0:P_BLK], d_ref[:, P_BLK:2 * P_BLK])
    part_q = d_ref[:, 0:Q_BLK]
    for i in range(1, 4):
        part_q = jnp.where(r == i, d_ref[:, Q_BLK * i:Q_BLK * (i + 1)], part_q)
    part_q = jnp.concatenate([part_q, jnp.zeros((1, LANES - Q_BLK), F32)], axis=1)
    dd[...] = jnp.broadcast_to(part_q, (8, LANES)).T[0:Q_BLK, 0:1] * half_p

    grp = lax.broadcasted_iota(jnp.int32, (Q_PAD, 128), 1) >> 4

    def regroup(j):
        v = [recv[j, s // 2, :, 128 * (s % 2):128 * (s % 2) + 128].astype(F32) for s in range(8)]
        for b in range(3):
            bit = 1 << b
            m = (grp & bit) == 0
            for s in range(8):
                if s & bit:
                    continue
                x, y = v[s], v[s | bit]
                v[s] = jnp.where(m, x, pltpu.roll(y, 16 * bit, 1))
                v[s | bit] = jnp.where(m, pltpu.roll(x, 128 - 16 * bit, 1), y)
        return [x.astype(BF16) for x in v]

    def second_dft(j):
        for i in range(3):
            arrival(j, i).wait_recv()
        v = regroup(j)
        lhs = jnp.concatenate([jnp.concatenate([v[c], v[4 + c]], axis=1) for c in range(4)], axis=0)
        return jnp.dot(lhs, e2f[j], preferred_element_type=F32)

    img[...] = second_dft(0)

    def accumulate(j, _):
        img[...] += second_dft(j)
        return 0
    lax.fori_loop(1, N_CHUNK, accumulate, 0)

    x_re = jnp.zeros((Q_PAD, P_ALL), F32)
    x_im = jnp.zeros((Q_PAD, P_ALL), F32)
    for c in range(4):
        i_re = img[96 * c:96 * c + 96, 0:P_ALL]
        i_im = img[96 * c:96 * c + 96, P_ALL:2 * P_ALL]
        x_re = x_re + st[0, c] * i_re + st[1, c] * i_im
        x_im = x_im + st[0, c] * i_im - st[1, c] * i_re
    lo = jnp.concatenate([x_re[:, 0:P_PAD], x_im[:, 0:P_PAD]], axis=1)
    hi = jnp.concatenate([x_re[:, P_BLK:P_BLK + P_PAD], x_im[:, P_BLK:P_BLK + P_PAD]], axis=1)
    first = k == 0
    psend[...] = jnp.where(first, hi, lo)
    swap = pltpu.make_async_remote_copy(src_ref=psend, dst_ref=precv, send_sem=psend_sem, recv_sem=precv_sem,
                                        device_id={'cols': 1 - k}, device_id_type=MESH)
    swap.start()
    mine = jnp.where(first, lo, hi)
    for j in range(N_CHUNK):
        for i in range(3):
            message(j, i).wait_send()
    swap.wait()
    total = mine + precv[...]
    out_ref[0] = (total[0:Q_BLK, 0:P_BLK] * dd[...]).T
    out_ref[1] = (total[0:Q_BLK, P_PAD:P_PAD + P_BLK] * dd[...]).T


def solution(mesh):
    sample_spec = ('exam', 'rows', 'cols')
    vmem = pl.BlockSpec(memory_space=pltpu.VMEM)
    hbm = pl.BlockSpec(memory_space=pltpu.HBM)
    sds = jax.ShapeDtypeStruct

    def local_fn(kspace, wts_y, wts_x, idx_y, idx_x, coil_maps, deapod):
        n = kspace.shape[2]
        e1, e2 = dft_constants()
        acc_shape = [sds((N_SRC * VS, LANES), F32)] * (2 * N_COPY)
        *samples, = pl.pallas_call(
            exchange_kernel,
            out_shape=[sds((2, 8, n), F32), sds((2, 4, n), F32), sds((2, 4, n), F32), sds((2, 16, LANES), jnp.int32),
                       sds((2, 16, LANES), jnp.int32)] + acc_shape,
            in_specs=[hbm] * 5,
            out_specs=[vmem] * (5 + 2 * N_COPY),
            scratch_shapes=[pltpu.VMEM((2, 8, n), F32), pltpu.VMEM((16, LANES), jnp.int32), pltpu.VMEM((16, LANES), jnp.int32),
                            pltpu.VMEM((8, n), F32), pltpu.SemaphoreType.DMA((5,)), pltpu.SemaphoreType.DMA((5,)),
                            pltpu.SemaphoreType.DMA((5,))],
            compiler_params=pltpu.CompilerParams(collective_id=0, has_side_effects=True, vmem_limit_bytes=8 * 2**20),
            name='exchange',
        )(kspace, wts_y, wts_x, idx_y.reshape(16, LANES), idx_x.reshape(16, LANES))
        y8, wy, wx, addr, roff = samples[:5]
        accs = pl.pallas_call(
            spread_kernel,
            out_shape=acc_shape,
            in_specs=[vmem] * (5 + 2 * N_COPY),
            out_specs=[vmem] * (2 * N_COPY),
            scratch_shapes=[pltpu.SMEM((2, 16, LANES), jnp.int32)] + [pltpu.VMEM((256, LANES), F32)] * 4 + [pltpu.SemaphoreType.DMA],
            input_output_aliases={5 + i: i for i in range(2 * N_COPY)},
            compiler_params=pltpu.CompilerParams(vmem_limit_bytes=8 * 2**20),
            name='spread',
        )(addr, y8, wy, wx, roff, *samples[5:])
        maps = jnp.transpose(coil_maps, (0, 3, 1, 2))
        return pl.pallas_call(
            transform_kernel,
            out_shape=sds((2, P_BLK, Q_BLK), F32),
            in_specs=[vmem] * (2 * N_COPY) + [hbm] * 4,
            out_specs=vmem,
            scratch_shapes=[pltpu.VMEM((KV, KV), BF16), pltpu.VMEM((KV, 2 * P_ALL), BF16), pltpu.VMEM((2, Q_BLK, 4, N_IMG), F32),
                            pltpu.VMEM((1, N_IMG), F32), pltpu.VMEM((Q_BLK, P_BLK), F32), pltpu.VMEM((KV, 256), BF16)] + [pltpu.VMEM((KV, LANES), F32)] * 3 + [
                pltpu.VMEM((96, LANES), F32),
                pltpu.VMEM((48, LANES), F32),
                pltpu.VMEM((N_CHUNK, 4, Q_PAD, 256), BF16),
                pltpu.VMEM((N_CHUNK, 4, Q_PAD, 256), BF16),
                pltpu.VMEM((96, LANES), F32),
                pltpu.VMEM((48, LANES), F32),
                pltpu.VMEM((N_CHUNK, 256, 2 * P_ALL), BF16),
                pltpu.VMEM((2, 4, Q_PAD, P_ALL), F32),
                pltpu.VMEM((4 * Q_PAD, 2 * P_ALL), F32),
                pltpu.VMEM((Q_PAD, P_ALL), F32),
                pltpu.VMEM((Q_PAD, P_ALL), F32),
                pltpu.SemaphoreType.DMA((N_CHUNK, 3)),
                pltpu.SemaphoreType.DMA((N_CHUNK, 4)),
                pltpu.SemaphoreType.DMA((2,)),
                pltpu.SemaphoreType.DMA((2,)),
                pltpu.SemaphoreType.DMA,
                pltpu.SemaphoreType.DMA,
                pltpu.SemaphoreType.DMA((4,)),
            ],
            compiler_params=pltpu.CompilerParams(collective_id=1, has_side_effects=True, vmem_limit_bytes=24 * 2**20),
            name='transform',
        )(*accs, e1, e2, maps, deapod.reshape(1, N_IMG))

    return jax.shard_map(
        local_fn,
        mesh=mesh,
        in_specs=(P(None, None, sample_spec), P(None, sample_spec), P(None, sample_spec), P(sample_spec), P(sample_spec), P(None, ('exam', 'cols'), None, 'rows'), P()),
        out_specs=P(None, ('exam', 'cols'), 'rows'),
        check_vma=False,
    )
```

```python
import functools
import math

import jax
import jax.numpy as jnp
import numpy as np
from jax import lax
from jax.experimental import pallas as pl
from jax.experimental.pallas import tpu as pltpu
from jax.sharding import PartitionSpec as P

F32, BF16 = jnp.float32, jnp.bfloat16
MESH = pl.DeviceIdType.MESH

N_IMG = 368
N_GRID = 736
ROW_BLK = 184
Q_BLK, Q_PAD = 92, 96
P_BLK, P_PAD, P_ALL = 184, 192, 384
N_CH = 8
TILE_U, STRIDE_U, N_SRC = 16, 13, 15
N_TGT = 12
COL_BLK = 368
VR = 384
VS = 392
KV = 2 * VR
LANES, ROWS = 128, 16
EDGE = 6
N_CHUNK = 6
N_COPY = 3
CHUNK_TILES = [(1 + 2 * j, 2 + 2 * j) for j in range(5)] + [(0, 11)]


def dft_constants():
    scale = 1.0 / math.sqrt(N_GRID)
    phase = ((np.arange(N_GRID)[:, None] - N_GRID // 2) * (np.arange(N_IMG)[None, :] - N_IMG // 2)) % N_GRID
    ang = phase.astype(np.float64) * (2.0 * math.pi / N_GRID)
    parts = (np.cos(ang) * scale, np.sin(ang) * scale)
    e1 = np.zeros((4, 2, Q_PAD, 2, VR))
    for dest in range(4):
        for cs in range(2):
            for half in range(2):
                    part = parts[cs][half * COL_BLK:(half + 1) * COL_BLK, dest * Q_BLK:(dest + 1) * Q_BLK]
                    e1[dest, cs, :Q_BLK, half, EDGE:EDGE + COL_BLK] = part.T
    e2 = np.zeros((N_CHUNK, 4, 2, TILE_U, 2, P_ALL))
    for j in range(N_CHUNK):
        for src in range(4):
            for tl in range(2):
                base = TILE_U * CHUNK_TILES[j][tl]
                rows = min(TILE_U, ROW_BLK - base)
                u0 = src * ROW_BLK + base
                for cs in range(2):
                    e2[j, src, tl, :rows, cs, :N_IMG] = parts[cs][u0:u0 + rows]
    return (jnp.asarray(e1.reshape(8 * Q_PAD, KV).astype(np.float32)).astype(BF16),
            jnp.asarray(e2.reshape(N_CHUNK * LANES, 2 * P_ALL).astype(np.float32)).astype(BF16))


def exchange_kernel(y_hbm, wy_hbm, wx_hbm, iy_hbm, ix_hbm, y_ref, wy_ref, wx_ref, addr_ref, roff_ref, *refs):
    accs = refs[:2 * N_COPY]
    y_in, iy, ix, y_send, in_sem, send_sem, recv_sem = refs[2 * N_COPY:]
    k = lax.axis_index('cols')
    r = lax.axis_index('rows')
    other = {'cols': 1 - k}
    barrier = pltpu.get_barrier_semaphore()
    pl.semaphore_signal(barrier, inc=1, device_id=other, device_id_type=MESH)
    loads = [(iy_hbm, iy), (ix_hbm, ix), (y_hbm, y_in), (wy_hbm, wy_ref.at[0]), (wx_hbm, wx_ref.at[0])]
    loads = [pltpu.make_async_copy(a, b, in_sem.at[i]) for i, (a, b) in enumerate(loads)]
    for c in loads:
        c.start()

    def send(i, src, dst):
        c = pltpu.make_async_remote_copy(src_ref=src, dst_ref=dst, send_sem=send_sem.at[i], recv_sem=recv_sem.at[i],
                                         device_id=other, device_id_type=MESH)
        c.start()
        return c

    loads[0].wait()
    loads[1].wait()
    row = iy[...] - r * ROW_BLK
    tile = jnp.zeros_like(row)
    for t in range(1, N_SRC):
        tile = tile + jnp.where(row >= STRIDE_U * t, 1, 0)
    addr_ref[0] = tile * VS + (ix[...] - k * COL_BLK)
    roff_ref[0] = (row + 14) & 15
    loads[2].wait()
    y_re, y_im = y_in[0], y_in[1]
    low = jnp.concatenate([y_re[0:4], y_im[0:4]], axis=0)
    high = jnp.concatenate([y_re[4:8], y_im[4:8]], axis=0)
    y_ref[0] = jnp.where(k == 0, low, high)
    y_send[...] = jnp.where(k == 0, high, low)
    loads[3].wait()
    loads[4].wait()
    pl.semaphore_wait(barrier, 1)
    copies = [send(0, wy_ref.at[0], wy_ref.at[1]), send(1, wx_ref.at[0], wx_ref.at[1]), send(2, addr_ref.at[0], addr_ref.at[1]),
              send(3, roff_ref.at[0], roff_ref.at[1]), send(4, y_send, y_ref.at[1])]

    def zero(i, _):
        for a in accs:
            a[pl.ds(pl.multiple_of(i * VS, 8), VS), :] = jnp.zeros((VS, LANES), F32)
        return 0
    lax.fori_loop(0, N_SRC, zero, 0)
    for c in copies:
        c.wait()


def split3(x):
    hi = x.astype(BF16).astype(F32)
    rest = x - hi
    mid = rest.astype(BF16).astype(F32)
    return [hi, mid, rest - mid]


def spread_kernel(addr_ref, y_ref, wy_ref, wx_ref, roff_ref, *refs):
    accs = refs[2 * N_COPY:4 * N_COPY]
    addr, sem = refs[4 * N_COPY], refs[-1]
    q_refs = refs[4 * N_COPY + 1:-1]
    to_smem = pltpu.make_async_copy(addr_ref, addr, sem)
    to_smem.start()
    n = y_ref.shape[2]

    r0 = lax.broadcasted_iota(jnp.int32, (80, 256), 0)
    l0 = lax.broadcasted_iota(jnp.int32, (80, 256), 1)
    ry = (r0 < 24) & (l0 < LANES) & ((r0 & 7) == (l0 >> 4))
    rw = (r0 >= 24) & (r0 < 72) & (l0 >= LANES) & (((r0 - 24) & 15) == (l0 & 15))
    expand = jnp.where(ry | rw, 1.0, 0.0).astype(BF16)
    rr = lax.broadcasted_iota(jnp.int32, (ROWS, 256), 0)
    n_blk = n // 256

    def prep(i, slot, q_ref):
        ds = [pl.ds(pl.multiple_of((i + n_blk * h) * LANES, LANES), LANES) for h in range(2)]
        y = jnp.concatenate([y_ref[slot, :, s] for s in ds], axis=1)
        wy = jnp.concatenate([wy_ref[slot, :, s] for s in ds], axis=1)
        d = (rr - jnp.concatenate([roff_ref[slot, pl.ds(i + n_blk * h, 1), :] for h in range(2)], axis=1)) & 15
        w16 = jnp.zeros((ROWS, 256), F32)
        for a in range(4):
            w16 = jnp.where(d == a, wy[a:a + 1], w16)
        lhs = jnp.concatenate(split3(y) + split3(w16) + [jnp.zeros((8, 256), F32)], axis=0).astype(BF16)
        o = lax.dot_general(lhs, expand, (((0,), (0,)), ((), ())), preferred_element_type=F32)
        q_ref[...] = o[:, :LANES] * o[:, LANES:]

    top = lax.broadcasted_iota(jnp.int32, (8, LANES), 0) < 4

    def scatter(i, qs):
        ds = [pl.ds(pl.multiple_of((i + n_blk * h) * LANES, LANES), LANES) for h in range(2)]
        wx = [jnp.concatenate([wx_ref[slot, :, s] for s in ds], axis=0) for slot in range(2)]
        for j in range(LANES):
            cols = [jnp.broadcast_to(wx[slot][:, j:j + 1], (8, LANES)) for slot in range(2)]
            for h in range(2):
                for slot in range(2):
                    acc = accs[slot * N_COPY + (2 * j + h) % N_COPY]
                    base = addr[slot, i + n_blk * h, j] + (0 if h else 4)
                    q = jnp.broadcast_to(qs[slot][j + LANES * h:j + LANES * h + 1, :], (8, LANES))
                    s = pl.ds(base, 8)
                    c = jnp.where(top, 0.0, cols[slot]) if h else jnp.where(top, cols[slot], 0.0)
                    acc[s, :] = acc[s, :] + c * q

    qa, qb = q_refs[:2], q_refs[2:]
    for slot in range(2):
        prep(0, slot, qa[slot])
    to_smem.wait()

    def two_blocks(i, _):
        for step, now, then in ((0, qa, qb), (1, qb, qa)):
            for slot in range(2):
                prep(lax.rem(2 * i + step + 1, n_blk), slot, then[slot])
            scatter(2 * i + step, now)
        return 0
    lax.fori_loop(0, n_blk // 2, two_blocks, 0)


def transform_kernel(*refs):
    own, nbr = refs[:N_COPY], refs[N_COPY:2 * N_COPY]
    (e1_hbm, e2_hbm, s_hbm, d_hbm, out_ref, e1_ref, e2_ref, s_ref, d_ref, dd, gch, raw0, f0, f11, gps, gns, msg, recv, gpr, gnr, e2f, st, img, psend, precv,
     msend_sem, mrecv_sem, gsend_sem, grecv_sem, psend_sem, precv_sem, in_sem) = refs[2 * N_COPY:]
    k = lax.axis_index('cols')
    r = lax.axis_index('rows')
    chip, core = r // 2, r % 2
    dests = [2 * (1 - chip) + core, 2 * (1 - chip) + (1 - core), 2 * chip + (1 - core)]
    nxt, prv = lax.rem(r + 1, 4), lax.rem(r + 3, 4)
    barrier = pltpu.get_barrier_semaphore()
    for d in dests:
        pl.semaphore_signal(barrier, inc=1, device_id={'rows': d}, device_id_type=MESH)
    pl.semaphore_signal(barrier, inc=1, device_id={'cols': 1 - k}, device_id_type=MESH)

    loads = [pltpu.make_async_copy(a, b, in_sem.at[i]) for i, (a, b) in
             enumerate(((e1_hbm, e1_ref), (e2_hbm, e2_ref), (s_hbm, s_ref), (d_hbm, d_ref)))]
    for c in loads:
        c.start()
    slots = ((own, k), (nbr, 1 - k))
    lane16 = lax.broadcasted_iota(jnp.int32, (ROWS, LANES), 1) & 15
    sub16 = lax.broadcasted_iota(jnp.int32, (ROWS, LANES), 0)

    def merged(accs, off, targets):
        wanted = {}
        for m in targets:
            deltas = {0: 0} if m is None else {t: STRIDE_U * t - TILE_U * m - 2 for t in range(N_SRC)}
            wanted[m] = {t: d for t, d in deltas.items() if abs(d) < ROWS}
        loaded = {}
        for t in sorted({t for w in wanted.values() for t in w}):
            s = pl.ds(t * VS + off, ROWS)
            v = accs[0][s, :]
            for acc in accs[1:]:
                v = v + acc[s, :]
            loaded[t] = v
        outs = []
        for m in targets:
            out = None
            for t, d in wanted[m].items():
                lo, hi = max(0, d), min(15, 15 + d)
                v = loaded[t]
                if lo > 0 or hi < 15:
                    v = jnp.where((lane16 >= lo) & (lane16 <= hi), v, 0.0)
                out = v if out is None else out + v
            outs.append(out)
        return outs

    def merge_all(targets, put):
        def rows(i, _):
            for step in range(2):
                for accs, half in slots:
                    off = pl.multiple_of((2 * i + 1 + step) * ROWS, ROWS)
                    put(pl.multiple_of(half * VR + off, ROWS), merged(accs, off, targets))
            return 0
        lax.fori_loop(0, VR // (2 * ROWS) - 1, rows, 0)
        last = VR - ROWS
        a = [merged(accs, 0, targets) for accs, _ in slots]
        b = [merged(accs, last, targets) for accs, _ in slots]
        for i, (_, half) in enumerate(slots):
            fix_a = [x + jnp.where(sub16 == 6, y, 0.0) for x, y in zip(a[i], b[1 - i])]
            fix_b = [y + jnp.where((sub16 == 4) | (sub16 == 5), x, 0.0) for x, y in zip(a[1 - i], b[i])]
            put(pl.multiple_of(half * VR, ROWS), fix_a)
            put(pl.multiple_of(half * VR + last, ROWS), fix_b)

    def put_chunk(off, vals):
        for i, v in enumerate(vals):
            gch[pl.ds(off, ROWS), LANES * i:LANES * (i + 1)] = v.astype(BF16)

    def put_edges(off, vals):
        for ref, v in zip((raw0, f0, f11), vals):
            ref[pl.ds(off, ROWS), :] = v

    lane = lax.broadcasted_iota(jnp.int32, (Q_PAD, 256), 1) & 127

    def first_dft(j, g):
        ab = jnp.dot(e1_ref[...], g, preferred_element_type=F32)
        for d in range(4):
            a = ab[192 * d:192 * d + 96]
            b = ab[192 * d + 96:192 * d + 192]
            b = jnp.concatenate([pltpu.roll(b[:, :128], 64, 1), pltpu.roll(b[:, 128:], 64, 1)], axis=1)
            msg[j, d] = jnp.where(lane < 64, a - b, a + b).astype(BF16)

    def message(j, i):
        d = dests[i]
        return pltpu.make_async_remote_copy(src_ref=msg.at[j, d], dst_ref=recv.at[j, r], send_sem=msend_sem.at[j, i],
                                            recv_sem=mrecv_sem.at[j, r], device_id={'rows': d}, device_id_type=MESH)

    def arrival(j, i):
        d = dests[i]
        return pltpu.make_async_remote_copy(src_ref=msg.at[j, d], dst_ref=recv.at[j, d], send_sem=msend_sem.at[j, i],
                                            recv_sem=mrecv_sem.at[j, d], device_id={'rows': d}, device_id_type=MESH)

    def post(j):
        for i in range(3):
            message(j, i).start()
        recv[j, r] = msg[j, r]

    merge_all(CHUNK_TILES[0], put_chunk)
    loads[0].wait()
    first_dft(0, gch[...])
    pl.semaphore_wait(barrier, 4)
    post(0)

    merge_all((None, 0, N_TGT - 1), put_edges)
    la = lax.broadcasted_iota(jnp.int32, (96, LANES), 1) & 15
    lb = lax.broadcasted_iota(jnp.int32, (48, LANES), 1) & 15

    def shifted(v, by):
        return pltpu.roll(v, by % LANES, 1) if by else v

    gp = jnp.zeros((96, LANES), F32)
    for c in range(8):
        gp = jnp.where((la >> 1) == c, shifted(raw0[96 * c:96 * c + 96, :], 2 * c - 14), gp)
    gps[...] = gp
    gn = jnp.zeros((48, LANES), F32)
    for c in range(16):
        gn = jnp.where(lb == c, shifted(f11[48 * c:48 * c + 48, :], c - 8), gn)
    gns[...] = gn
    to_prv = pltpu.make_async_remote_copy(src_ref=gps, dst_ref=gpr, send_sem=gsend_sem.at[0], recv_sem=grecv_sem.at[0],
                                          device_id={'rows': prv}, device_id_type=MESH)
    to_nxt = pltpu.make_async_remote_copy(src_ref=gns, dst_ref=gnr, send_sem=gsend_sem.at[1], recv_sem=grecv_sem.at[1],
                                          device_id={'rows': nxt}, device_id_type=MESH)
    to_prv.start()
    to_nxt.start()

    for j in range(1, N_CHUNK - 1):
        merge_all(CHUNK_TILES[j], put_chunk)
        first_dft(j, gch[...])
        post(j)

    to_prv.wait()
    to_nxt.wait()
    gp, gn = gpr[...], gnr[...]
    for c in range(8):
        s = slice(96 * c, 96 * c + 96)
        gch[s, LANES:2 * LANES] = (f11[s, :] + jnp.where((la >> 1) == 3, shifted(gp, 6 - 2 * c), 0.0)).astype(BF16)
    for c in range(16):
        s = slice(48 * c, 48 * c + 48)
        gch[s, 0:LANES] = (f0[s, :] + jnp.where(lb == 0, shifted(gn, -c), 0.0)).astype(BF16)
    first_dft(N_CHUNK - 1, gch[...])
    post(N_CHUNK - 1)

    for c in loads[1:]:
        c.wait()
    for j in range(N_CHUNK):
        for h in range(2):
            v = e2_ref[LANES * j + 64 * h:LANES * j + 64 * h + 64, :]
            e2f[j, LANES * h:LANES * h + 64, :] = v
            e2f[j, LANES * h + 64:LANES * h + LANES, 0:P_ALL] = -v[:, P_ALL:2 * P_ALL]
            e2f[j, LANES * h + 64:LANES * h + LANES, P_ALL:2 * P_ALL] = v[:, 0:P_ALL]
    st[...] = jnp.zeros_like(st)
    for s in range(2):
        for c in range(4):
            st[s, c, 0:Q_BLK, 0:N_IMG] = s_ref[s, :, c, :]

    half_p = jnp.where(k == 0, d_ref[:, 0:P_BLK], d_ref[:, P_BLK:2 * P_BLK])
    part_q = d_ref[:, 0:Q_BLK]
    for i in range(1, 4):
        part_q = jnp.where(r == i, d_ref[:, Q_BLK * i:Q_BLK * (i + 1)], part_q)
    part_q = jnp.concatenate([part_q, jnp.zeros((1, LANES - Q_BLK), F32)], axis=1)
    dd[...] = jnp.broadcast_to(part_q, (8, LANES)).T[0:Q_BLK, 0:1] * half_p

    coil = (lax.broadcasted_iota(jnp.int32, (Q_PAD, LANES), 1) >> 4) & 3

    def regroup(j, pair):
        v = [recv[j, 2 * pair + s // 2, :, LANES * (s % 2):LANES * (s % 2 + 1)] for s in range(4)]
        for bit in (1, 2):
            m = (coil & bit) == 0
            for s in range(4):
                if s & bit:
                    continue
                x, y = v[s], v[s | bit]
                v[s] = jnp.where(m, x, pltpu.roll(y, ROWS * bit, 1))
                v[s | bit] = jnp.where(m, pltpu.roll(x, LANES - ROWS * bit, 1), y)
        return v

    def second_dft(j):
        for i in range(3):
            arrival(j, i).wait_recv()
        first, second = regroup(j, 0), regroup(j, 1)
        lhs = jnp.concatenate([jnp.concatenate([first[c], second[c]], axis=1) for c in range(4)], axis=0)
        return jnp.dot(lhs, e2f[j], preferred_element_type=F32)

    img[...] = second_dft(0)

    def accumulate(j, _):
        img[...] += second_dft(j)
        return 0
    lax.fori_loop(1, N_CHUNK, accumulate, 0)

    x_re = jnp.zeros((Q_PAD, P_ALL), F32)
    x_im = jnp.zeros((Q_PAD, P_ALL), F32)
    for c in range(4):
        i_re = img[96 * c:96 * c + 96, 0:P_ALL]
        i_im = img[96 * c:96 * c + 96, P_ALL:2 * P_ALL]
        x_re = x_re + st[0, c] * i_re + st[1, c] * i_im
        x_im = x_im + st[0, c] * i_im - st[1, c] * i_re
    lo = jnp.concatenate([x_re[:, 0:P_PAD], x_im[:, 0:P_PAD]], axis=1)
    hi = jnp.concatenate([x_re[:, P_BLK:P_BLK + P_PAD], x_im[:, P_BLK:P_BLK + P_PAD]], axis=1)
    first = k == 0
    psend[...] = jnp.where(first, hi, lo)
    swap = pltpu.make_async_remote_copy(src_ref=psend, dst_ref=precv, send_sem=psend_sem, recv_sem=precv_sem,
                                        device_id={'cols': 1 - k}, device_id_type=MESH)
    swap.start()
    mine = jnp.where(first, lo, hi)
    for j in range(N_CHUNK):
        for i in range(3):
            message(j, i).wait_send()
    swap.wait()
    total = mine + precv[...]
    out_ref[0] = (total[0:Q_BLK, 0:P_BLK] * dd[...]).T
    out_ref[1] = (total[0:Q_BLK, P_PAD:P_PAD + P_BLK] * dd[...]).T


def solution(mesh):
    sample_spec = ('exam', 'rows', 'cols')
    vmem = pl.BlockSpec(memory_space=pltpu.VMEM)
    hbm = pl.BlockSpec(memory_space=pltpu.HBM)
    sds = jax.ShapeDtypeStruct

    def local_fn(kspace, wts_y, wts_x, idx_y, idx_x, coil_maps, deapod):
        n = kspace.shape[2]
        e1, e2 = dft_constants()
        acc_shape = [sds((N_SRC * VS, LANES), F32)] * (2 * N_COPY)
        *samples, = pl.pallas_call(
            exchange_kernel,
            out_shape=[sds((2, 8, n), F32), sds((2, 4, n), F32), sds((2, 4, n), F32), sds((2, 16, LANES), jnp.int32),
                       sds((2, 16, LANES), jnp.int32)] + acc_shape,
            in_specs=[hbm] * 5,
            out_specs=[vmem] * (5 + 2 * N_COPY),
            scratch_shapes=[pltpu.VMEM((2, 8, n), F32), pltpu.VMEM((16, LANES), jnp.int32), pltpu.VMEM((16, LANES), jnp.int32),
                            pltpu.VMEM((8, n), F32), pltpu.SemaphoreType.DMA((5,)), pltpu.SemaphoreType.DMA((5,)),
                            pltpu.SemaphoreType.DMA((5,))],
            compiler_params=pltpu.CompilerParams(collective_id=0, has_side_effects=True, vmem_limit_bytes=8 * 2**20),
            name='exchange',
        )(kspace, wts_y, wts_x, idx_y.reshape(16, LANES), idx_x.reshape(16, LANES))
        y8, wy, wx, addr, roff = samples[:5]
        accs = pl.pallas_call(
            spread_kernel,
            out_shape=acc_shape,
            in_specs=[vmem] * (5 + 2 * N_COPY),
            out_specs=[vmem] * (2 * N_COPY),
            scratch_shapes=[pltpu.SMEM((2, 16, LANES), jnp.int32)] + [pltpu.VMEM((256, LANES), F32)] * 4 + [pltpu.SemaphoreType.DMA],
            input_output_aliases={5 + i: i for i in range(2 * N_COPY)},
            compiler_params=pltpu.CompilerParams(vmem_limit_bytes=8 * 2**20),
            name='spread',
        )(addr, y8, wy, wx, roff, *samples[5:])
        maps = jnp.transpose(coil_maps, (0, 3, 1, 2))
        return pl.pallas_call(
            transform_kernel,
            out_shape=sds((2, P_BLK, Q_BLK), F32),
            in_specs=[vmem] * (2 * N_COPY) + [hbm] * 4,
            out_specs=vmem,
            scratch_shapes=[pltpu.VMEM((KV, KV), BF16), pltpu.VMEM((KV, 2 * P_ALL), BF16), pltpu.VMEM((2, Q_BLK, 4, N_IMG), F32),
                            pltpu.VMEM((1, N_IMG), F32), pltpu.VMEM((Q_BLK, P_BLK), F32), pltpu.VMEM((KV, 256), BF16)] + [pltpu.VMEM((KV, LANES), F32)] * 3 + [
                pltpu.VMEM((96, LANES), F32),
                pltpu.VMEM((48, LANES), F32),
                pltpu.VMEM((N_CHUNK, 4, Q_PAD, 256), BF16),
                pltpu.VMEM((N_CHUNK, 4, Q_PAD, 256), BF16),
                pltpu.VMEM((96, LANES), F32),
                pltpu.VMEM((48, LANES), F32),
                pltpu.VMEM((N_CHUNK, 256, 2 * P_ALL), BF16),
                pltpu.VMEM((2, 4, Q_PAD, P_ALL), F32),
                pltpu.VMEM((4 * Q_PAD, 2 * P_ALL), F32),
                pltpu.VMEM((Q_PAD, P_ALL), F32),
                pltpu.VMEM((Q_PAD, P_ALL), F32),
                pltpu.SemaphoreType.DMA((N_CHUNK, 3)),
                pltpu.SemaphoreType.DMA((N_CHUNK, 4)),
                pltpu.SemaphoreType.DMA((2,)),
                pltpu.SemaphoreType.DMA((2,)),
                pltpu.SemaphoreType.DMA,
                pltpu.SemaphoreType.DMA,
                pltpu.SemaphoreType.DMA((4,)),
            ],
            compiler_params=pltpu.CompilerParams(collective_id=1, has_side_effects=True, vmem_limit_bytes=24 * 2**20),
            name='transform',
        )(*accs, e1, e2, maps, deapod.reshape(1, N_IMG))

    return jax.shard_map(
        local_fn,
        mesh=mesh,
        in_specs=(P(None, None, sample_spec), P(None, sample_spec), P(None, sample_spec), P(sample_spec), P(sample_spec), P(None, ('exam', 'cols'), None, 'rows'), P()),
        out_specs=P(None, ('exam', 'cols'), 'rows'),
        check_vma=False,
    )
```

```python
import math

import jax
import jax.numpy as jnp
import numpy as np
from jax import lax
from jax.experimental import pallas as pl
from jax.experimental.pallas import tpu as pltpu
from jax.sharding import PartitionSpec as P

F32, BF16 = jnp.float32, jnp.bfloat16
MESH = pl.DeviceIdType.MESH

N_IMG = 368
N_GRID = 736
ROW_BLK = 184
Q_BLK, Q_PAD = 92, 96
P_BLK, P_PAD, P_ALL = 184, 192, 384
N_CH = 8
TILE_U, STRIDE_U, N_SRC = 16, 13, 15
N_TGT = 12
COL_BLK = 368
VR = 384
VS = 392
KV = 2 * VR
LANES, ROWS = 128, 16
EDGE = 6
WIDE, P_TWO, GN_ROWS, MIB = 2 * LANES, 2 * P_ALL, 48, 2**20
N_CHUNK = 6
N_COPY = 3
N_ACC = 2 * N_COPY
SUBS = [(0, 48), (48, 32), (80, 16)]
POSTS = [[(j, s) for s in range(3)] for j in range(2)] + [[(j, 0)] for j in range(2, N_CHUNK)]
POSTS[-1] += [(j, s) for s in (1, 2) for j in range(2, N_CHUNK)]
CHUNK_TILES = [(1 + 2 * j, 2 + 2 * j) for j in range(5)] + [(0, 11)]


def dft_constants():
    scale = 1.0 / math.sqrt(N_GRID)
    phase = ((np.arange(N_GRID)[:, None] - N_GRID // 2) * (np.arange(N_IMG)[None, :] - N_IMG // 2)) % N_GRID
    ang = phase.astype(np.float64) * (2.0 * math.pi / N_GRID)
    parts = (np.cos(ang) * scale, np.sin(ang) * scale)
    e1 = np.zeros((4, 2, Q_PAD, 2, VR))
    for dest in range(4):
        for cs in range(2):
            for half in range(2):
                part = parts[cs][half * COL_BLK:(half + 1) * COL_BLK, dest * Q_BLK:(dest + 1) * Q_BLK]
                e1[dest, cs, :Q_BLK, half, EDGE:EDGE + COL_BLK] = part.T
    e2 = np.zeros((N_CHUNK, 4, 2, TILE_U, 2, P_ALL))
    for j in range(N_CHUNK):
        for src in range(4):
            for tl in range(2):
                base = TILE_U * CHUNK_TILES[j][tl]
                rows = min(TILE_U, ROW_BLK - base)
                u0 = src * ROW_BLK + base
                for cs in range(2):
                    e2[j, src, tl, :rows, cs, :N_IMG] = parts[cs][u0:u0 + rows]
    return (jnp.asarray(e1.reshape(8 * Q_PAD, KV).astype(np.float32)).astype(BF16),
            jnp.asarray(e2.reshape(N_CHUNK * LANES, P_TWO).astype(np.float32)).astype(BF16))


def zero_kernel(*refs):
    *accs, token = refs

    def zero(i, _):
        for a in accs:
            a[pl.ds(pl.multiple_of(i * VS, 8), VS), :] = jnp.zeros((VS, LANES), F32)
        return 0
    lax.fori_loop(0, N_SRC, zero, 0)
    token[...] = jnp.zeros_like(token)


def exchange_kernel(_, y_hbm, wy_hbm, wx_hbm, iy_hbm, ix_hbm, y_ref, wy_ref, wx_ref, addr_ref, roff_ref, *refs):
    y_in, iy, ix, y_send, in_sem, send_sem, recv_sem = refs
    k = lax.axis_index('cols')
    r = lax.axis_index('rows')
    other = {'cols': 1 - k}
    barrier = pltpu.get_barrier_semaphore()
    pl.semaphore_signal(barrier, inc=1, device_id=other, device_id_type=MESH)
    loads = [(iy_hbm, iy), (ix_hbm, ix), (y_hbm, y_in), (wy_hbm, wy_ref.at[0]), (wx_hbm, wx_ref.at[0])]
    loads = [pltpu.make_async_copy(a, b, in_sem.at[i]) for i, (a, b) in enumerate(loads)]
    for c in loads:
        c.start()

    def send(i, src, dst):
        c = pltpu.make_async_remote_copy(src_ref=src, dst_ref=dst, send_sem=send_sem.at[i], recv_sem=recv_sem.at[i],
                                         device_id=other, device_id_type=MESH)
        c.start()
        return c

    loads[0].wait()
    loads[1].wait()
    row = iy[...] - r * ROW_BLK
    tile = jnp.zeros_like(row)
    for t in range(1, N_SRC):
        tile = tile + jnp.where(row >= STRIDE_U * t, 1, 0)
    addr_ref[0] = tile * VS + (ix[...] - k * COL_BLK)
    roff_ref[0] = (row + 14) & 15
    loads[2].wait()
    y_re, y_im = y_in[0], y_in[1]
    low = jnp.concatenate([y_re[0:4], y_im[0:4]], axis=0)
    high = jnp.concatenate([y_re[4:8], y_im[4:8]], axis=0)
    y_ref[0] = jnp.where(k == 0, low, high)
    y_send[...] = jnp.where(k == 0, high, low)
    loads[3].wait()
    loads[4].wait()
    pl.semaphore_wait(barrier, 1)
    copies = [send(0, wy_ref.at[0], wy_ref.at[1]), send(1, wx_ref.at[0], wx_ref.at[1]), send(2, addr_ref.at[0], addr_ref.at[1]),
              send(3, roff_ref.at[0], roff_ref.at[1]), send(4, y_send, y_ref.at[1])]

    for c in copies:
        c.wait()


def split3(x):
    hi = x.astype(BF16).astype(F32)
    rest = x - hi
    mid = rest.astype(BF16).astype(F32)
    return [hi, mid, rest - mid]


def spread_kernel(addr_ref, y_ref, wy_ref, wx_ref, roff_ref, *refs):
    accs = refs[N_ACC:4 * N_COPY]
    addr, sem = refs[4 * N_COPY], refs[-1]
    q_refs = refs[4 * N_COPY + 1:-1]
    to_smem = pltpu.make_async_copy(addr_ref, addr, sem)
    to_smem.start()
    n = y_ref.shape[2]

    r0 = lax.broadcasted_iota(jnp.int32, (80, WIDE), 0)
    l0 = lax.broadcasted_iota(jnp.int32, (80, WIDE), 1)
    ry = (r0 < 24) & (l0 < LANES) & ((r0 & 7) == (l0 >> 4))
    rw = (r0 >= 24) & (r0 < 72) & (l0 >= LANES) & (((r0 - 24) & 15) == (l0 & 15))
    expand = jnp.where(ry | rw, 1.0, 0.0).astype(BF16)
    rr = lax.broadcasted_iota(jnp.int32, (ROWS, WIDE), 0)
    n_blk = n // WIDE

    def prep(i, slot, q_ref):
        ds = [pl.ds(pl.multiple_of((i + n_blk * h) * LANES, LANES), LANES) for h in range(2)]
        y = jnp.concatenate([y_ref[slot, :, s] for s in ds], axis=1)
        wy = jnp.concatenate([wy_ref[slot, :, s] for s in ds], axis=1)
        d = (rr - jnp.concatenate([roff_ref[slot, pl.ds(i + n_blk * h, 1), :] for h in range(2)], axis=1)) & 15
        w16 = jnp.zeros((ROWS, WIDE), F32)
        for a in range(4):
            w16 = jnp.where(d == a, wy[a:a + 1], w16)
        lhs = jnp.concatenate(split3(y) + split3(w16) + [jnp.zeros((8, WIDE), F32)], axis=0).astype(BF16)
        o = lax.dot_general(lhs, expand, (((0,), (0,)), ((), ())), preferred_element_type=F32)
        q_ref[...] = o[:, :LANES] * o[:, LANES:]

    top = lax.broadcasted_iota(jnp.int32, (8, LANES), 0) < 4

    def scatter(i, qs):
        ds = [pl.ds(pl.multiple_of((i + n_blk * h) * LANES, LANES), LANES) for h in range(2)]
        wx = [jnp.concatenate([wx_ref[slot, :, s] for s in ds], axis=0) for slot in range(2)]
        for j in range(LANES):
            cols = [jnp.broadcast_to(wx[slot][:, j:j + 1], (8, LANES)) for slot in range(2)]
            for h in range(2):
                for slot in range(2):
                    acc = accs[slot * N_COPY + (2 * j + h) % N_COPY]
                    base = addr[slot, i + n_blk * h, j] + (0 if h else 4)
                    q = jnp.broadcast_to(qs[slot][j + LANES * h:j + LANES * h + 1, :], (8, LANES))
                    s = pl.ds(base, 8)
                    c = jnp.where(top, 0.0, cols[slot]) if h else jnp.where(top, cols[slot], 0.0)
                    acc[s, :] = acc[s, :] + c * q

    qa, qb = q_refs[:2], q_refs[2:]
    for slot in range(2):
        prep(0, slot, qa[slot])
    to_smem.wait()

    def two_blocks(i, _):
        for step, now, then in ((0, qa, qb), (1, qb, qa)):
            for slot in range(2):
                prep(lax.rem(2 * i + step + 1, n_blk), slot, then[slot])
            scatter(2 * i + step, now)
        return 0
    lax.fori_loop(0, n_blk // 2, two_blocks, 0)


def transform_kernel(*refs):
    own, nbr = refs[:N_COPY], refs[N_COPY:N_ACC]
    (e1_hbm, e2_hbm, s_hbm, d_hbm, out_ref, e1_ref, e2_ref, s_ref, d_ref, dd, gch, raw0, f0, f11, gps, gns, msg, recv, gpr, gnr, e2f, st, img, mine, psend, precv,
     msend_sem, mrecv_sem, gsend_sem, grecv_sem, psend_sem, precv_sem, in_sem) = refs[N_ACC:]
    k = lax.axis_index('cols')
    r = lax.axis_index('rows')
    chip, core = r // 2, r % 2
    dests = [2 * (1 - chip) + core, 2 * (1 - chip) + (1 - core), 2 * chip + (1 - core)]
    nxt, prv = lax.rem(r + 1, 4), lax.rem(r + 3, 4)
    barrier = pltpu.get_barrier_semaphore()
    for d in dests:
        pl.semaphore_signal(barrier, inc=1, device_id={'rows': d}, device_id_type=MESH)
    pl.semaphore_signal(barrier, inc=1, device_id={'cols': 1 - k}, device_id_type=MESH)

    loads = [pltpu.make_async_copy(a, b, in_sem.at[i]) for i, (a, b) in
             enumerate(((e1_hbm, e1_ref), (e2_hbm, e2_ref), (s_hbm, s_ref), (d_hbm, d_ref)))]
    for c in loads:
        c.start()
    slots = ((own, k), (nbr, 1 - k))
    lane16 = lax.broadcasted_iota(jnp.int32, (ROWS, LANES), 1) & 15
    sub16 = lax.broadcasted_iota(jnp.int32, (ROWS, LANES), 0)

    def merged(accs, off, targets):
        wanted = {}
        for m in targets:
            deltas = {0: 0} if m is None else {t: STRIDE_U * t - TILE_U * m - 2 for t in range(N_SRC)}
            wanted[m] = {t: d for t, d in deltas.items() if abs(d) < ROWS}
        loaded = {}
        for t in sorted({t for w in wanted.values() for t in w}):
            s = pl.ds(t * VS + off, ROWS)
            v = accs[0][s, :]
            for acc in accs[1:]:
                v = v + acc[s, :]
            loaded[t] = v
        outs = []
        for m in targets:
            out = None
            for t, d in wanted[m].items():
                lo, hi = max(0, d), min(15, 15 + d)
                v = loaded[t]
                if lo > 0 or hi < 15:
                    v = jnp.where((lane16 >= lo) & (lane16 <= hi), v, 0.0)
                out = v if out is None else out + v
            outs.append(out)
        return outs

    def merge_all(targets, put):
        def rows(i, _):
            for step in range(2):
                for accs, half in slots:
                    off = pl.multiple_of((2 * i + 1 + step) * ROWS, ROWS)
                    put(pl.multiple_of(half * VR + off, ROWS), merged(accs, off, targets))
            return 0
        lax.fori_loop(0, VR // (2 * ROWS) - 1, rows, 0)
        last = VR - ROWS
        a = [merged(accs, 0, targets) for accs, _ in slots]
        b = [merged(accs, last, targets) for accs, _ in slots]
        for i, (_, half) in enumerate(slots):
            fix_a = [x + jnp.where(sub16 == 6, y, 0.0) for x, y in zip(a[i], b[1 - i])]
            fix_b = [y + jnp.where((sub16 == 4) | (sub16 == 5), x, 0.0) for x, y in zip(a[1 - i], b[i])]
            put(pl.multiple_of(half * VR, ROWS), fix_a)
            put(pl.multiple_of(half * VR + last, ROWS), fix_b)

    def put_chunk(off, vals):
        for i, v in enumerate(vals):
            gch[pl.ds(off, ROWS), LANES * i:LANES * (i + 1)] = v.astype(BF16)

    def put_edges(off, vals):
        for ref, v in zip((raw0, f0, f11), vals):
            ref[pl.ds(off, ROWS), :] = v

    lane = lax.broadcasted_iota(jnp.int32, (Q_PAD, WIDE), 1) & 127

    def swap(sub):
        rows = pl.ds(*SUBS[sub])
        return pltpu.make_async_remote_copy(src_ref=psend.at[rows], dst_ref=precv.at[rows], send_sem=psend_sem.at[sub],
                                            recv_sem=precv_sem.at[sub], device_id={'cols': 1 - k}, device_id_type=MESH)

    def first_dft(j, g):
        ab = jnp.dot(e1_ref[...], g, preferred_element_type=F32)
        for d in range(4):
            a = ab[192 * d:192 * d + Q_PAD]
            b = ab[192 * d + Q_PAD:192 * d + 192]
            b = jnp.concatenate([pltpu.roll(b[:, :128], 64, 1), pltpu.roll(b[:, 128:], 64, 1)], axis=1)
            msg[j, d] = jnp.where(lane < 64, a - b, a + b).astype(BF16)

    def copy_of(j, sub, i, slot):
        d = dests[i]
        rows = pl.ds(*SUBS[sub])
        return pltpu.make_async_remote_copy(src_ref=msg.at[j, d, rows], dst_ref=recv.at[j, slot, rows], send_sem=msend_sem.at[j, sub, i],
                                            recv_sem=mrecv_sem.at[j, sub, slot], device_id={'rows': d}, device_id_type=MESH)

    def post(chunk):
        for j, sub in POSTS[chunk]:
            for i in range(3):
                copy_of(j, sub, i, r).start()
        recv[chunk, r] = msg[chunk, r]

    merge_all(CHUNK_TILES[0], put_chunk)
    loads[0].wait()
    first_dft(0, gch[...])
    pl.semaphore_wait(barrier, 4)
    post(0)

    merge_all((None, 0, N_TGT - 1), put_edges)
    la = lax.broadcasted_iota(jnp.int32, (Q_PAD, LANES), 1) & 15
    lb = lax.broadcasted_iota(jnp.int32, (GN_ROWS, LANES), 1) & 15

    def shifted(v, by):
        return pltpu.roll(v, by % LANES, 1) if by else v

    gp = jnp.zeros((Q_PAD, LANES), F32)
    for c in range(8):
        gp = jnp.where((la >> 1) == c, shifted(raw0[Q_PAD * c:Q_PAD * c + Q_PAD, :], 2 * c - 14), gp)
    gps[...] = gp
    gn = jnp.zeros((GN_ROWS, LANES), F32)
    for c in range(16):
        gn = jnp.where(lb == c, shifted(f11[GN_ROWS * c:GN_ROWS * c + GN_ROWS, :], c - 8), gn)
    gns[...] = gn
    to_prv = pltpu.make_async_remote_copy(src_ref=gps, dst_ref=gpr, send_sem=gsend_sem.at[0], recv_sem=grecv_sem.at[0],
                                          device_id={'rows': prv}, device_id_type=MESH)
    to_nxt = pltpu.make_async_remote_copy(src_ref=gns, dst_ref=gnr, send_sem=gsend_sem.at[1], recv_sem=grecv_sem.at[1],
                                          device_id={'rows': nxt}, device_id_type=MESH)
    to_prv.start()
    to_nxt.start()

    for j in range(1, N_CHUNK - 1):
        merge_all(CHUNK_TILES[j], put_chunk)
        first_dft(j, gch[...])
        post(j)

    to_prv.wait()
    to_nxt.wait()
    gp, gn = gpr[...], gnr[...]
    for c in range(8):
        s = slice(Q_PAD * c, Q_PAD * c + Q_PAD)
        gch[s, LANES:WIDE] = (f11[s, :] + jnp.where((la >> 1) == 3, shifted(gp, 6 - 2 * c), 0.0)).astype(BF16)
    for c in range(16):
        s = slice(GN_ROWS * c, GN_ROWS * c + GN_ROWS)
        gch[s, 0:LANES] = (f0[s, :] + jnp.where(lb == 0, shifted(gn, -c), 0.0)).astype(BF16)
    first_dft(N_CHUNK - 1, gch[...])
    post(N_CHUNK - 1)

    for c in loads[1:]:
        c.wait()
    for j in range(N_CHUNK):
        for h in range(2):
            v = e2_ref[LANES * j + 64 * h:LANES * j + 64 * h + 64, :]
            e2f[j, LANES * h:LANES * h + 64, :] = v
            e2f[j, LANES * h + 64:LANES * h + LANES, 0:P_ALL] = -v[:, P_ALL:P_TWO]
            e2f[j, LANES * h + 64:LANES * h + LANES, P_ALL:P_TWO] = v[:, 0:P_ALL]
    st[...] = jnp.zeros_like(st)
    for s in range(2):
        for c in range(4):
            st[s, c, 0:Q_BLK, 0:N_IMG] = s_ref[s, :, c, :]

    half_p = jnp.where(k == 0, d_ref[:, 0:P_BLK], d_ref[:, P_BLK:2 * P_BLK])
    part_q = d_ref[:, 0:Q_BLK]
    for i in range(1, 4):
        part_q = jnp.where(r == i, d_ref[:, Q_BLK * i:Q_BLK * (i + 1)], part_q)
    part_q = jnp.concatenate([part_q, jnp.zeros((1, LANES - Q_BLK), F32)], axis=1)
    dd[...] = jnp.broadcast_to(part_q, (8, LANES)).T[0:Q_BLK, 0:1] * half_p

    first_col = k == 0
    for sub, (row0, rows) in enumerate(SUBS):
        coil = (lax.broadcasted_iota(jnp.int32, (rows, LANES), 1) >> 4) & 3

        def regroup(j, pair):
            v = [recv[j, 2 * pair + t // 2, pl.ds(row0, rows), LANES * (t % 2):LANES * (t % 2 + 1)] for t in range(4)]
            for bit in (1, 2):
                m = (coil & bit) == 0
                for t in range(4):
                    if t & bit:
                        continue
                    x, y = v[t], v[t | bit]
                    v[t] = jnp.where(m, x, pltpu.roll(y, ROWS * bit, 1))
                    v[t | bit] = jnp.where(m, pltpu.roll(x, LANES - ROWS * bit, 1), y)
            return v

        def second_dft(j):
            for i in range(3):
                copy_of(j, sub, i, dests[i]).wait_recv()
            both = regroup(j, 0), regroup(j, 1)
            lhs = jnp.concatenate([jnp.concatenate([both[0][c], both[1][c]], axis=1) for c in range(4)], axis=0)
            return jnp.dot(lhs, e2f[j], preferred_element_type=F32)

        acc = img.at[pl.ds(4 * row0, 4 * rows)]
        acc[...] = second_dft(0)

        def accumulate(j, _):
            acc[...] += second_dft(j)
            return 0
        lax.fori_loop(1, N_CHUNK, accumulate, 0)

        x_re = jnp.zeros((rows, P_ALL), F32)
        x_im = jnp.zeros((rows, P_ALL), F32)
        for c in range(4):
            i_re = acc[rows * c:rows * (c + 1), 0:P_ALL]
            i_im = acc[rows * c:rows * (c + 1), P_ALL:P_TWO]
            s_re, s_im = st[0, c, row0:row0 + rows], st[1, c, row0:row0 + rows]
            x_re = x_re + s_re * i_re + s_im * i_im
            x_im = x_im + s_re * i_im - s_im * i_re
        lo = jnp.concatenate([x_re[:, 0:P_PAD], x_im[:, 0:P_PAD]], axis=1)
        hi = jnp.concatenate([x_re[:, P_BLK:P_BLK + P_PAD], x_im[:, P_BLK:P_BLK + P_PAD]], axis=1)
        psend[row0:row0 + rows] = jnp.where(first_col, hi, lo)
        swap(sub).start()
        mine[row0:row0 + rows] = jnp.where(first_col, lo, hi)

    for j in range(N_CHUNK):
        for sub in range(len(SUBS)):
            for i in range(3):
                copy_of(j, sub, i, r).wait_send()
    for sub in range(len(SUBS)):
        swap(sub).wait()
    total = mine[...] + precv[...]
    out_ref[0] = (total[0:Q_BLK, 0:P_BLK] * dd[...]).T
    out_ref[1] = (total[0:Q_BLK, P_PAD:P_PAD + P_BLK] * dd[...]).T


def solution(mesh):
    sample_spec = ('exam', 'rows', 'cols')
    vmem = pl.BlockSpec(memory_space=pltpu.VMEM)
    hbm = pl.BlockSpec(memory_space=pltpu.HBM)
    sds = jax.ShapeDtypeStruct

    def local_fn(kspace, wts_y, wts_x, idx_y, idx_x, coil_maps, deapod):
        n = kspace.shape[2]
        e1, e2 = dft_constants()
        acc_shape = [sds((N_SRC * VS, LANES), F32)] * (N_ACC)
        *accs, token = pl.pallas_call(
            zero_kernel,
            out_shape=acc_shape + [sds((8, LANES), F32)],
            out_specs=[vmem] * (N_ACC + 1),
            compiler_params=pltpu.CompilerParams(vmem_limit_bytes=MIB),
            cost_estimate=pl.CostEstimate(flops=2 * 10**9, bytes_accessed=2 * 10**7, transcendentals=0),
            name='zero',
        )()
        samples = pl.pallas_call(
            exchange_kernel,
            out_shape=[sds((2, 8, n), F32), sds((2, 4, n), F32), sds((2, 4, n), F32), sds((2, 16, LANES), jnp.int32),
                       sds((2, 16, LANES), jnp.int32)],
            in_specs=[vmem] + [hbm] * 5,
            out_specs=[vmem] * 5,
            scratch_shapes=[pltpu.VMEM((2, 8, n), F32), pltpu.VMEM((16, LANES), jnp.int32), pltpu.VMEM((16, LANES), jnp.int32),
                            pltpu.VMEM((8, n), F32), pltpu.SemaphoreType.DMA((5,)), pltpu.SemaphoreType.DMA((5,)),
                            pltpu.SemaphoreType.DMA((5,))],
            compiler_params=pltpu.CompilerParams(collective_id=0, has_side_effects=True, vmem_limit_bytes=8 * MIB),
            name='exchange',
        )(token, kspace, wts_y, wts_x, idx_y.reshape(16, LANES), idx_x.reshape(16, LANES))
        y8, wy, wx, addr, roff = samples
        accs = pl.pallas_call(
            spread_kernel,
            out_shape=acc_shape,
            in_specs=[vmem] * (5 + N_ACC),
            out_specs=[vmem] * (N_ACC),
            scratch_shapes=[pltpu.SMEM((2, 16, LANES), jnp.int32)] + [pltpu.VMEM((WIDE, LANES), F32)] * 4 + [pltpu.SemaphoreType.DMA],
            input_output_aliases={5 + i: i for i in range(N_ACC)},
            compiler_params=pltpu.CompilerParams(vmem_limit_bytes=8 * MIB),
            name='spread',
        )(addr, y8, wy, wx, roff, *accs)
        maps = jnp.transpose(coil_maps, (0, 3, 1, 2))
        return pl.pallas_call(
            transform_kernel,
            out_shape=sds((2, P_BLK, Q_BLK), F32),
            in_specs=[vmem] * (N_ACC) + [hbm] * 4,
            out_specs=vmem,
            scratch_shapes=[pltpu.VMEM((KV, KV), BF16), pltpu.VMEM((KV, P_TWO), BF16), pltpu.VMEM((2, Q_BLK, 4, N_IMG), F32),
                            pltpu.VMEM((1, N_IMG), F32), pltpu.VMEM((Q_BLK, P_BLK), F32), pltpu.VMEM((KV, WIDE), BF16)] + [pltpu.VMEM((KV, LANES), F32)] * 3 + [
                pltpu.VMEM((Q_PAD, LANES), F32),
                pltpu.VMEM((GN_ROWS, LANES), F32),
                pltpu.VMEM((N_CHUNK, 4, Q_PAD, WIDE), BF16),
                pltpu.VMEM((N_CHUNK, 4, Q_PAD, WIDE), BF16),
                pltpu.VMEM((Q_PAD, LANES), F32),
                pltpu.VMEM((GN_ROWS, LANES), F32),
                pltpu.VMEM((N_CHUNK, WIDE, P_TWO), BF16),
                pltpu.VMEM((2, 4, Q_PAD, P_ALL), F32),
                pltpu.VMEM((4 * Q_PAD, P_TWO), F32),
                pltpu.VMEM((Q_PAD, P_ALL), F32),
                pltpu.VMEM((Q_PAD, P_ALL), F32),
                pltpu.VMEM((Q_PAD, P_ALL), F32),
                pltpu.SemaphoreType.DMA((N_CHUNK, len(SUBS), 3)),
                pltpu.SemaphoreType.DMA((N_CHUNK, len(SUBS), 4)),
                pltpu.SemaphoreType.DMA((2,)),
                pltpu.SemaphoreType.DMA((2,)),
                pltpu.SemaphoreType.DMA((len(SUBS),)),
                pltpu.SemaphoreType.DMA((len(SUBS),)),
                pltpu.SemaphoreType.DMA((4,)),
            ],
            compiler_params=pltpu.CompilerParams(collective_id=1, has_side_effects=True, vmem_limit_bytes=24 * MIB),
            name='transform',
        )(*accs, e1, e2, maps, deapod.reshape(1, N_IMG))

    return jax.shard_map(
        local_fn,
        mesh=mesh,
        in_specs=(P(None, None, sample_spec), P(None, sample_spec), P(None, sample_spec), P(sample_spec), P(sample_spec), P(None, ('exam', 'cols'), None, 'rows'), P()),
        out_specs=P(None, ('exam', 'cols'), 'rows'),
        check_vma=False,
    )
```

```python
import math

import jax
import jax.numpy as jnp
import numpy as np
from jax import lax
from jax.experimental import pallas as pl
from jax.experimental.pallas import tpu as pltpu
from jax.sharding import PartitionSpec as P

F32, BF16 = jnp.float32, jnp.bfloat16
MESH = pl.DeviceIdType.MESH

N_IMG = 368
N_GRID = 736
ROW_BLK = 184
Q_BLK, Q_PAD = 92, 96
P_BLK, P_PAD, P_ALL = 184, 192, 384
N_CH = 8
TILE_U, STRIDE_U, N_SRC = 16, 13, 15
N_TGT = 12
COL_BLK = 368
VR = 384
VS = 392
KV = 2 * VR
LANES, ROWS = 128, 16
EDGE = 6
WIDE, P_TWO, GN_ROWS, MIB = 2 * LANES, 2 * P_ALL, 48, 2**20
N_CHUNK = 6
N_COPY = 3
N_ACC = 2 * N_COPY
SUBS = [(0, 64), (64, 32), (0, Q_PAD)]
FULL, N_WHOLE = 2, 2
WHOLE, SPLIT = range(N_WHOLE), range(N_WHOLE, N_CHUNK)
POSTS = [[(j, FULL)] for j in WHOLE] + [[(j, 0)] for j in SPLIT]
POSTS[-1] += [(j, 1) for j in SPLIT]
SENT = [(j, FULL) for j in WHOLE] + [(j, sub) for j in SPLIT for sub in range(2)]
CHUNK_TILES = [(1 + 2 * j, 2 + 2 * j) for j in range(5)] + [(0, 11)]


def dft_constants():
    scale = 1.0 / math.sqrt(N_GRID)
    phase = ((np.arange(N_GRID)[:, None] - N_GRID // 2) * (np.arange(N_IMG)[None, :] - N_IMG // 2)) % N_GRID
    ang = phase.astype(np.float64) * (2.0 * math.pi / N_GRID)
    parts = (np.cos(ang) * scale, np.sin(ang) * scale)
    e1 = np.zeros((4, 2, Q_PAD, 2, VR))
    for dest in range(4):
        for cs in range(2):
            for half in range(2):
                part = parts[cs][half * COL_BLK:(half + 1) * COL_BLK, dest * Q_BLK:(dest + 1) * Q_BLK]
                e1[dest, cs, :Q_BLK, half, EDGE:EDGE + COL_BLK] = part.T
    e2 = np.zeros((N_CHUNK, 4, 2, TILE_U, 2, P_ALL))
    for j in range(N_CHUNK):
        for src in range(4):
            for tl in range(2):
                base = TILE_U * CHUNK_TILES[j][tl]
                rows = min(TILE_U, ROW_BLK - base)
                u0 = src * ROW_BLK + base
                for cs in range(2):
                    e2[j, src, tl, :rows, cs, :N_IMG] = parts[cs][u0:u0 + rows]
    return (jnp.asarray(e1.reshape(8 * Q_PAD, KV).astype(np.float32)).astype(BF16),
            jnp.asarray(e2.reshape(N_CHUNK * LANES, P_TWO).astype(np.float32)).astype(BF16))


def zero_kernel(*refs):
    *accs, token = refs

    def zero(i, _):
        for a in accs:
            a[pl.ds(pl.multiple_of(i * VS, 8), VS), :] = jnp.zeros((VS, LANES), F32)
        return 0
    lax.fori_loop(0, N_SRC, zero, 0)
    token[...] = jnp.zeros_like(token)


def exchange_kernel(_, y_hbm, wy_hbm, wx_hbm, iy_hbm, ix_hbm, e2_ref, s_ref, d_ref,
                    y_ref, wy_ref, wx_ref, addr_ref, roff_ref, e2f, st, dd, *refs):
    y_in, iy, ix, y_send, in_sem, send_sem, recv_sem = refs
    k = lax.axis_index('cols')
    r = lax.axis_index('rows')
    other = {'cols': 1 - k}
    barrier = pltpu.get_barrier_semaphore()
    pl.semaphore_signal(barrier, inc=1, device_id=other, device_id_type=MESH)
    loads = [(iy_hbm, iy), (ix_hbm, ix), (y_hbm, y_in), (wy_hbm, wy_ref.at[0]), (wx_hbm, wx_ref.at[0])]
    loads = [pltpu.make_async_copy(a, b, in_sem.at[i]) for i, (a, b) in enumerate(loads)]
    for c in loads:
        c.start()

    def send(i, src, dst):
        c = pltpu.make_async_remote_copy(src_ref=src, dst_ref=dst, send_sem=send_sem.at[i], recv_sem=recv_sem.at[i],
                                         device_id=other, device_id_type=MESH)
        c.start()
        return c

    loads[0].wait()
    loads[1].wait()
    row = iy[...] - r * ROW_BLK
    tile = jnp.zeros_like(row)
    for t in range(1, N_SRC):
        tile = tile + jnp.where(row >= STRIDE_U * t, 1, 0)
    addr_ref[0] = tile * VS + (ix[...] - k * COL_BLK)
    roff_ref[0] = (row + 14) & 15
    loads[2].wait()
    y_re, y_im = y_in[0], y_in[1]
    low = jnp.concatenate([y_re[0:4], y_im[0:4]], axis=0)
    high = jnp.concatenate([y_re[4:8], y_im[4:8]], axis=0)
    y_ref[0] = jnp.where(k == 0, low, high)
    y_send[...] = jnp.where(k == 0, high, low)
    loads[3].wait()
    loads[4].wait()
    pl.semaphore_wait(barrier, 1)
    copies = [send(0, wy_ref.at[0], wy_ref.at[1]), send(1, wx_ref.at[0], wx_ref.at[1]), send(2, addr_ref.at[0], addr_ref.at[1]),
              send(3, roff_ref.at[0], roff_ref.at[1]), send(4, y_send, y_ref.at[1])]

    for j in range(N_CHUNK):
        for h in range(2):
            v = e2_ref[LANES * j + 64 * h:LANES * j + 64 * h + 64, :]
            e2f[j, LANES * h:LANES * h + 64, :] = v
            e2f[j, LANES * h + 64:LANES * h + LANES, 0:P_ALL] = -v[:, P_ALL:P_TWO]
            e2f[j, LANES * h + 64:LANES * h + LANES, P_ALL:P_TWO] = v[:, 0:P_ALL]
    st[...] = jnp.zeros_like(st)
    for s in range(2):
        for c in range(4):
            st[s, c, 0:Q_BLK, 0:N_IMG] = s_ref[s, :, c, :]

    half_p = jnp.where(k == 0, d_ref[:, 0:P_BLK], d_ref[:, P_BLK:2 * P_BLK])
    part_q = d_ref[:, 0:Q_BLK]
    for i in range(1, 4):
        part_q = jnp.where(r == i, d_ref[:, Q_BLK * i:Q_BLK * (i + 1)], part_q)
    part_q = jnp.concatenate([part_q, jnp.zeros((1, LANES - Q_BLK), F32)], axis=1)
    dd[...] = jnp.broadcast_to(part_q, (8, LANES)).T[0:Q_BLK, 0:1] * half_p

    for c in copies:
        c.wait()


def split3(x):
    hi = x.astype(BF16).astype(F32)
    rest = x - hi
    mid = rest.astype(BF16).astype(F32)
    return [hi, mid, rest - mid]


def spread_kernel(addr_ref, y_ref, wy_ref, wx_ref, roff_ref, *refs):
    accs = refs[N_ACC:4 * N_COPY]
    addr, sem = refs[4 * N_COPY], refs[-1]
    q_refs = refs[4 * N_COPY + 1:-1]
    to_smem = pltpu.make_async_copy(addr_ref, addr, sem)
    to_smem.start()
    n = y_ref.shape[2]

    r0 = lax.broadcasted_iota(jnp.int32, (80, WIDE), 0)
    l0 = lax.broadcasted_iota(jnp.int32, (80, WIDE), 1)
    ry = (r0 < 24) & (l0 < LANES) & ((r0 & 7) == (l0 >> 4))
    rw = (r0 >= 24) & (r0 < 72) & (l0 >= LANES) & (((r0 - 24) & 15) == (l0 & 15))
    expand = jnp.where(ry | rw, 1.0, 0.0).astype(BF16)
    rr = lax.broadcasted_iota(jnp.int32, (ROWS, WIDE), 0)
    n_blk = n // WIDE

    def prep(i, slot, q_ref):
        ds = [pl.ds(pl.multiple_of((i + n_blk * h) * LANES, LANES), LANES) for h in range(2)]
        y = jnp.concatenate([y_ref[slot, :, s] for s in ds], axis=1)
        wy = jnp.concatenate([wy_ref[slot, :, s] for s in ds], axis=1)
        d = (rr - jnp.concatenate([roff_ref[slot, pl.ds(i + n_blk * h, 1), :] for h in range(2)], axis=1)) & 15
        w16 = jnp.zeros((ROWS, WIDE), F32)
        for a in range(4):
            w16 = jnp.where(d == a, wy[a:a + 1], w16)
        lhs = jnp.concatenate(split3(y) + split3(w16) + [jnp.zeros((8, WIDE), F32)], axis=0).astype(BF16)
        o = lax.dot_general(lhs, expand, (((0,), (0,)), ((), ())), preferred_element_type=F32)
        q_ref[...] = o[:, :LANES] * o[:, LANES:]

    top = lax.broadcasted_iota(jnp.int32, (8, LANES), 0) < 4

    def scatter(i, qs):
        ds = [pl.ds(pl.multiple_of((i + n_blk * h) * LANES, LANES), LANES) for h in range(2)]
        wx = [jnp.concatenate([wx_ref[slot, :, s] for s in ds], axis=0) for slot in range(2)]
        for j in range(LANES):
            cols = [jnp.broadcast_to(wx[slot][:, j:j + 1], (8, LANES)) for slot in range(2)]
            for h in range(2):
                for slot in range(2):
                    acc = accs[slot * N_COPY + (2 * j + h) % N_COPY]
                    base = addr[slot, i + n_blk * h, j] + (0 if h else 4)
                    q = jnp.broadcast_to(qs[slot][j + LANES * h:j + LANES * h + 1, :], (8, LANES))
                    s = pl.ds(base, 8)
                    c = jnp.where(top, 0.0, cols[slot]) if h else jnp.where(top, cols[slot], 0.0)
                    acc[s, :] = acc[s, :] + c * q

    qa, qb = q_refs[:2], q_refs[2:]
    for slot in range(2):
        prep(0, slot, qa[slot])
    to_smem.wait()

    def two_blocks(i, _):
        for step, now, then in ((0, qa, qb), (1, qb, qa)):
            for slot in range(2):
                prep(lax.rem(2 * i + step + 1, n_blk), slot, then[slot])
            scatter(2 * i + step, now)
        return 0
    lax.fori_loop(0, n_blk // 2, two_blocks, 0)


def transform_kernel(*refs):
    own, nbr = refs[:N_COPY], refs[N_COPY:N_ACC]
    (e1_ref, e2f, st, dd, out_ref, gch, raw0, f0, f11, gps, gns, msg, recv, gpr, gnr, img, mine, psend, precv,
     msend_sem, mrecv_sem, gsend_sem, grecv_sem, psend_sem, precv_sem) = refs[N_ACC:]
    k = lax.axis_index('cols')
    r = lax.axis_index('rows')
    chip, core = r // 2, r % 2
    dests = [2 * (1 - chip) + core, 2 * (1 - chip) + (1 - core), 2 * chip + (1 - core)]
    nxt, prv = lax.rem(r + 1, 4), lax.rem(r + 3, 4)
    barrier = pltpu.get_barrier_semaphore()
    for d in dests:
        pl.semaphore_signal(barrier, inc=1, device_id={'rows': d}, device_id_type=MESH)
    pl.semaphore_signal(barrier, inc=1, device_id={'cols': 1 - k}, device_id_type=MESH)

    slots = ((own, k), (nbr, 1 - k))
    lane16 = lax.broadcasted_iota(jnp.int32, (ROWS, LANES), 1) & 15
    sub16 = lax.broadcasted_iota(jnp.int32, (ROWS, LANES), 0)

    def merged(accs, off, targets):
        wanted = {}
        for m in targets:
            deltas = {0: 0} if m is None else {t: STRIDE_U * t - TILE_U * m - 2 for t in range(N_SRC)}
            wanted[m] = {t: d for t, d in deltas.items() if abs(d) < ROWS}
        loaded = {}
        for t in sorted({t for w in wanted.values() for t in w}):
            s = pl.ds(t * VS + off, ROWS)
            v = accs[0][s, :]
            for acc in accs[1:]:
                v = v + acc[s, :]
            loaded[t] = v
        outs = []
        for m in targets:
            out = None
            for t, d in wanted[m].items():
                lo, hi = max(0, d), min(15, 15 + d)
                v = loaded[t]
                if lo > 0 or hi < 15:
                    v = jnp.where((lane16 >= lo) & (lane16 <= hi), v, 0.0)
                out = v if out is None else out + v
            outs.append(out)
        return outs

    def merge_all(targets, put):
        def rows(i, _):
            for step in range(2):
                for accs, half in slots:
                    off = pl.multiple_of((2 * i + 1 + step) * ROWS, ROWS)
                    put(pl.multiple_of(half * VR + off, ROWS), merged(accs, off, targets))
            return 0
        lax.fori_loop(0, VR // (2 * ROWS) - 1, rows, 0)
        last = VR - ROWS
        a = [merged(accs, 0, targets) for accs, _ in slots]
        b = [merged(accs, last, targets) for accs, _ in slots]
        for i, (_, half) in enumerate(slots):
            fix_a = [x + jnp.where(sub16 == 6, y, 0.0) for x, y in zip(a[i], b[1 - i])]
            fix_b = [y + jnp.where((sub16 == 4) | (sub16 == 5), x, 0.0) for x, y in zip(a[1 - i], b[i])]
            put(pl.multiple_of(half * VR, ROWS), fix_a)
            put(pl.multiple_of(half * VR + last, ROWS), fix_b)

    def put_chunk(off, vals):
        for i, v in enumerate(vals):
            gch[pl.ds(off, ROWS), LANES * i:LANES * (i + 1)] = v.astype(BF16)

    def put_edges(off, vals):
        for ref, v in zip((raw0, f0, f11), vals):
            ref[pl.ds(off, ROWS), :] = v

    lane = lax.broadcasted_iota(jnp.int32, (Q_PAD, WIDE), 1) & 127

    def swap(sub):
        rows = pl.ds(*SUBS[sub])
        return pltpu.make_async_remote_copy(src_ref=psend.at[rows], dst_ref=precv.at[rows], send_sem=psend_sem.at[sub],
                                            recv_sem=precv_sem.at[sub], device_id={'cols': 1 - k}, device_id_type=MESH)

    def first_dft(j, g):
        ab = jnp.dot(e1_ref[...], g, preferred_element_type=F32)
        for d in range(4):
            a = ab[192 * d:192 * d + Q_PAD]
            b = ab[192 * d + Q_PAD:192 * d + 192]
            b = jnp.concatenate([pltpu.roll(b[:, :128], 64, 1), pltpu.roll(b[:, 128:], 64, 1)], axis=1)
            msg[j, d] = jnp.where(lane < 64, a - b, a + b).astype(BF16)

    def copy_of(j, sub, i, slot):
        d = dests[i]
        rows = pl.ds(*SUBS[sub])
        return pltpu.make_async_remote_copy(src_ref=msg.at[j, d, rows], dst_ref=recv.at[j, slot, rows], send_sem=msend_sem.at[j, sub, i],
                                            recv_sem=mrecv_sem.at[j, sub, slot], device_id={'rows': d}, device_id_type=MESH)

    def post(chunk):
        for j, sub in POSTS[chunk]:
            for i in range(3):
                copy_of(j, sub, i, r).start()
        recv[chunk, r] = msg[chunk, r]

    merge_all(CHUNK_TILES[0], put_chunk)
    first_dft(0, gch[...])
    pl.semaphore_wait(barrier, 4)
    post(0)

    merge_all((None, 0, N_TGT - 1), put_edges)
    la = lax.broadcasted_iota(jnp.int32, (Q_PAD, LANES), 1) & 15
    lb = lax.broadcasted_iota(jnp.int32, (GN_ROWS, LANES), 1) & 15

    def shifted(v, by):
        return pltpu.roll(v, by % LANES, 1) if by else v

    gp = jnp.zeros((Q_PAD, LANES), F32)
    for c in range(8):
        gp = jnp.where((la >> 1) == c, shifted(raw0[Q_PAD * c:Q_PAD * c + Q_PAD, :], 2 * c - 14), gp)
    gps[...] = gp
    gn = jnp.zeros((GN_ROWS, LANES), F32)
    for c in range(16):
        gn = jnp.where(lb == c, shifted(f11[GN_ROWS * c:GN_ROWS * c + GN_ROWS, :], c - 8), gn)
    gns[...] = gn
    to_prv = pltpu.make_async_remote_copy(src_ref=gps, dst_ref=gpr, send_sem=gsend_sem.at[0], recv_sem=grecv_sem.at[0],
                                          device_id={'rows': prv}, device_id_type=MESH)
    to_nxt = pltpu.make_async_remote_copy(src_ref=gns, dst_ref=gnr, send_sem=gsend_sem.at[1], recv_sem=grecv_sem.at[1],
                                          device_id={'rows': nxt}, device_id_type=MESH)
    to_prv.start()
    to_nxt.start()

    for j in range(1, N_CHUNK - 1):
        merge_all(CHUNK_TILES[j], put_chunk)
        first_dft(j, gch[...])
        post(j)

    to_prv.wait()
    to_nxt.wait()
    gp, gn = gpr[...], gnr[...]
    for c in range(8):
        s = slice(Q_PAD * c, Q_PAD * c + Q_PAD)
        gch[s, LANES:WIDE] = (f11[s, :] + jnp.where((la >> 1) == 3, shifted(gp, 6 - 2 * c), 0.0)).astype(BF16)
    for c in range(16):
        s = slice(GN_ROWS * c, GN_ROWS * c + GN_ROWS)
        gch[s, 0:LANES] = (f0[s, :] + jnp.where(lb == 0, shifted(gn, -c), 0.0)).astype(BF16)
    first_dft(N_CHUNK - 1, gch[...])
    post(N_CHUNK - 1)

    first_col = k == 0

    def second_dft(j, sub):
        row0, rows = SUBS[sub]
        for i in range(3):
            copy_of(j, sub, i, dests[i]).wait_recv()
        coil = (lax.broadcasted_iota(jnp.int32, (rows, LANES), 1) >> 4) & 3
        halves = []
        for pair in range(2):
            v = [recv[j, 2 * pair + t // 2, pl.ds(row0, rows), LANES * (t % 2):LANES * (t % 2 + 1)] for t in range(4)]
            for bit in (1, 2):
                m = (coil & bit) == 0
                for t in range(4):
                    if t & bit:
                        continue
                    x, y = v[t], v[t | bit]
                    v[t] = jnp.where(m, x, pltpu.roll(y, ROWS * bit, 1))
                    v[t | bit] = jnp.where(m, pltpu.roll(x, LANES - ROWS * bit, 1), y)
            halves.append(v)
        lhs = jnp.concatenate([jnp.concatenate([halves[0][c], halves[1][c]], axis=1) for c in range(4)], axis=0)
        return jnp.dot(lhs, e2f[j], preferred_element_type=F32)

    img[...] = second_dft(0, FULL)
    for j in WHOLE[1:]:
        img[...] += second_dft(j, FULL)
    for sub in range(2):
        row0, rows = SUBS[sub]

        def accumulate(j, _):
            part = second_dft(j, sub)
            for c in range(4):
                img[Q_PAD * c + row0:Q_PAD * c + row0 + rows] += part[rows * c:rows * (c + 1)]
            return 0
        lax.fori_loop(N_WHOLE, N_CHUNK, accumulate, 0)

        x_re = jnp.zeros((rows, P_ALL), F32)
        x_im = jnp.zeros((rows, P_ALL), F32)
        for c in range(4):
            i_re = img[Q_PAD * c + row0:Q_PAD * c + row0 + rows, 0:P_ALL]
            i_im = img[Q_PAD * c + row0:Q_PAD * c + row0 + rows, P_ALL:P_TWO]
            s_re, s_im = st[0, c, row0:row0 + rows], st[1, c, row0:row0 + rows]
            x_re = x_re + s_re * i_re + s_im * i_im
            x_im = x_im + s_re * i_im - s_im * i_re
        lo = jnp.concatenate([x_re[:, 0:P_PAD], x_im[:, 0:P_PAD]], axis=1)
        hi = jnp.concatenate([x_re[:, P_BLK:P_BLK + P_PAD], x_im[:, P_BLK:P_BLK + P_PAD]], axis=1)
        psend[row0:row0 + rows] = jnp.where(first_col, hi, lo)
        swap(sub).start()
        mine[row0:row0 + rows] = jnp.where(first_col, lo, hi)

    for j, sub in SENT:
        for i in range(3):
            copy_of(j, sub, i, r).wait_send()
    for sub in range(2):
        swap(sub).wait()
    total = mine[...] + precv[...]
    out_ref[0] = (total[0:Q_BLK, 0:P_BLK] * dd[...]).T
    out_ref[1] = (total[0:Q_BLK, P_PAD:P_PAD + P_BLK] * dd[...]).T


def solution(mesh):
    sample_spec = ('exam', 'rows', 'cols')
    vmem = pl.BlockSpec(memory_space=pltpu.VMEM)
    hbm = pl.BlockSpec(memory_space=pltpu.HBM)
    sds = jax.ShapeDtypeStruct

    def local_fn(kspace, wts_y, wts_x, idx_y, idx_x, coil_maps, deapod):
        n = kspace.shape[2]
        e1, e2 = dft_constants()
        maps = jnp.transpose(coil_maps, (0, 3, 1, 2))
        acc_shape = [sds((N_SRC * VS, LANES), F32)] * (N_ACC)
        *accs, token = pl.pallas_call(
            zero_kernel,
            out_shape=acc_shape + [sds((8, LANES), F32)],
            out_specs=[vmem] * (N_ACC + 1),
            compiler_params=pltpu.CompilerParams(vmem_limit_bytes=MIB),
            cost_estimate=pl.CostEstimate(flops=2 * 10**9, bytes_accessed=2 * 10**7, transcendentals=0),
            name='zero',
        )()
        samples = pl.pallas_call(
            exchange_kernel,
            out_shape=[sds((2, 8, n), F32), sds((2, 4, n), F32), sds((2, 4, n), F32), sds((2, 16, LANES), jnp.int32),
                       sds((2, 16, LANES), jnp.int32), sds((N_CHUNK, WIDE, P_TWO), BF16), sds((2, 4, Q_PAD, P_ALL), F32), sds((Q_BLK, P_BLK), F32)],
            in_specs=[vmem] + [hbm] * 5 + [vmem] * 3,
            out_specs=[vmem] * 8,
            scratch_shapes=[pltpu.VMEM((2, 8, n), F32), pltpu.VMEM((16, LANES), jnp.int32), pltpu.VMEM((16, LANES), jnp.int32),
                            pltpu.VMEM((8, n), F32), pltpu.SemaphoreType.DMA((5,)), pltpu.SemaphoreType.DMA((5,)),
                            pltpu.SemaphoreType.DMA((5,))],
            compiler_params=pltpu.CompilerParams(collective_id=0, has_side_effects=True, vmem_limit_bytes=8 * MIB),
            name='exchange',
        )(token, kspace, wts_y, wts_x, idx_y.reshape(16, LANES), idx_x.reshape(16, LANES), e2, maps, deapod.reshape(1, N_IMG))
        y8, wy, wx, addr, roff, e2f, st, dd = samples
        accs = pl.pallas_call(
            spread_kernel,
            out_shape=acc_shape,
            in_specs=[vmem] * (5 + N_ACC),
            out_specs=[vmem] * (N_ACC),
            scratch_shapes=[pltpu.SMEM((2, 16, LANES), jnp.int32)] + [pltpu.VMEM((WIDE, LANES), F32)] * 4 + [pltpu.SemaphoreType.DMA],
            input_output_aliases={5 + i: i for i in range(N_ACC)},
            compiler_params=pltpu.CompilerParams(vmem_limit_bytes=8 * MIB),
            cost_estimate=pl.CostEstimate(flops=2 * 10**9, bytes_accessed=2 * 10**7, transcendentals=0),
            name='spread',
        )(addr, y8, wy, wx, roff, *accs)
        return pl.pallas_call(
            transform_kernel,
            out_shape=sds((2, P_BLK, Q_BLK), F32),
            in_specs=[vmem] * (N_ACC + 4),
            out_specs=vmem,
            scratch_shapes=[pltpu.VMEM((KV, WIDE), BF16)] + [pltpu.VMEM((KV, LANES), F32)] * 3 + [
                pltpu.VMEM((Q_PAD, LANES), F32),
                pltpu.VMEM((GN_ROWS, LANES), F32),
                pltpu.VMEM((N_CHUNK, 4, Q_PAD, WIDE), BF16),
                pltpu.VMEM((N_CHUNK, 4, Q_PAD, WIDE), BF16),
                pltpu.VMEM((Q_PAD, LANES), F32),
                pltpu.VMEM((GN_ROWS, LANES), F32),
                pltpu.VMEM((4 * Q_PAD, P_TWO), F32),
                pltpu.VMEM((Q_PAD, P_ALL), F32),
                pltpu.VMEM((Q_PAD, P_ALL), F32),
                pltpu.VMEM((Q_PAD, P_ALL), F32),
                pltpu.SemaphoreType.DMA((N_CHUNK, len(SUBS), 3)),
                pltpu.SemaphoreType.DMA((N_CHUNK, len(SUBS), 4)),
                pltpu.SemaphoreType.DMA((2,)),
                pltpu.SemaphoreType.DMA((2,)),
                pltpu.SemaphoreType.DMA((len(SUBS),)),
                pltpu.SemaphoreType.DMA((len(SUBS),)),
            ],
            compiler_params=pltpu.CompilerParams(collective_id=1, has_side_effects=True, vmem_limit_bytes=24 * MIB),
            name='transform',
        )(*accs, e1, e2f, st, dd)

    return jax.shard_map(
        local_fn,
        mesh=mesh,
        in_specs=(P(None, None, sample_spec), P(None, sample_spec), P(None, sample_spec), P(sample_spec), P(sample_spec), P(None, ('exam', 'cols'), None, 'rows'), P()),
        out_specs=P(None, ('exam', 'cols'), 'rows'),
        check_vma=False,
    )
```

```python
import math

import jax
import jax.numpy as jnp
import numpy as np
from jax import lax
from jax.experimental import pallas as pl
from jax.experimental.pallas import tpu as pltpu
from jax.sharding import PartitionSpec as P

F32, BF16 = jnp.float32, jnp.bfloat16
MESH = pl.DeviceIdType.MESH

N_IMG = 368
N_GRID = 736
ROW_BLK = 184
Q_BLK, Q_PAD = 92, 96
P_BLK, P_PAD, P_ALL = 184, 192, 384
N_CH = 8
TILE_U, STRIDE_U, N_SRC = 16, 13, 15
N_TGT = 12
COL_BLK = 368
VR = 384
VS = 392
KV = 2 * VR
LANES, ROWS = 128, 16
EDGE = 6
WIDE, P_TWO, GN_ROWS, MIB = 2 * LANES, 2 * P_ALL, 48, 2**20
N_CHUNK = 6
N_COPY = 3
N_ACC = 2 * N_COPY
SUBS = [(0, 64), (64, 32), (0, Q_PAD)]
FULL, N_WHOLE = 2, 2
WHOLE, SPLIT = range(N_WHOLE), range(N_WHOLE, N_CHUNK)
POSTS = [[(j, FULL)] for j in WHOLE] + [[(j, 0)] for j in SPLIT]
POSTS += [[(j, 1) for j in SPLIT]]
SENT = [(j, FULL) for j in WHOLE] + [(j, sub) for j in SPLIT for sub in range(2)]
CHUNK_TILES = [(1 + 2 * j, 2 + 2 * j) for j in range(5)] + [(0, 11)]


def dft_constants():
    scale = 1.0 / math.sqrt(N_GRID)
    phase = ((np.arange(N_GRID)[:, None] - N_GRID // 2) * (np.arange(N_IMG)[None, :] - N_IMG // 2)) % N_GRID
    ang = phase.astype(np.float64) * (2.0 * math.pi / N_GRID)
    parts = (np.cos(ang) * scale, np.sin(ang) * scale)
    e1 = np.zeros((4, 2, Q_PAD, 2, VR))
    for dest in range(4):
        for cs in range(2):
            for half in range(2):
                part = parts[cs][half * COL_BLK:(half + 1) * COL_BLK, dest * Q_BLK:(dest + 1) * Q_BLK]
                e1[dest, cs, :Q_BLK, half, EDGE:EDGE + COL_BLK] = part.T
    e2 = np.zeros((N_CHUNK, 4, 2, TILE_U, 2, P_ALL))
    for j in range(N_CHUNK):
        for src in range(4):
            for tl in range(2):
                base = TILE_U * CHUNK_TILES[j][tl]
                rows = min(TILE_U, ROW_BLK - base)
                u0 = src * ROW_BLK + base
                for cs in range(2):
                    e2[j, src, tl, :rows, cs, :N_IMG] = parts[cs][u0:u0 + rows]
    return (jnp.asarray(e1.reshape(8 * Q_PAD, KV).astype(np.float32)).astype(BF16),
            jnp.asarray(e2.reshape(N_CHUNK * LANES, P_TWO).astype(np.float32)).astype(BF16))


def zero_kernel(*refs):
    *accs, token = refs

    def zero(i, _):
        for a in accs:
            a[pl.ds(pl.multiple_of(i * VS, 8), VS), :] = jnp.zeros((VS, LANES), F32)
        return 0
    lax.fori_loop(0, N_SRC, zero, 0)
    token[...] = jnp.zeros_like(token)


def exchange_kernel(_, y_hbm, wy_hbm, wx_hbm, iy_hbm, ix_hbm, e2_ref,
                    y_ref, wy_ref, wx_ref, addr_ref, roff_ref, e2f, *refs):
    y_in, iy, ix, y_send, in_sem, send_sem, recv_sem = refs
    k = lax.axis_index('cols')
    r = lax.axis_index('rows')
    other = {'cols': 1 - k}
    barrier = pltpu.get_barrier_semaphore()
    pl.semaphore_signal(barrier, inc=1, device_id=other, device_id_type=MESH)
    loads = [(iy_hbm, iy), (ix_hbm, ix), (y_hbm, y_in), (wy_hbm, wy_ref.at[0]), (wx_hbm, wx_ref.at[0])]
    loads = [pltpu.make_async_copy(a, b, in_sem.at[i]) for i, (a, b) in enumerate(loads)]
    for c in loads:
        c.start()

    def send(i, src, dst):
        c = pltpu.make_async_remote_copy(src_ref=src, dst_ref=dst, send_sem=send_sem.at[i], recv_sem=recv_sem.at[i],
                                         device_id=other, device_id_type=MESH)
        c.start()
        return c

    loads[0].wait()
    loads[1].wait()
    row = iy[...] - r * ROW_BLK
    tile = jnp.zeros_like(row)
    for t in range(1, N_SRC):
        tile = tile + jnp.where(row >= STRIDE_U * t, 1, 0)
    addr_ref[0] = tile * VS + (ix[...] - k * COL_BLK)
    roff_ref[0] = (row + 14) & 15
    loads[2].wait()
    y_re, y_im = y_in[0], y_in[1]
    low = jnp.concatenate([y_re[0:4], y_im[0:4]], axis=0)
    high = jnp.concatenate([y_re[4:8], y_im[4:8]], axis=0)
    y_ref[0] = jnp.where(k == 0, low, high)
    y_send[...] = jnp.where(k == 0, high, low)
    loads[3].wait()
    loads[4].wait()
    pl.semaphore_wait(barrier, 1)
    copies = [send(0, wy_ref.at[0], wy_ref.at[1]), send(1, wx_ref.at[0], wx_ref.at[1]), send(2, addr_ref.at[0], addr_ref.at[1]),
              send(3, roff_ref.at[0], roff_ref.at[1]), send(4, y_send, y_ref.at[1])]

    for j in range(N_CHUNK):
        for h in range(2):
            v = e2_ref[LANES * j + 64 * h:LANES * j + 64 * h + 64, :]
            e2f[j, LANES * h:LANES * h + 64, :] = v
            e2f[j, LANES * h + 64:LANES * h + LANES, 0:P_ALL] = -v[:, P_ALL:P_TWO]
            e2f[j, LANES * h + 64:LANES * h + LANES, P_ALL:P_TWO] = v[:, 0:P_ALL]
    for c in copies:
        c.wait()


def split3(x):
    hi = x.astype(BF16).astype(F32)
    rest = x - hi
    mid = rest.astype(BF16).astype(F32)
    return [hi, mid, rest - mid]


def spread_kernel(addr_ref, y_ref, wy_ref, wx_ref, roff_ref, *refs):
    accs = refs[N_ACC:4 * N_COPY]
    addr, sem = refs[4 * N_COPY], refs[-1]
    q_refs = refs[4 * N_COPY + 1:-1]
    to_smem = pltpu.make_async_copy(addr_ref, addr, sem)
    to_smem.start()
    n = y_ref.shape[2]

    r0 = lax.broadcasted_iota(jnp.int32, (80, WIDE), 0)
    l0 = lax.broadcasted_iota(jnp.int32, (80, WIDE), 1)
    ry = (r0 < 24) & (l0 < LANES) & ((r0 & 7) == (l0 >> 4))
    rw = (r0 >= 24) & (r0 < 72) & (l0 >= LANES) & (((r0 - 24) & 15) == (l0 & 15))
    expand = jnp.where(ry | rw, 1.0, 0.0).astype(BF16)
    rr = lax.broadcasted_iota(jnp.int32, (ROWS, WIDE), 0)
    n_blk = n // WIDE

    def prep(i, slot, q_ref):
        ds = [pl.ds(pl.multiple_of((i + n_blk * h) * LANES, LANES), LANES) for h in range(2)]
        y = jnp.concatenate([y_ref[slot, :, s] for s in ds], axis=1)
        wy = jnp.concatenate([wy_ref[slot, :, s] for s in ds], axis=1)
        d = (rr - jnp.concatenate([roff_ref[slot, pl.ds(i + n_blk * h, 1), :] for h in range(2)], axis=1)) & 15
        w16 = jnp.zeros((ROWS, WIDE), F32)
        for a in range(4):
            w16 = jnp.where(d == a, wy[a:a + 1], w16)
        lhs = jnp.concatenate(split3(y) + split3(w16) + [jnp.zeros((8, WIDE), F32)], axis=0).astype(BF16)
        o = lax.dot_general(lhs, expand, (((0,), (0,)), ((), ())), preferred_element_type=F32)
        q_ref[...] = o[:, :LANES] * o[:, LANES:]

    top = lax.broadcasted_iota(jnp.int32, (8, LANES), 0) < 4

    def scatter(i, qs):
        ds = [pl.ds(pl.multiple_of((i + n_blk * h) * LANES, LANES), LANES) for h in range(2)]
        wx = [jnp.concatenate([wx_ref[slot, :, s] for s in ds], axis=0) for slot in range(2)]
        for j in range(LANES):
            cols = [jnp.broadcast_to(wx[slot][:, j:j + 1], (8, LANES)) for slot in range(2)]
            for h in range(2):
                for slot in range(2):
                    acc = accs[slot * N_COPY + (2 * j + h) % N_COPY]
                    base = addr[slot, i + n_blk * h, j] + (0 if h else 4)
                    q = jnp.broadcast_to(qs[slot][j + LANES * h:j + LANES * h + 1, :], (8, LANES))
                    s = pl.ds(base, 8)
                    c = jnp.where(top, 0.0, cols[slot]) if h else jnp.where(top, cols[slot], 0.0)
                    acc[s, :] = acc[s, :] + c * q

    qa, qb = q_refs[:2], q_refs[2:]
    for slot in range(2):
        prep(0, slot, qa[slot])
    to_smem.wait()

    def two_blocks(i, _):
        for step, now, then in ((0, qa, qb), (1, qb, qa)):
            for slot in range(2):
                prep(lax.rem(2 * i + step + 1, n_blk), slot, then[slot])
            scatter(2 * i + step, now)
        return 0
    lax.fori_loop(0, n_blk // 2, two_blocks, 0)


def transform_kernel(*refs):
    own, nbr = refs[:N_COPY], refs[N_COPY:N_ACC]
    (e1_ref, e2f, s_ref, d_ref, out_ref, st, dd, gch, raw0, f0, f11, gps, gns, msg, recv, gpr, gnr, img, mine, psend, precv,
     msend_sem, mrecv_sem, gsend_sem, grecv_sem, psend_sem, precv_sem) = refs[N_ACC:]
    k = lax.axis_index('cols')
    r = lax.axis_index('rows')
    chip, core = r // 2, r % 2
    dests = [2 * (1 - chip) + core, 2 * (1 - chip) + (1 - core), 2 * chip + (1 - core)]
    nxt, prv = lax.rem(r + 1, 4), lax.rem(r + 3, 4)
    barrier = pltpu.get_barrier_semaphore()
    for d in dests:
        pl.semaphore_signal(barrier, inc=1, device_id={'rows': d}, device_id_type=MESH)
    pl.semaphore_signal(barrier, inc=1, device_id={'cols': 1 - k}, device_id_type=MESH)

    slots = ((own, k), (nbr, 1 - k))
    lane16 = lax.broadcasted_iota(jnp.int32, (ROWS, LANES), 1) & 15
    sub16 = lax.broadcasted_iota(jnp.int32, (ROWS, LANES), 0)

    def merged(accs, off, targets):
        wanted = {}
        for m in targets:
            deltas = {0: 0} if m is None else {t: STRIDE_U * t - TILE_U * m - 2 for t in range(N_SRC)}
            wanted[m] = {t: d for t, d in deltas.items() if abs(d) < ROWS}
        loaded = {}
        for t in sorted({t for w in wanted.values() for t in w}):
            s = pl.ds(t * VS + off, ROWS)
            v = accs[0][s, :]
            for acc in accs[1:]:
                v = v + acc[s, :]
            loaded[t] = v
        outs = []
        for m in targets:
            out = None
            for t, d in wanted[m].items():
                lo, hi = max(0, d), min(15, 15 + d)
                v = loaded[t]
                if lo > 0 or hi < 15:
                    v = jnp.where((lane16 >= lo) & (lane16 <= hi), v, 0.0)
                out = v if out is None else out + v
            outs.append(out)
        return outs

    def merge_all(targets, put):
        def rows(i, _):
            for step in range(2):
                for accs, half in slots:
                    off = pl.multiple_of((2 * i + 1 + step) * ROWS, ROWS)
                    put(pl.multiple_of(half * VR + off, ROWS), merged(accs, off, targets))
            return 0
        lax.fori_loop(0, VR // (2 * ROWS) - 1, rows, 0)
        last = VR - ROWS
        a = [merged(accs, 0, targets) for accs, _ in slots]
        b = [merged(accs, last, targets) for accs, _ in slots]
        for i, (_, half) in enumerate(slots):
            fix_a = [x + jnp.where(sub16 == 6, y, 0.0) for x, y in zip(a[i], b[1 - i])]
            fix_b = [y + jnp.where((sub16 == 4) | (sub16 == 5), x, 0.0) for x, y in zip(a[1 - i], b[i])]
            put(pl.multiple_of(half * VR, ROWS), fix_a)
            put(pl.multiple_of(half * VR + last, ROWS), fix_b)

    def put_chunk(off, vals):
        for i, v in enumerate(vals):
            gch[pl.ds(off, ROWS), LANES * i:LANES * (i + 1)] = v.astype(BF16)

    def put_edges(off, vals):
        for ref, v in zip((raw0, f0, f11), vals):
            ref[pl.ds(off, ROWS), :] = v

    lane = lax.broadcasted_iota(jnp.int32, (Q_PAD, WIDE), 1) & 127

    def swap(sub):
        rows = pl.ds(*SUBS[sub])
        return pltpu.make_async_remote_copy(src_ref=psend.at[rows], dst_ref=precv.at[rows], send_sem=psend_sem.at[sub],
                                            recv_sem=precv_sem.at[sub], device_id={'cols': 1 - k}, device_id_type=MESH)

    def first_dft(j, g):
        ab = jnp.dot(e1_ref[...], g, preferred_element_type=F32)
        for d in range(4):
            a = ab[192 * d:192 * d + Q_PAD]
            b = ab[192 * d + Q_PAD:192 * d + 192]
            b = jnp.concatenate([pltpu.roll(b[:, :128], 64, 1), pltpu.roll(b[:, 128:], 64, 1)], axis=1)
            msg[j, d] = jnp.where(lane < 64, a - b, a + b).astype(BF16)

    def copy_of(j, sub, i, slot):
        d = dests[i]
        rows = pl.ds(*SUBS[sub])
        return pltpu.make_async_remote_copy(src_ref=msg.at[j, d, rows], dst_ref=recv.at[j, slot, rows], send_sem=msend_sem.at[j, sub, i],
                                            recv_sem=mrecv_sem.at[j, sub, slot], device_id={'rows': d}, device_id_type=MESH)

    def post(chunk):
        for j, sub in POSTS[chunk]:
            for i in range(3):
                copy_of(j, sub, i, r).start()
        if chunk < N_CHUNK:
            recv[chunk, r] = msg[chunk, r]

    merge_all(CHUNK_TILES[0], put_chunk)
    first_dft(0, gch[...])
    pl.semaphore_wait(barrier, 4)
    post(0)

    merge_all((None, 0, N_TGT - 1), put_edges)
    la = lax.broadcasted_iota(jnp.int32, (Q_PAD, LANES), 1) & 15
    lb = lax.broadcasted_iota(jnp.int32, (GN_ROWS, LANES), 1) & 15

    def shifted(v, by):
        return pltpu.roll(v, by % LANES, 1) if by else v

    gp = jnp.zeros((Q_PAD, LANES), F32)
    for c in range(8):
        gp = jnp.where((la >> 1) == c, shifted(raw0[Q_PAD * c:Q_PAD * c + Q_PAD, :], 2 * c - 14), gp)
    gps[...] = gp
    gn = jnp.zeros((GN_ROWS, LANES), F32)
    for c in range(16):
        gn = jnp.where(lb == c, shifted(f11[GN_ROWS * c:GN_ROWS * c + GN_ROWS, :], c - 8), gn)
    gns[...] = gn
    to_prv = pltpu.make_async_remote_copy(src_ref=gps, dst_ref=gpr, send_sem=gsend_sem.at[0], recv_sem=grecv_sem.at[0],
                                          device_id={'rows': prv}, device_id_type=MESH)
    to_nxt = pltpu.make_async_remote_copy(src_ref=gns, dst_ref=gnr, send_sem=gsend_sem.at[1], recv_sem=grecv_sem.at[1],
                                          device_id={'rows': nxt}, device_id_type=MESH)
    to_prv.start()
    to_nxt.start()

    for j in range(1, N_CHUNK - 1):
        merge_all(CHUNK_TILES[j], put_chunk)
        first_dft(j, gch[...])
        post(j)

    to_prv.wait()
    to_nxt.wait()
    gp, gn = gpr[...], gnr[...]
    for c in range(8):
        s = slice(Q_PAD * c, Q_PAD * c + Q_PAD)
        gch[s, LANES:WIDE] = (f11[s, :] + jnp.where((la >> 1) == 3, shifted(gp, 6 - 2 * c), 0.0)).astype(BF16)
    for c in range(16):
        s = slice(GN_ROWS * c, GN_ROWS * c + GN_ROWS)
        gch[s, 0:LANES] = (f0[s, :] + jnp.where(lb == 0, shifted(gn, -c), 0.0)).astype(BF16)
    first_dft(N_CHUNK - 1, gch[...])
    post(N_CHUNK - 1)

    d_all = d_ref[...].reshape(1, N_IMG)
    st[...] = jnp.zeros_like(st)
    for s in range(2):
        for c in range(4):
            st[s, c, 0:Q_BLK, 0:N_IMG] = s_ref[s, :, c, :]

    half_p = jnp.where(k == 0, d_all[:, 0:P_BLK], d_all[:, P_BLK:2 * P_BLK])
    part_q = d_all[:, 0:Q_BLK]
    for i in range(1, 4):
        part_q = jnp.where(r == i, d_all[:, Q_BLK * i:Q_BLK * (i + 1)], part_q)
    part_q = jnp.concatenate([part_q, jnp.zeros((1, LANES - Q_BLK), F32)], axis=1)
    dd[...] = jnp.broadcast_to(part_q, (8, LANES)).T[0:Q_BLK, 0:1] * half_p

    first_col = k == 0

    def second_dft(j, sub):
        row0, rows = SUBS[sub]
        for i in range(3):
            copy_of(j, sub, i, dests[i]).wait_recv()
        coil = (lax.broadcasted_iota(jnp.int32, (rows, LANES), 1) >> 4) & 3
        halves = []
        for pair in range(2):
            v = [recv[j, 2 * pair + t // 2, pl.ds(row0, rows), LANES * (t % 2):LANES * (t % 2 + 1)] for t in range(4)]
            for bit in (1, 2):
                m = (coil & bit) == 0
                for t in range(4):
                    if t & bit:
                        continue
                    x, y = v[t], v[t | bit]
                    v[t] = jnp.where(m, x, pltpu.roll(y, ROWS * bit, 1))
                    v[t | bit] = jnp.where(m, pltpu.roll(x, LANES - ROWS * bit, 1), y)
            halves.append(v)
        lhs = jnp.concatenate([jnp.concatenate([halves[0][c], halves[1][c]], axis=1) for c in range(4)], axis=0)
        return jnp.dot(lhs, e2f[j], preferred_element_type=F32)

    img[...] = second_dft(0, FULL)
    for j in WHOLE[1:]:
        img[...] += second_dft(j, FULL)
    for sub in range(2):
        row0, rows = SUBS[sub]

        def accumulate(j, _):
            part = second_dft(j, sub)
            for c in range(4):
                img[Q_PAD * c + row0:Q_PAD * c + row0 + rows] += part[rows * c:rows * (c + 1)]
            return 0
        lax.fori_loop(N_WHOLE, N_CHUNK - 1, accumulate, 0)
        if sub == 0:
            post(N_CHUNK)
        accumulate(N_CHUNK - 1, 0)

        x_re = jnp.zeros((rows, P_ALL), F32)
        x_im = jnp.zeros((rows, P_ALL), F32)
        for c in range(4):
            i_re = img[Q_PAD * c + row0:Q_PAD * c + row0 + rows, 0:P_ALL]
            i_im = img[Q_PAD * c + row0:Q_PAD * c + row0 + rows, P_ALL:P_TWO]
            s_re, s_im = st[0, c, row0:row0 + rows], st[1, c, row0:row0 + rows]
            x_re = x_re + s_re * i_re + s_im * i_im
            x_im = x_im + s_re * i_im - s_im * i_re
        lo = jnp.concatenate([x_re[:, 0:P_PAD], x_im[:, 0:P_PAD]], axis=1)
        hi = jnp.concatenate([x_re[:, P_BLK:P_BLK + P_PAD], x_im[:, P_BLK:P_BLK + P_PAD]], axis=1)
        psend[row0:row0 + rows] = jnp.where(first_col, hi, lo)
        swap(sub).start()
        mine[row0:row0 + rows] = jnp.where(first_col, lo, hi)

    for j, sub in SENT:
        for i in range(3):
            copy_of(j, sub, i, r).wait_send()
    for sub in range(2):
        swap(sub).wait()
    total = mine[...] + precv[...]
    out_ref[0] = (total[0:Q_BLK, 0:P_BLK] * dd[...]).T
    out_ref[1] = (total[0:Q_BLK, P_PAD:P_PAD + P_BLK] * dd[...]).T


def solution(mesh):
    sample_spec = ('exam', 'rows', 'cols')
    vmem = pl.BlockSpec(memory_space=pltpu.VMEM)
    hbm = pl.BlockSpec(memory_space=pltpu.HBM)
    sds = jax.ShapeDtypeStruct

    def local_fn(kspace, wts_y, wts_x, idx_y, idx_x, coil_maps, deapod):
        n = kspace.shape[2]
        e1, e2 = dft_constants()
        maps = jnp.transpose(coil_maps, (0, 3, 1, 2))
        acc_shape = [sds((N_SRC * VS, LANES), F32)] * (N_ACC)
        *accs, token = pl.pallas_call(
            zero_kernel,
            out_shape=acc_shape + [sds((8, LANES), F32)],
            out_specs=[vmem] * (N_ACC + 1),
            compiler_params=pltpu.CompilerParams(vmem_limit_bytes=MIB),
            cost_estimate=pl.CostEstimate(flops=2 * 10**9, bytes_accessed=2 * 10**7, transcendentals=0),
            name='zero',
        )()
        samples = pl.pallas_call(
            exchange_kernel,
            out_shape=[sds((2, 8, n), F32), sds((2, 4, n), F32), sds((2, 4, n), F32), sds((2, 16, LANES), jnp.int32),
                       sds((2, 16, LANES), jnp.int32), sds((N_CHUNK, WIDE, P_TWO), BF16)],
            in_specs=[vmem] + [hbm] * 5 + [vmem],
            out_specs=[vmem] * 6,
            scratch_shapes=[pltpu.VMEM((2, 8, n), F32), pltpu.VMEM((16, LANES), jnp.int32), pltpu.VMEM((16, LANES), jnp.int32),
                            pltpu.VMEM((8, n), F32), pltpu.SemaphoreType.DMA((5,)), pltpu.SemaphoreType.DMA((5,)),
                            pltpu.SemaphoreType.DMA((5,))],
            compiler_params=pltpu.CompilerParams(collective_id=0, has_side_effects=True, vmem_limit_bytes=8 * MIB),
            name='exchange',
        )(token, kspace, wts_y, wts_x, idx_y.reshape(16, LANES), idx_x.reshape(16, LANES), e2)
        y8, wy, wx, addr, roff, e2f = samples
        accs = pl.pallas_call(
            spread_kernel,
            out_shape=acc_shape,
            in_specs=[vmem] * (5 + N_ACC),
            out_specs=[vmem] * (N_ACC),
            scratch_shapes=[pltpu.SMEM((2, 16, LANES), jnp.int32)] + [pltpu.VMEM((WIDE, LANES), F32)] * 4 + [pltpu.SemaphoreType.DMA],
            input_output_aliases={5 + i: i for i in range(N_ACC)},
            compiler_params=pltpu.CompilerParams(vmem_limit_bytes=8 * MIB),
            cost_estimate=pl.CostEstimate(flops=2 * 10**9, bytes_accessed=2 * 10**7, transcendentals=0),
            name='spread',
        )(addr, y8, wy, wx, roff, *accs)
        return pl.pallas_call(
            transform_kernel,
            out_shape=sds((2, P_BLK, Q_BLK), F32),
            in_specs=[vmem] * (N_ACC + 4),
            out_specs=vmem,
            scratch_shapes=[pltpu.VMEM((2, 4, Q_PAD, P_ALL), F32), pltpu.VMEM((Q_BLK, P_BLK), F32), pltpu.VMEM((KV, WIDE), BF16)] + [pltpu.VMEM((KV, LANES), F32)] * 3 + [
                pltpu.VMEM((Q_PAD, LANES), F32),
                pltpu.VMEM((GN_ROWS, LANES), F32),
                pltpu.VMEM((N_CHUNK, 4, Q_PAD, WIDE), BF16),
                pltpu.VMEM((N_CHUNK, 4, Q_PAD, WIDE), BF16),
                pltpu.VMEM((Q_PAD, LANES), F32),
                pltpu.VMEM((GN_ROWS, LANES), F32),
                pltpu.VMEM((4 * Q_PAD, P_TWO), F32),
                pltpu.VMEM((Q_PAD, P_ALL), F32),
                pltpu.VMEM((Q_PAD, P_ALL), F32),
                pltpu.VMEM((Q_PAD, P_ALL), F32),
                pltpu.SemaphoreType.DMA((N_CHUNK, len(SUBS), 3)),
                pltpu.SemaphoreType.DMA((N_CHUNK, len(SUBS), 4)),
                pltpu.SemaphoreType.DMA((2,)),
                pltpu.SemaphoreType.DMA((2,)),
                pltpu.SemaphoreType.DMA((len(SUBS),)),
                pltpu.SemaphoreType.DMA((len(SUBS),)),
            ],
            compiler_params=pltpu.CompilerParams(collective_id=1, has_side_effects=True, vmem_limit_bytes=24 * MIB),
            name='transform',
        )(*accs, e1, e2f, maps, deapod)

    return jax.shard_map(
        local_fn,
        mesh=mesh,
        in_specs=(P(None, None, sample_spec), P(None, sample_spec), P(None, sample_spec), P(sample_spec), P(sample_spec), P(None, ('exam', 'cols'), None, 'rows'), P()),
        out_specs=P(None, ('exam', 'cols'), 'rows'),
        check_vma=False,
    )
```

```python
import math

import jax
import jax.numpy as jnp
import numpy as np
from jax import lax
from jax.experimental import pallas as pl
from jax.experimental.pallas import tpu as pltpu
from jax.sharding import PartitionSpec as P

F32, BF16 = jnp.float32, jnp.bfloat16
MESH = pl.DeviceIdType.MESH

N_IMG = 368
N_GRID = 736
ROW_BLK = 184
Q_BLK, Q_PAD = 92, 96
P_BLK, P_PAD, P_ALL = 184, 192, 384
N_CH = 8
TILE_U, STRIDE_U, N_SRC = 16, 13, 15
N_TGT = 12
COL_BLK = 368
VR = 384
VS = 392
KV = 2 * VR
LANES, ROWS = 128, 16
EDGE = 6
WIDE, P_TWO, GN_ROWS, MIB = 2 * LANES, 2 * P_ALL, 48, 2**20
N_CHUNK = 6
N_COPY = 3
N_ACC = 2 * N_COPY
SUBS = [(0, 64), (64, 32), (0, Q_PAD)]
FULL, N_WHOLE = 2, 2
WHOLE, SPLIT = range(N_WHOLE), range(N_WHOLE, N_CHUNK)
POSTS = [[(j, FULL)] for j in WHOLE] + [[(j, 0)] for j in SPLIT]
POSTS += [[(j, 1) for j in SPLIT]]
LAST = N_CHUNK - 1
SUBS_LAST = [(0, 96), (96, 48)]
SENT = [(j, FULL) for j in WHOLE] + [(j, sub) for j in SPLIT for sub in range(2)]
CHUNK_TILES = [(1 + 2 * j, 2 + 2 * j) for j in range(5)] + [(0, 11)]


def dft_constants():
    scale = 1.0 / math.sqrt(N_GRID)
    phase = ((np.arange(N_GRID)[:, None] - N_GRID // 2) * (np.arange(N_IMG)[None, :] - N_IMG // 2)) % N_GRID
    ang = phase.astype(np.float64) * (2.0 * math.pi / N_GRID)
    parts = (np.cos(ang) * scale, np.sin(ang) * scale)
    e1 = np.zeros((4, 2, Q_PAD, 2, VR))
    for dest in range(4):
        for cs in range(2):
            for half in range(2):
                part = parts[cs][half * COL_BLK:(half + 1) * COL_BLK, dest * Q_BLK:(dest + 1) * Q_BLK]
                e1[dest, cs, :Q_BLK, half, EDGE:EDGE + COL_BLK] = part.T
    e2 = np.zeros((N_CHUNK, 4, 2, TILE_U, 2, P_ALL))
    for j in range(N_CHUNK):
        for src in range(4):
            for tl in range(2):
                base = TILE_U * CHUNK_TILES[j][tl]
                rows = min(TILE_U, ROW_BLK - base)
                u0 = src * ROW_BLK + base
                for cs in range(2):
                    e2[j, src, tl, :rows, cs, :N_IMG] = parts[cs][u0:u0 + rows]
    return (jnp.asarray(e1.reshape(8 * Q_PAD, KV).astype(np.float32)).astype(BF16),
            jnp.asarray(e2.reshape(N_CHUNK * LANES, P_TWO).astype(np.float32)).astype(BF16))


def j_is_last(j):
    return isinstance(j, int) and j == LAST


def zero_kernel(*refs):
    *accs, token = refs

    def zero(i, _):
        for a in accs:
            a[pl.ds(pl.multiple_of(i * VS, 8), VS), :] = jnp.zeros((VS, LANES), F32)
        return 0
    lax.fori_loop(0, N_SRC, zero, 0)
    token[...] = jnp.zeros_like(token)


def exchange_kernel(_, y_hbm, wy_hbm, wx_hbm, iy_hbm, ix_hbm, e2_ref,
                    y_ref, wy_ref, wx_ref, addr_ref, roff_ref, e2f, *refs):
    y_in, iy, ix, y_send, in_sem, send_sem, recv_sem = refs
    k = lax.axis_index('cols')
    r = lax.axis_index('rows')
    other = {'cols': 1 - k}
    barrier = pltpu.get_barrier_semaphore()
    pl.semaphore_signal(barrier, inc=1, device_id=other, device_id_type=MESH)
    loads = [(iy_hbm, iy), (ix_hbm, ix), (y_hbm, y_in), (wy_hbm, wy_ref.at[0]), (wx_hbm, wx_ref.at[0])]
    loads = [pltpu.make_async_copy(a, b, in_sem.at[i]) for i, (a, b) in enumerate(loads)]
    for c in loads:
        c.start()

    def send(i, src, dst):
        c = pltpu.make_async_remote_copy(src_ref=src, dst_ref=dst, send_sem=send_sem.at[i], recv_sem=recv_sem.at[i],
                                         device_id=other, device_id_type=MESH)
        c.start()
        return c

    loads[0].wait()
    loads[1].wait()
    row = iy[...] - r * ROW_BLK
    tile = jnp.zeros_like(row)
    for t in range(1, N_SRC):
        tile = tile + jnp.where(row >= STRIDE_U * t, 1, 0)
    addr_ref[0] = tile * VS + (ix[...] - k * COL_BLK)
    roff_ref[0] = (row + 14) & 15
    loads[2].wait()
    y_re, y_im = y_in[0], y_in[1]
    low = jnp.concatenate([y_re[0:4], y_im[0:4]], axis=0)
    high = jnp.concatenate([y_re[4:8], y_im[4:8]], axis=0)
    y_ref[0] = jnp.where(k == 0, low, high)
    y_send[...] = jnp.where(k == 0, high, low)
    loads[3].wait()
    loads[4].wait()
    pl.semaphore_wait(barrier, 1)
    copies = [send(0, wy_ref.at[0], wy_ref.at[1]), send(1, wx_ref.at[0], wx_ref.at[1]), send(2, addr_ref.at[0], addr_ref.at[1]),
              send(3, roff_ref.at[0], roff_ref.at[1]), send(4, y_send, y_ref.at[1])]

    for j in range(N_CHUNK):
        for h in range(2):
            v = e2_ref[LANES * j + 64 * h:LANES * j + 64 * h + 64, :]
            e2f[j, LANES * h:LANES * h + 64, :] = v
            e2f[j, LANES * h + 64:LANES * h + LANES, 0:P_ALL] = -v[:, P_ALL:P_TWO]
            e2f[j, LANES * h + 64:LANES * h + LANES, P_ALL:P_TWO] = v[:, 0:P_ALL]
    for c in copies:
        c.wait()


def split3(x):
    hi = x.astype(BF16).astype(F32)
    rest = x - hi
    mid = rest.astype(BF16).astype(F32)
    return [hi, mid, rest - mid]


def spread_kernel(addr_ref, y_ref, wy_ref, wx_ref, roff_ref, *refs):
    accs = refs[N_ACC:4 * N_COPY]
    addr, sem = refs[4 * N_COPY], refs[-1]
    q_refs = refs[4 * N_COPY + 1:-1]
    to_smem = pltpu.make_async_copy(addr_ref, addr, sem)
    to_smem.start()
    n = y_ref.shape[2]

    r0 = lax.broadcasted_iota(jnp.int32, (80, WIDE), 0)
    l0 = lax.broadcasted_iota(jnp.int32, (80, WIDE), 1)
    ry = (r0 < 24) & (l0 < LANES) & ((r0 & 7) == (l0 >> 4))
    rw = (r0 >= 24) & (r0 < 72) & (l0 >= LANES) & (((r0 - 24) & 15) == (l0 & 15))
    expand = jnp.where(ry | rw, 1.0, 0.0).astype(BF16)
    rr = lax.broadcasted_iota(jnp.int32, (ROWS, WIDE), 0)
    n_blk = n // WIDE

    def prep(i, slot, q_ref):
        ds = [pl.ds(pl.multiple_of((i + n_blk * h) * LANES, LANES), LANES) for h in range(2)]
        y = jnp.concatenate([y_ref[slot, :, s] for s in ds], axis=1)
        wy = jnp.concatenate([wy_ref[slot, :, s] for s in ds], axis=1)
        d = (rr - jnp.concatenate([roff_ref[slot, pl.ds(i + n_blk * h, 1), :] for h in range(2)], axis=1)) & 15
        w16 = jnp.zeros((ROWS, WIDE), F32)
        for a in range(4):
            w16 = jnp.where(d == a, wy[a:a + 1], w16)
        lhs = jnp.concatenate(split3(y) + split3(w16) + [jnp.zeros((8, WIDE), F32)], axis=0).astype(BF16)
        o = lax.dot_general(lhs, expand, (((0,), (0,)), ((), ())), preferred_element_type=F32)
        q_ref[...] = o[:, :LANES] * o[:, LANES:]

    top = lax.broadcasted_iota(jnp.int32, (8, LANES), 0) < 4

    def scatter(i, qs):
        ds = [pl.ds(pl.multiple_of((i + n_blk * h) * LANES, LANES), LANES) for h in range(2)]
        wx = [jnp.concatenate([wx_ref[slot, :, s] for s in ds], axis=0) for slot in range(2)]
        for j in range(LANES):
            cols = [jnp.broadcast_to(wx[slot][:, j:j + 1], (8, LANES)) for slot in range(2)]
            for h in range(2):
                for slot in range(2):
                    acc = accs[slot * N_COPY + (2 * j + h) % N_COPY]
                    base = addr[slot, i + n_blk * h, j] + (0 if h else 4)
                    q = jnp.broadcast_to(qs[slot][j + LANES * h:j + LANES * h + 1, :], (8, LANES))
                    s = pl.ds(base, 8)
                    c = jnp.where(top, 0.0, cols[slot]) if h else jnp.where(top, cols[slot], 0.0)
                    acc[s, :] = acc[s, :] + c * q

    qa, qb = q_refs[:2], q_refs[2:]
    for slot in range(2):
        prep(0, slot, qa[slot])
    to_smem.wait()

    def two_blocks(i, _):
        for step, now, then in ((0, qa, qb), (1, qb, qa)):
            for slot in range(2):
                prep(lax.rem(2 * i + step + 1, n_blk), slot, then[slot])
            scatter(2 * i + step, now)
        return 0
    lax.fori_loop(0, n_blk // 2, two_blocks, 0)


def transform_kernel(*refs):
    own, nbr = refs[:N_COPY], refs[N_COPY:N_ACC]
    (e1_ref, e2f, s_ref, d_ref, out_ref, st, dd, gch, raw0, f0, f11, gps, gns, msg, recv, msg_last, recv_last, gpr, gnr, img, mine, psend, precv,
     msend_sem, mrecv_sem, gsend_sem, grecv_sem, psend_sem, precv_sem) = refs[N_ACC:]
    k = lax.axis_index('cols')
    r = lax.axis_index('rows')
    chip, core = r // 2, r % 2
    dests = [2 * (1 - chip) + core, 2 * (1 - chip) + (1 - core), 2 * chip + (1 - core)]
    nxt, prv = lax.rem(r + 1, 4), lax.rem(r + 3, 4)
    barrier = pltpu.get_barrier_semaphore()
    for d in dests:
        pl.semaphore_signal(barrier, inc=1, device_id={'rows': d}, device_id_type=MESH)
    pl.semaphore_signal(barrier, inc=1, device_id={'cols': 1 - k}, device_id_type=MESH)

    slots = ((own, k), (nbr, 1 - k))
    lane16 = lax.broadcasted_iota(jnp.int32, (ROWS, LANES), 1) & 15
    sub16 = lax.broadcasted_iota(jnp.int32, (ROWS, LANES), 0)

    def merged(accs, off, targets):
        wanted = {}
        for m in targets:
            deltas = {0: 0} if m is None else {t: STRIDE_U * t - TILE_U * m - 2 for t in range(N_SRC)}
            wanted[m] = {t: d for t, d in deltas.items() if abs(d) < ROWS}
        loaded = {}
        for t in sorted({t for w in wanted.values() for t in w}):
            s = pl.ds(t * VS + off, ROWS)
            v = accs[0][s, :]
            for acc in accs[1:]:
                v = v + acc[s, :]
            loaded[t] = v
        outs = []
        for m in targets:
            out = None
            for t, d in wanted[m].items():
                lo, hi = max(0, d), min(15, 15 + d)
                v = loaded[t]
                if lo > 0 or hi < 15:
                    v = jnp.where((lane16 >= lo) & (lane16 <= hi), v, 0.0)
                out = v if out is None else out + v
            outs.append(out)
        return outs

    def merge_all(targets, put):
        def rows(i, _):
            for step in range(2):
                for accs, half in slots:
                    off = pl.multiple_of((2 * i + 1 + step) * ROWS, ROWS)
                    put(pl.multiple_of(half * VR + off, ROWS), merged(accs, off, targets))
            return 0
        lax.fori_loop(0, VR // (2 * ROWS) - 1, rows, 0)
        last = VR - ROWS
        a = [merged(accs, 0, targets) for accs, _ in slots]
        b = [merged(accs, last, targets) for accs, _ in slots]
        for i, (_, half) in enumerate(slots):
            fix_a = [x + jnp.where(sub16 == 6, y, 0.0) for x, y in zip(a[i], b[1 - i])]
            fix_b = [y + jnp.where((sub16 == 4) | (sub16 == 5), x, 0.0) for x, y in zip(a[1 - i], b[i])]
            put(pl.multiple_of(half * VR, ROWS), fix_a)
            put(pl.multiple_of(half * VR + last, ROWS), fix_b)

    def put_chunk(off, vals):
        for i, v in enumerate(vals):
            gch[pl.ds(off, ROWS), LANES * i:LANES * (i + 1)] = v.astype(BF16)

    def put_edges(off, vals):
        for ref, v in zip((raw0, f0, f11), vals):
            ref[pl.ds(off, ROWS), :] = v

    lane = lax.broadcasted_iota(jnp.int32, (Q_PAD, WIDE), 1) & 127

    def swap(sub):
        rows = pl.ds(*SUBS[sub])
        return pltpu.make_async_remote_copy(src_ref=psend.at[rows], dst_ref=precv.at[rows], send_sem=psend_sem.at[sub],
                                            recv_sem=precv_sem.at[sub], device_id={'cols': 1 - k}, device_id_type=MESH)

    def first_dft(j, g):
        ab = jnp.dot(e1_ref[...], g, preferred_element_type=F32)
        for d in range(4):
            a = ab[192 * d:192 * d + Q_PAD]
            b = ab[192 * d + Q_PAD:192 * d + 192]
            b = jnp.concatenate([pltpu.roll(b[:, :128], 64, 1), pltpu.roll(b[:, 128:], 64, 1)], axis=1)
            h = jnp.where(lane < 64, a - b, a + b).astype(BF16)
            if not j_is_last(j):
                msg[j, d] = h
                continue
            for sub, (at, _) in enumerate(SUBS_LAST):
                row0, rows = SUBS[sub]
                half = rows // 2
                upper = h[row0:row0 + half, LANES:WIDE]
                lower = pltpu.roll(h[row0 + half:row0 + rows, LANES:WIDE], 8, 1)
                msg_last[d, at:at + rows] = h[row0:row0 + rows, 0:LANES]
                msg_last[d, at + rows:at + rows + half] = jnp.where((lane[0:half, 0:LANES] & 8) == 0, upper, lower)

    def copy_of(j, sub, i, slot):
        d = dests[i]
        if j_is_last(j):
            rows = pl.ds(*SUBS_LAST[sub])
            src, dst = msg_last.at[d, rows], recv_last.at[slot, rows]
        else:
            rows = pl.ds(*SUBS[sub])
            src, dst = msg.at[j, d, rows], recv.at[j, slot, rows]
        return pltpu.make_async_remote_copy(src_ref=src, dst_ref=dst, send_sem=msend_sem.at[j, sub, i],
                                            recv_sem=mrecv_sem.at[j, sub, slot], device_id={'rows': d}, device_id_type=MESH)

    def post(chunk):
        for j, sub in POSTS[chunk]:
            for i in range(3):
                copy_of(j, sub, i, r).start()
        if chunk < LAST:
            recv[chunk, r] = msg[chunk, r]
        elif chunk == LAST:
            recv_last[r] = msg_last[r]

    merge_all(CHUNK_TILES[0], put_chunk)
    first_dft(0, gch[...])
    pl.semaphore_wait(barrier, 4)
    post(0)

    merge_all((None, 0, N_TGT - 1), put_edges)
    la = lax.broadcasted_iota(jnp.int32, (Q_PAD, LANES), 1) & 15
    lb = lax.broadcasted_iota(jnp.int32, (GN_ROWS, LANES), 1) & 15

    def shifted(v, by):
        return pltpu.roll(v, by % LANES, 1) if by else v

    gp = jnp.zeros((Q_PAD, LANES), F32)
    for c in range(8):
        gp = jnp.where((la >> 1) == c, shifted(raw0[Q_PAD * c:Q_PAD * c + Q_PAD, :], 2 * c - 14), gp)
    gps[...] = gp
    gn = jnp.zeros((GN_ROWS, LANES), F32)
    for c in range(16):
        gn = jnp.where(lb == c, shifted(f11[GN_ROWS * c:GN_ROWS * c + GN_ROWS, :], c - 8), gn)
    gns[...] = gn
    to_prv = pltpu.make_async_remote_copy(src_ref=gps, dst_ref=gpr, send_sem=gsend_sem.at[0], recv_sem=grecv_sem.at[0],
                                          device_id={'rows': prv}, device_id_type=MESH)
    to_nxt = pltpu.make_async_remote_copy(src_ref=gns, dst_ref=gnr, send_sem=gsend_sem.at[1], recv_sem=grecv_sem.at[1],
                                          device_id={'rows': nxt}, device_id_type=MESH)
    to_prv.start()
    to_nxt.start()

    for j in range(1, N_CHUNK - 1):
        merge_all(CHUNK_TILES[j], put_chunk)
        first_dft(j, gch[...])
        post(j)

    to_prv.wait()
    to_nxt.wait()
    gp, gn = gpr[...], gnr[...]
    for c in range(8):
        s = slice(Q_PAD * c, Q_PAD * c + Q_PAD)
        gch[s, LANES:WIDE] = (f11[s, :] + jnp.where((la >> 1) == 3, shifted(gp, 6 - 2 * c), 0.0)).astype(BF16)
    for c in range(16):
        s = slice(GN_ROWS * c, GN_ROWS * c + GN_ROWS)
        gch[s, 0:LANES] = (f0[s, :] + jnp.where(lb == 0, shifted(gn, -c), 0.0)).astype(BF16)
    first_dft(LAST, gch[...])
    post(LAST)

    d_all = d_ref[...].reshape(1, N_IMG)
    st[...] = jnp.zeros_like(st)
    for s in range(2):
        for c in range(4):
            st[s, c, 0:Q_BLK, 0:N_IMG] = s_ref[s, :, c, :]

    half_p = jnp.where(k == 0, d_all[:, 0:P_BLK], d_all[:, P_BLK:2 * P_BLK])
    part_q = d_all[:, 0:Q_BLK]
    for i in range(1, 4):
        part_q = jnp.where(r == i, d_all[:, Q_BLK * i:Q_BLK * (i + 1)], part_q)
    part_q = jnp.concatenate([part_q, jnp.zeros((1, LANES - Q_BLK), F32)], axis=1)
    dd[...] = jnp.broadcast_to(part_q, (8, LANES)).T[0:Q_BLK, 0:1] * half_p

    first_col = k == 0

    def second_dft(j, sub):
        row0, rows = SUBS[sub]
        for i in range(3):
            copy_of(j, sub, i, dests[i]).wait_recv()
        coil = (lax.broadcasted_iota(jnp.int32, (rows, LANES), 1) >> 4) & 3
        halves = []
        for pair in range(2):
            v = []
            for src in (2 * pair, 2 * pair + 1):
                if j_is_last(j):
                    at = SUBS_LAST[sub][0]
                    folded = recv_last[src, at + rows:at + rows + rows // 2]
                    v += [recv_last[src, at:at + rows], jnp.concatenate([folded, pltpu.roll(folded, LANES - 8, 1)], axis=0)]
                else:
                    v += [recv[j, src, pl.ds(row0, rows), LANES * t:LANES * (t + 1)] for t in range(2)]
            for bit in (1, 2):
                m = (coil & bit) == 0
                for t in range(4):
                    if t & bit:
                        continue
                    x, y = v[t], v[t | bit]
                    v[t] = jnp.where(m, x, pltpu.roll(y, ROWS * bit, 1))
                    v[t | bit] = jnp.where(m, pltpu.roll(x, LANES - ROWS * bit, 1), y)
            halves.append(v)
        lhs = jnp.concatenate([jnp.concatenate([halves[0][c], halves[1][c]], axis=1) for c in range(4)], axis=0)
        return jnp.dot(lhs, e2f[j], preferred_element_type=F32)

    img[...] = second_dft(0, FULL)
    for j in WHOLE[1:]:
        img[...] += second_dft(j, FULL)
    for sub in range(2):
        row0, rows = SUBS[sub]

        def accumulate(j, _):
            part = second_dft(j, sub)
            for c in range(4):
                img[Q_PAD * c + row0:Q_PAD * c + row0 + rows] += part[rows * c:rows * (c + 1)]
            return 0
        lax.fori_loop(N_WHOLE, N_WHOLE + 1, accumulate, 0)
        if sub == 0:
            post(N_CHUNK)
        lax.fori_loop(N_WHOLE + 1, LAST, accumulate, 0)
        accumulate(LAST, 0)

        x_re = jnp.zeros((rows, P_ALL), F32)
        x_im = jnp.zeros((rows, P_ALL), F32)
        for c in range(4):
            i_re = img[Q_PAD * c + row0:Q_PAD * c + row0 + rows, 0:P_ALL]
            i_im = img[Q_PAD * c + row0:Q_PAD * c + row0 + rows, P_ALL:P_TWO]
            s_re, s_im = st[0, c, row0:row0 + rows], st[1, c, row0:row0 + rows]
            x_re = x_re + s_re * i_re + s_im * i_im
            x_im = x_im + s_re * i_im - s_im * i_re
        lo = jnp.concatenate([x_re[:, 0:P_PAD], x_im[:, 0:P_PAD]], axis=1)
        hi = jnp.concatenate([x_re[:, P_BLK:P_BLK + P_PAD], x_im[:, P_BLK:P_BLK + P_PAD]], axis=1)
        psend[row0:row0 + rows] = jnp.where(first_col, hi, lo)
        swap(sub).start()
        mine[row0:row0 + rows] = jnp.where(first_col, lo, hi)

    for j, sub in SENT:
        for i in range(3):
            copy_of(j, sub, i, r).wait_send()
    for sub in range(2):
        swap(sub).wait()
    total = mine[...] + precv[...]
    out_ref[0] = (total[0:Q_BLK, 0:P_BLK] * dd[...]).T
    out_ref[1] = (total[0:Q_BLK, P_PAD:P_PAD + P_BLK] * dd[...]).T


def solution(mesh):
    sample_spec = ('exam', 'rows', 'cols')
    vmem = pl.BlockSpec(memory_space=pltpu.VMEM)
    hbm = pl.BlockSpec(memory_space=pltpu.HBM)
    sds = jax.ShapeDtypeStruct

    def local_fn(kspace, wts_y, wts_x, idx_y, idx_x, coil_maps, deapod):
        n = kspace.shape[2]
        e1, e2 = dft_constants()
        maps = jnp.transpose(coil_maps, (0, 3, 1, 2))
        acc_shape = [sds((N_SRC * VS, LANES), F32)] * (N_ACC)
        *accs, token = pl.pallas_call(
            zero_kernel,
            out_shape=acc_shape + [sds((8, LANES), F32)],
            out_specs=[vmem] * (N_ACC + 1),
            compiler_params=pltpu.CompilerParams(vmem_limit_bytes=MIB),
            cost_estimate=pl.CostEstimate(flops=2 * 10**9, bytes_accessed=2 * 10**7, transcendentals=0),
            name='zero',
        )()
        samples = pl.pallas_call(
            exchange_kernel,
            out_shape=[sds((2, 8, n), F32), sds((2, 4, n), F32), sds((2, 4, n), F32), sds((2, 16, LANES), jnp.int32),
                       sds((2, 16, LANES), jnp.int32), sds((N_CHUNK, WIDE, P_TWO), BF16)],
            in_specs=[vmem] + [hbm] * 5 + [vmem],
            out_specs=[vmem] * 6,
            scratch_shapes=[pltpu.VMEM((2, 8, n), F32), pltpu.VMEM((16, LANES), jnp.int32), pltpu.VMEM((16, LANES), jnp.int32),
                            pltpu.VMEM((8, n), F32), pltpu.SemaphoreType.DMA((5,)), pltpu.SemaphoreType.DMA((5,)),
                            pltpu.SemaphoreType.DMA((5,))],
            compiler_params=pltpu.CompilerParams(collective_id=0, has_side_effects=True, vmem_limit_bytes=8 * MIB),
            name='exchange',
        )(token, kspace, wts_y, wts_x, idx_y.reshape(16, LANES), idx_x.reshape(16, LANES), e2)
        y8, wy, wx, addr, roff, e2f = samples
        accs = pl.pallas_call(
            spread_kernel,
            out_shape=acc_shape,
            in_specs=[vmem] * (5 + N_ACC),
            out_specs=[vmem] * (N_ACC),
            scratch_shapes=[pltpu.SMEM((2, 16, LANES), jnp.int32)] + [pltpu.VMEM((WIDE, LANES), F32)] * 4 + [pltpu.SemaphoreType.DMA],
            input_output_aliases={5 + i: i for i in range(N_ACC)},
            compiler_params=pltpu.CompilerParams(vmem_limit_bytes=8 * MIB),
            cost_estimate=pl.CostEstimate(flops=2 * 10**9, bytes_accessed=2 * 10**7, transcendentals=0),
            name='spread',
        )(addr, y8, wy, wx, roff, *accs)
        return pl.pallas_call(
            transform_kernel,
            out_shape=sds((2, P_BLK, Q_BLK), F32),
            in_specs=[vmem] * (N_ACC + 4),
            out_specs=vmem,
            scratch_shapes=[pltpu.VMEM((2, 4, Q_PAD, P_ALL), F32), pltpu.VMEM((Q_BLK, P_BLK), F32), pltpu.VMEM((KV, WIDE), BF16)] + [pltpu.VMEM((KV, LANES), F32)] * 3 + [
                pltpu.VMEM((Q_PAD, LANES), F32),
                pltpu.VMEM((GN_ROWS, LANES), F32),
                pltpu.VMEM((LAST, 4, Q_PAD, WIDE), BF16),
                pltpu.VMEM((LAST, 4, Q_PAD, WIDE), BF16),
                pltpu.VMEM((4, 144, LANES), BF16),
                pltpu.VMEM((4, 144, LANES), BF16),
                pltpu.VMEM((Q_PAD, LANES), F32),
                pltpu.VMEM((GN_ROWS, LANES), F32),
                pltpu.VMEM((4 * Q_PAD, P_TWO), F32),
                pltpu.VMEM((Q_PAD, P_ALL), F32),
                pltpu.VMEM((Q_PAD, P_ALL), F32),
                pltpu.VMEM((Q_PAD, P_ALL), F32),
                pltpu.SemaphoreType.DMA((N_CHUNK, len(SUBS), 3)),
                pltpu.SemaphoreType.DMA((N_CHUNK, len(SUBS), 4)),
                pltpu.SemaphoreType.DMA((2,)),
                pltpu.SemaphoreType.DMA((2,)),
                pltpu.SemaphoreType.DMA((len(SUBS),)),
                pltpu.SemaphoreType.DMA((len(SUBS),)),
            ],
            compiler_params=pltpu.CompilerParams(collective_id=1, has_side_effects=True, vmem_limit_bytes=24 * MIB),
            name='transform',
        )(*accs, e1, e2f, maps, deapod)

    return jax.shard_map(
        local_fn,
        mesh=mesh,
        in_specs=(P(None, None, sample_spec), P(None, sample_spec), P(None, sample_spec), P(sample_spec), P(sample_spec), P(None, ('exam', 'cols'), None, 'rows'), P()),
        out_specs=P(None, ('exam', 'cols'), 'rows'),
        check_vma=False,
    )
```

```python
import math

import jax
import jax.numpy as jnp
import numpy as np
from jax import lax
from jax.experimental import pallas as pl
from jax.experimental.pallas import tpu as pltpu
from jax.sharding import PartitionSpec as P

F32, BF16 = jnp.float32, jnp.bfloat16
MESH = pl.DeviceIdType.MESH

N_IMG = 368
N_GRID = 736
ROW_BLK = 184
Q_BLK, Q_PAD = 92, 96
P_BLK, P_PAD, P_ALL = 184, 192, 384
N_CH = 8
TILE_U, STRIDE_U, N_SRC = 16, 13, 15
N_TGT = 12
COL_BLK = 368
VR = 384
VS = 392
KV = 2 * VR
LANES, ROWS = 128, 16
EDGE = 6
WIDE, P_TWO, GN_ROWS, MIB = 2 * LANES, 2 * P_ALL, 48, 2**20
N_CHUNK = 6
N_COPY = 3
N_ACC = 2 * N_COPY
SUBS = [(0, 64), (64, 32), (0, Q_PAD)]
FULL, N_WHOLE = 2, 2
WHOLE, SPLIT = range(N_WHOLE), range(N_WHOLE, N_CHUNK)
POSTS = [[(j, FULL)] for j in WHOLE] + [[(j, 0)] for j in SPLIT]
POSTS += [[(j, 1) for j in SPLIT]]
LAST = N_CHUNK - 1
SUBS_LAST = [(0, 96), (96, 48)]
SENT = [(j, FULL) for j in WHOLE] + [(j, sub) for j in SPLIT for sub in range(2)]
CHUNK_TILES = [(1 + 2 * j, 2 + 2 * j) for j in range(5)] + [(0, 11)]


def dft_constants():
    scale = 1.0 / math.sqrt(N_GRID)
    phase = ((np.arange(N_GRID)[:, None] - N_GRID // 2) * (np.arange(N_IMG)[None, :] - N_IMG // 2)) % N_GRID
    ang = phase.astype(np.float64) * (2.0 * math.pi / N_GRID)
    parts = (np.cos(ang) * scale, np.sin(ang) * scale)
    e1 = np.zeros((4, 2, Q_PAD, 2, VR))
    for dest in range(4):
        for cs in range(2):
            for half in range(2):
                part = parts[cs][half * COL_BLK:(half + 1) * COL_BLK, dest * Q_BLK:(dest + 1) * Q_BLK]
                e1[dest, cs, :Q_BLK, half, EDGE:EDGE + COL_BLK] = part.T
    e2 = np.zeros((N_CHUNK, 4, 2, TILE_U, 2, P_ALL))
    for j in range(N_CHUNK):
        for src in range(4):
            for tl in range(2):
                base = TILE_U * CHUNK_TILES[j][tl]
                rows = min(TILE_U, ROW_BLK - base)
                u0 = src * ROW_BLK + base
                for cs in range(2):
                    e2[j, src, tl, :rows, cs, :N_IMG] = parts[cs][u0:u0 + rows]
    return (jnp.asarray(e1.reshape(8 * Q_PAD, KV).astype(np.float32)).astype(BF16),
            jnp.asarray(e2.reshape(N_CHUNK * LANES, P_TWO).astype(np.float32)).astype(BF16))


def j_is_last(j):
    return isinstance(j, int) and j == LAST


def exchange_kernel(y_hbm, wy_hbm, wx_hbm, iy_hbm, ix_hbm, e2_hbm, y_ref, wy_ref, wx_ref, addr_ref, roff_ref, e2f, *refs):
    accs = refs[:N_ACC]
    e2_ref, y_in, iy, ix, y_send, in_sem, send_sem, recv_sem = refs[N_ACC:]
    k = lax.axis_index('cols')
    r = lax.axis_index('rows')
    other = {'cols': 1 - k}
    barrier = pltpu.get_barrier_semaphore()
    pl.semaphore_signal(barrier, inc=1, device_id=other, device_id_type=MESH)
    loads = [(iy_hbm, iy), (ix_hbm, ix), (y_hbm, y_in), (wy_hbm, wy_ref.at[0]), (wx_hbm, wx_ref.at[0]), (e2_hbm, e2_ref)]
    loads = [pltpu.make_async_copy(a, b, in_sem.at[i]) for i, (a, b) in enumerate(loads)]
    for c in loads:
        c.start()

    def send(i, src, dst):
        c = pltpu.make_async_remote_copy(src_ref=src, dst_ref=dst, send_sem=send_sem.at[i], recv_sem=recv_sem.at[i],
                                         device_id=other, device_id_type=MESH)
        c.start()
        return c

    loads[3].wait()
    loads[4].wait()
    pl.semaphore_wait(barrier, 1)
    copies = [send(0, wy_ref.at[0], wy_ref.at[1]), send(1, wx_ref.at[0], wx_ref.at[1])]
    loads[0].wait()
    loads[1].wait()
    row = iy[...] - r * ROW_BLK
    tile = jnp.zeros_like(row)
    for t in range(1, N_SRC):
        tile = tile + jnp.where(row >= STRIDE_U * t, 1, 0)
    addr_ref[0] = tile * VS + (ix[...] - k * COL_BLK)
    roff_ref[0] = (row + 14) & 15
    loads[2].wait()
    y_re, y_im = y_in[0], y_in[1]
    low = jnp.concatenate([y_re[0:4], y_im[0:4]], axis=0)
    high = jnp.concatenate([y_re[4:8], y_im[4:8]], axis=0)
    y_ref[0] = jnp.where(k == 0, low, high)
    y_send[...] = jnp.where(k == 0, high, low)
    copies += [send(2, addr_ref.at[0], addr_ref.at[1]), send(3, roff_ref.at[0], roff_ref.at[1]), send(4, y_send, y_ref.at[1])]

    def zero(i, _):
        for a in accs:
            a[pl.ds(pl.multiple_of(i * VS, 8), VS), :] = jnp.zeros((VS, LANES), F32)
        return 0
    lax.fori_loop(0, N_SRC, zero, 0)
    loads[-1].wait()
    for j in range(N_CHUNK):
        for h in range(2):
            v = e2_ref[LANES * j + 64 * h:LANES * j + 64 * h + 64, :]
            e2f[j, LANES * h:LANES * h + 64, :] = v
            e2f[j, LANES * h + 64:LANES * h + LANES, 0:P_ALL] = -v[:, P_ALL:P_TWO]
            e2f[j, LANES * h + 64:LANES * h + LANES, P_ALL:P_TWO] = v[:, 0:P_ALL]
    for c in copies:
        c.wait()


def split3(x):
    hi = x.astype(BF16).astype(F32)
    rest = x - hi
    mid = rest.astype(BF16).astype(F32)
    return [hi, mid, rest - mid]


def spread_kernel(addr_ref, y_ref, wy_ref, wx_ref, roff_ref, *refs):
    accs = refs[N_ACC:4 * N_COPY]
    addr, sem = refs[4 * N_COPY], refs[-1]
    q_refs = refs[4 * N_COPY + 1:-1]
    to_smem = pltpu.make_async_copy(addr_ref, addr, sem)
    to_smem.start()
    n = y_ref.shape[2]

    r0 = lax.broadcasted_iota(jnp.int32, (80, WIDE), 0)
    l0 = lax.broadcasted_iota(jnp.int32, (80, WIDE), 1)
    ry = (r0 < 24) & (l0 < LANES) & ((r0 & 7) == (l0 >> 4))
    rw = (r0 >= 24) & (r0 < 72) & (l0 >= LANES) & (((r0 - 24) & 15) == (l0 & 15))
    expand = jnp.where(ry | rw, 1.0, 0.0).astype(BF16)
    rr = lax.broadcasted_iota(jnp.int32, (ROWS, WIDE), 0)
    n_blk = n // WIDE

    def prep(i, slot, q_ref):
        ds = [pl.ds(pl.multiple_of((i + n_blk * h) * LANES, LANES), LANES) for h in range(2)]
        y = jnp.concatenate([y_ref[slot, :, s] for s in ds], axis=1)
        wy = jnp.concatenate([wy_ref[slot, :, s] for s in ds], axis=1)
        d = (rr - jnp.concatenate([roff_ref[slot, pl.ds(i + n_blk * h, 1), :] for h in range(2)], axis=1)) & 15
        w16 = jnp.zeros((ROWS, WIDE), F32)
        for a in range(4):
            w16 = jnp.where(d == a, wy[a:a + 1], w16)
        lhs = jnp.concatenate(split3(y) + split3(w16) + [jnp.zeros((8, WIDE), F32)], axis=0).astype(BF16)
        o = lax.dot_general(lhs, expand, (((0,), (0,)), ((), ())), preferred_element_type=F32)
        q_ref[...] = o[:, :LANES] * o[:, LANES:]

    top = lax.broadcasted_iota(jnp.int32, (8, LANES), 0) < 4

    def scatter(i, qs):
        ds = [pl.ds(pl.multiple_of((i + n_blk * h) * LANES, LANES), LANES) for h in range(2)]
        wx = [jnp.concatenate([wx_ref[slot, :, s] for s in ds], axis=0) for slot in range(2)]
        for j in range(LANES):
            cols = [jnp.broadcast_to(wx[slot][:, j:j + 1], (8, LANES)) for slot in range(2)]
            for h in range(2):
                for slot in range(2):
                    acc = accs[slot * N_COPY + (2 * j + h) % N_COPY]
                    base = addr[slot, i + n_blk * h, j] + (0 if h else 4)
                    q = jnp.broadcast_to(qs[slot][j + LANES * h:j + LANES * h + 1, :], (8, LANES))
                    s = pl.ds(base, 8)
                    c = jnp.where(top, 0.0, cols[slot]) if h else jnp.where(top, cols[slot], 0.0)
                    acc[s, :] = acc[s, :] + c * q

    qa, qb = q_refs[:2], q_refs[2:]
    for slot in range(2):
        prep(0, slot, qa[slot])
    to_smem.wait()

    def two_blocks(i, _):
        for step, now, then in ((0, qa, qb), (1, qb, qa)):
            for slot in range(2):
                prep(lax.rem(2 * i + step + 1, n_blk), slot, then[slot])
            scatter(2 * i + step, now)
        return 0
    lax.fori_loop(0, n_blk // 2, two_blocks, 0)


def transform_kernel(*refs):
    own, nbr = refs[:N_COPY], refs[N_COPY:N_ACC]
    (e1_ref, e2f, s_ref, d_ref, out_ref, st, dd, gch, raw0, f0, f11, gps, gns, msg, recv, msg_last, recv_last, gpr, gnr, img, mine, psend, precv,
     msend_sem, mrecv_sem, gsend_sem, grecv_sem, psend_sem, precv_sem) = refs[N_ACC:]
    k = lax.axis_index('cols')
    r = lax.axis_index('rows')
    chip, core = r // 2, r % 2
    dests = [2 * (1 - chip) + core, 2 * (1 - chip) + (1 - core), 2 * chip + (1 - core)]
    nxt, prv = lax.rem(r + 1, 4), lax.rem(r + 3, 4)
    barrier = pltpu.get_barrier_semaphore()
    for d in dests:
        pl.semaphore_signal(barrier, inc=1, device_id={'rows': d}, device_id_type=MESH)
    pl.semaphore_signal(barrier, inc=1, device_id={'cols': 1 - k}, device_id_type=MESH)

    slots = ((own, k), (nbr, 1 - k))
    lane16 = lax.broadcasted_iota(jnp.int32, (ROWS, LANES), 1) & 15
    sub16 = lax.broadcasted_iota(jnp.int32, (ROWS, LANES), 0)

    def merged(accs, off, targets):
        wanted = {}
        for m in targets:
            deltas = {0: 0} if m is None else {t: STRIDE_U * t - TILE_U * m - 2 for t in range(N_SRC)}
            wanted[m] = {t: d for t, d in deltas.items() if abs(d) < ROWS}
        loaded = {}
        for t in sorted({t for w in wanted.values() for t in w}):
            s = pl.ds(t * VS + off, ROWS)
            v = accs[0][s, :]
            for acc in accs[1:]:
                v = v + acc[s, :]
            loaded[t] = v
        outs = []
        for m in targets:
            out = None
            for t, d in wanted[m].items():
                lo, hi = max(0, d), min(15, 15 + d)
                v = loaded[t]
                if lo > 0 or hi < 15:
                    v = jnp.where((lane16 >= lo) & (lane16 <= hi), v, 0.0)
                out = v if out is None else out + v
            outs.append(out)
        return outs

    def merge_all(targets, put):
        def rows(i, _):
            for step in range(2):
                for accs, half in slots:
                    off = pl.multiple_of((2 * i + 1 + step) * ROWS, ROWS)
                    put(pl.multiple_of(half * VR + off, ROWS), merged(accs, off, targets))
            return 0
        lax.fori_loop(0, VR // (2 * ROWS) - 1, rows, 0)
        last = VR - ROWS
        a = [merged(accs, 0, targets) for accs, _ in slots]
        b = [merged(accs, last, targets) for accs, _ in slots]
        for i, (_, half) in enumerate(slots):
            fix_a = [x + jnp.where(sub16 == 6, y, 0.0) for x, y in zip(a[i], b[1 - i])]
            fix_b = [y + jnp.where((sub16 == 4) | (sub16 == 5), x, 0.0) for x, y in zip(a[1 - i], b[i])]
            put(pl.multiple_of(half * VR, ROWS), fix_a)
            put(pl.multiple_of(half * VR + last, ROWS), fix_b)

    def put_chunk(off, vals):
        for i, v in enumerate(vals):
            gch[pl.ds(off, ROWS), LANES * i:LANES * (i + 1)] = v.astype(BF16)

    def put_edges(off, vals):
        for ref, v in zip((raw0, f0, f11), vals):
            ref[pl.ds(off, ROWS), :] = v

    lane = lax.broadcasted_iota(jnp.int32, (Q_PAD, WIDE), 1) & 127

    def swap(sub):
        rows = pl.ds(*SUBS[sub])
        return pltpu.make_async_remote_copy(src_ref=psend.at[rows], dst_ref=precv.at[rows], send_sem=psend_sem.at[sub],
                                            recv_sem=precv_sem.at[sub], device_id={'cols': 1 - k}, device_id_type=MESH)

    def first_dft(j, g):
        ab = jnp.dot(e1_ref[...], g, preferred_element_type=F32)
        for d in range(4):
            a = ab[192 * d:192 * d + Q_PAD]
            b = ab[192 * d + Q_PAD:192 * d + 192]
            b = jnp.concatenate([pltpu.roll(b[:, :128], 64, 1), pltpu.roll(b[:, 128:], 64, 1)], axis=1)
            h = jnp.where(lane < 64, a - b, a + b).astype(BF16)
            if not j_is_last(j):
                msg[j, d] = h
                continue
            for sub, (at, _) in enumerate(SUBS_LAST):
                row0, rows = SUBS[sub]
                half = rows // 2
                upper = h[row0:row0 + half, LANES:WIDE]
                lower = pltpu.roll(h[row0 + half:row0 + rows, LANES:WIDE], 8, 1)
                msg_last[d, at:at + rows] = h[row0:row0 + rows, 0:LANES]
                msg_last[d, at + rows:at + rows + half] = jnp.where((lane[0:half, 0:LANES] & 8) == 0, upper, lower)

    def copy_of(j, sub, i, slot):
        d = dests[i]
        if j_is_last(j):
            rows = pl.ds(*SUBS_LAST[sub])
            src, dst = msg_last.at[d, rows], recv_last.at[slot, rows]
        else:
            rows = pl.ds(*SUBS[sub])
            src, dst = msg.at[j, d, rows], recv.at[j, slot, rows]
        return pltpu.make_async_remote_copy(src_ref=src, dst_ref=dst, send_sem=msend_sem.at[j, sub, i],
                                            recv_sem=mrecv_sem.at[j, sub, slot], device_id={'rows': d}, device_id_type=MESH)

    def post(chunk):
        for j, sub in POSTS[chunk]:
            for i in range(3):
                copy_of(j, sub, i, r).start()
        if chunk < LAST:
            recv[chunk, r] = msg[chunk, r]
        elif chunk == LAST:
            recv_last[r] = msg_last[r]

    merge_all(CHUNK_TILES[0], put_chunk)
    first_dft(0, gch[...])
    pl.semaphore_wait(barrier, 4)
    post(0)

    merge_all((None, 0, N_TGT - 1), put_edges)
    la = lax.broadcasted_iota(jnp.int32, (Q_PAD, LANES), 1) & 15
    lb = lax.broadcasted_iota(jnp.int32, (GN_ROWS, LANES), 1) & 15

    def shifted(v, by):
        return pltpu.roll(v, by % LANES, 1) if by else v

    gp = jnp.zeros((Q_PAD, LANES), F32)
    for c in range(8):
        gp = jnp.where((la >> 1) == c, shifted(raw0[Q_PAD * c:Q_PAD * c + Q_PAD, :], 2 * c - 14), gp)
    gps[...] = gp
    gn = jnp.zeros((GN_ROWS, LANES), F32)
    for c in range(16):
        gn = jnp.where(lb == c, shifted(f11[GN_ROWS * c:GN_ROWS * c + GN_ROWS, :], c - 8), gn)
    gns[...] = gn
    to_prv = pltpu.make_async_remote_copy(src_ref=gps, dst_ref=gpr, send_sem=gsend_sem.at[0], recv_sem=grecv_sem.at[0],
                                          device_id={'rows': prv}, device_id_type=MESH)
    to_nxt = pltpu.make_async_remote_copy(src_ref=gns, dst_ref=gnr, send_sem=gsend_sem.at[1], recv_sem=grecv_sem.at[1],
                                          device_id={'rows': nxt}, device_id_type=MESH)
    to_prv.start()
    to_nxt.start()

    for j in range(1, N_CHUNK - 1):
        merge_all(CHUNK_TILES[j], put_chunk)
        first_dft(j, gch[...])
        post(j)

    to_prv.wait()
    to_nxt.wait()
    gp, gn = gpr[...], gnr[...]
    for c in range(8):
        s = slice(Q_PAD * c, Q_PAD * c + Q_PAD)
        gch[s, LANES:WIDE] = (f11[s, :] + jnp.where((la >> 1) == 3, shifted(gp, 6 - 2 * c), 0.0)).astype(BF16)
    for c in range(16):
        s = slice(GN_ROWS * c, GN_ROWS * c + GN_ROWS)
        gch[s, 0:LANES] = (f0[s, :] + jnp.where(lb == 0, shifted(gn, -c), 0.0)).astype(BF16)
    first_dft(LAST, gch[...])
    post(LAST)

    d_all = d_ref[...].reshape(1, N_IMG)
    st[...] = jnp.zeros_like(st)
    for s in range(2):
        for c in range(4):
            st[s, c, 0:Q_BLK, 0:N_IMG] = s_ref[s, :, c, :]

    half_p = jnp.where(k == 0, d_all[:, 0:P_BLK], d_all[:, P_BLK:2 * P_BLK])
    part_q = d_all[:, 0:Q_BLK]
    for i in range(1, 4):
        part_q = jnp.where(r == i, d_all[:, Q_BLK * i:Q_BLK * (i + 1)], part_q)
    part_q = jnp.concatenate([part_q, jnp.zeros((1, LANES - Q_BLK), F32)], axis=1)
    dd[...] = jnp.broadcast_to(part_q, (8, LANES)).T[0:Q_BLK, 0:1] * half_p

    first_col = k == 0

    def second_dft(j, sub):
        row0, rows = SUBS[sub]
        for i in range(3):
            copy_of(j, sub, i, dests[i]).wait_recv()
        coil = (lax.broadcasted_iota(jnp.int32, (rows, LANES), 1) >> 4) & 3
        halves = []
        for pair in range(2):
            v = []
            for src in (2 * pair, 2 * pair + 1):
                if j_is_last(j):
                    at = SUBS_LAST[sub][0]
                    folded = recv_last[src, at + rows:at + rows + rows // 2]
                    v += [recv_last[src, at:at + rows], jnp.concatenate([folded, pltpu.roll(folded, LANES - 8, 1)], axis=0)]
                else:
                    v += [recv[j, src, pl.ds(row0, rows), LANES * t:LANES * (t + 1)] for t in range(2)]
            for bit in (1, 2):
                m = (coil & bit) == 0
                for t in range(4):
                    if t & bit:
                        continue
                    x, y = v[t], v[t | bit]
                    v[t] = jnp.where(m, x, pltpu.roll(y, ROWS * bit, 1))
                    v[t | bit] = jnp.where(m, pltpu.roll(x, LANES - ROWS * bit, 1), y)
            halves.append(v)
        lhs = jnp.concatenate([jnp.concatenate([halves[0][c], halves[1][c]], axis=1) for c in range(4)], axis=0)
        return jnp.dot(lhs, e2f[j], preferred_element_type=F32)

    img[...] = second_dft(0, FULL)
    for j in WHOLE[1:]:
        img[...] += second_dft(j, FULL)
    for sub in range(2):
        row0, rows = SUBS[sub]

        def accumulate(j, _):
            part = second_dft(j, sub)
            for c in range(4):
                img[Q_PAD * c + row0:Q_PAD * c + row0 + rows] += part[rows * c:rows * (c + 1)]
            return 0
        lax.fori_loop(N_WHOLE, N_WHOLE + 1, accumulate, 0)
        if sub == 0:
            post(N_CHUNK)
        lax.fori_loop(N_WHOLE + 1, LAST, accumulate, 0)
        accumulate(LAST, 0)

        x_re = jnp.zeros((rows, P_ALL), F32)
        x_im = jnp.zeros((rows, P_ALL), F32)
        for c in range(4):
            i_re = img[Q_PAD * c + row0:Q_PAD * c + row0 + rows, 0:P_ALL]
            i_im = img[Q_PAD * c + row0:Q_PAD * c + row0 + rows, P_ALL:P_TWO]
            s_re, s_im = st[0, c, row0:row0 + rows], st[1, c, row0:row0 + rows]
            x_re = x_re + s_re * i_re + s_im * i_im
            x_im = x_im + s_re * i_im - s_im * i_re
        lo = jnp.concatenate([x_re[:, 0:P_PAD], x_im[:, 0:P_PAD]], axis=1)
        hi = jnp.concatenate([x_re[:, P_BLK:P_BLK + P_PAD], x_im[:, P_BLK:P_BLK + P_PAD]], axis=1)
        psend[row0:row0 + rows] = jnp.where(first_col, hi, lo)
        swap(sub).start()
        mine[row0:row0 + rows] = jnp.where(first_col, lo, hi)

    for j, sub in SENT:
        for i in range(3):
            copy_of(j, sub, i, r).wait_send()
    for sub in range(2):
        swap(sub).wait()
    total = mine[...] + precv[...]
    out_ref[0] = (total[0:Q_BLK, 0:P_BLK] * dd[...]).T
    out_ref[1] = (total[0:Q_BLK, P_PAD:P_PAD + P_BLK] * dd[...]).T


def solution(mesh):
    sample_spec = ('exam', 'rows', 'cols')
    vmem = pl.BlockSpec(memory_space=pltpu.VMEM)
    hbm = pl.BlockSpec(memory_space=pltpu.HBM)
    sds = jax.ShapeDtypeStruct

    def local_fn(kspace, wts_y, wts_x, idx_y, idx_x, coil_maps, deapod):
        n = kspace.shape[2]
        e1, e2 = dft_constants()
        maps = jnp.transpose(coil_maps, (0, 3, 1, 2))
        acc_shape = [sds((N_SRC * VS, LANES), F32)] * (N_ACC)
        inputs = (kspace, wts_y, wts_x, idx_y.reshape(16, LANES), idx_x.reshape(16, LANES), e2)
        *samples, = pl.pallas_call(
            exchange_kernel,
            out_shape=[sds((2, 8, n), F32), sds((2, 4, n), F32), sds((2, 4, n), F32), sds((2, 16, LANES), jnp.int32),
                       sds((2, 16, LANES), jnp.int32), sds((N_CHUNK, WIDE, P_TWO), BF16)] + acc_shape,
            in_specs=[hbm] * 6,
            out_specs=[vmem] * (6 + N_ACC),
            scratch_shapes=[pltpu.VMEM((KV, P_TWO), BF16), pltpu.VMEM((2, 8, n), F32), pltpu.VMEM((16, LANES), jnp.int32), pltpu.VMEM((16, LANES), jnp.int32),
                            pltpu.VMEM((8, n), F32), pltpu.SemaphoreType.DMA((6,)), pltpu.SemaphoreType.DMA((5,)),
                            pltpu.SemaphoreType.DMA((5,))],
            compiler_params=pltpu.CompilerParams(collective_id=0, has_side_effects=True, vmem_limit_bytes=8 * MIB),
            name='exchange',
        )(*[pltpu.with_memory_space_constraint(x, pltpu.HBM) for x in inputs])
        y8, wy, wx, addr, roff, e2f = samples[:6]
        accs = pl.pallas_call(
            spread_kernel,
            out_shape=acc_shape,
            in_specs=[vmem] * (5 + N_ACC),
            out_specs=[vmem] * (N_ACC),
            scratch_shapes=[pltpu.SMEM((2, 16, LANES), jnp.int32)] + [pltpu.VMEM((WIDE, LANES), F32)] * 4 + [pltpu.SemaphoreType.DMA],
            input_output_aliases={5 + i: i for i in range(N_ACC)},
            compiler_params=pltpu.CompilerParams(vmem_limit_bytes=8 * MIB),
            cost_estimate=pl.CostEstimate(flops=2 * 10**9, bytes_accessed=2 * 10**7, transcendentals=0),
            name='spread',
        )(addr, y8, wy, wx, roff, *samples[6:])
        return pl.pallas_call(
            transform_kernel,
            out_shape=sds((2, P_BLK, Q_BLK), F32),
            in_specs=[vmem] * (N_ACC + 4),
            out_specs=vmem,
            scratch_shapes=[pltpu.VMEM((2, 4, Q_PAD, P_ALL), F32), pltpu.VMEM((Q_BLK, P_BLK), F32), pltpu.VMEM((KV, WIDE), BF16)] + [pltpu.VMEM((KV, LANES), F32)] * 3 + [
                pltpu.VMEM((Q_PAD, LANES), F32),
                pltpu.VMEM((GN_ROWS, LANES), F32),
                pltpu.VMEM((LAST, 4, Q_PAD, WIDE), BF16),
                pltpu.VMEM((LAST, 4, Q_PAD, WIDE), BF16),
                pltpu.VMEM((4, 144, LANES), BF16),
                pltpu.VMEM((4, 144, LANES), BF16),
                pltpu.VMEM((Q_PAD, LANES), F32),
                pltpu.VMEM((GN_ROWS, LANES), F32),
                pltpu.VMEM((4 * Q_PAD, P_TWO), F32),
                pltpu.VMEM((Q_PAD, P_ALL), F32),
                pltpu.VMEM((Q_PAD, P_ALL), F32),
                pltpu.VMEM((Q_PAD, P_ALL), F32),
                pltpu.SemaphoreType.DMA((N_CHUNK, len(SUBS), 3)),
                pltpu.SemaphoreType.DMA((N_CHUNK, len(SUBS), 4)),
                pltpu.SemaphoreType.DMA((2,)),
                pltpu.SemaphoreType.DMA((2,)),
                pltpu.SemaphoreType.DMA((len(SUBS),)),
                pltpu.SemaphoreType.DMA((len(SUBS),)),
            ],
            compiler_params=pltpu.CompilerParams(collective_id=1, has_side_effects=True, vmem_limit_bytes=24 * MIB),
            name='transform',
        )(*accs, e1, e2f, maps, deapod)

    return jax.shard_map(
        local_fn,
        mesh=mesh,
        in_specs=(P(None, None, sample_spec), P(None, sample_spec), P(None, sample_spec), P(sample_spec), P(sample_spec), P(None, ('exam', 'cols'), None, 'rows'), P()),
        out_specs=P(None, ('exam', 'cols'), 'rows'),
        check_vma=False,
    )
```

```python
import math

import jax
import jax.numpy as jnp
import numpy as np
from jax import lax
from jax.experimental import pallas as pl
from jax.experimental.pallas import tpu as pltpu
from jax.sharding import PartitionSpec as P

F32, BF16 = jnp.float32, jnp.bfloat16
MESH = pl.DeviceIdType.MESH

N_IMG = 368
N_GRID = 736
ROW_BLK = 184
Q_BLK, Q_PAD = 92, 96
P_BLK, P_PAD, P_ALL = 184, 192, 384
N_CH = 8
TILE_U, STRIDE_U, N_SRC = 16, 13, 15
N_TGT = 12
COL_BLK = 368
VR = 384
VS = 392
KV = 2 * VR
LANES, ROWS = 128, 16
EDGE = 6
WIDE, P_TWO, GN_ROWS, MIB = 2 * LANES, 2 * P_ALL, 48, 2**20
N_CHUNK = 6
N_COPY = 3
N_ACC = 2 * N_COPY
SUBS = [(0, 64), (64, 32), (0, Q_PAD)]
FULL, N_WHOLE = 2, 2
WHOLE, SPLIT = range(N_WHOLE), range(N_WHOLE, N_CHUNK)
POSTS = [[(j, FULL)] for j in WHOLE] + [[(j, 0)] for j in SPLIT]
POSTS += [[(j, 1) for j in SPLIT]]
LAST = N_CHUNK - 1
SUBS_LAST = [(0, 96), (96, 48)]
SENT = [(j, FULL) for j in WHOLE] + [(j, sub) for j in SPLIT for sub in range(2)]
CHUNK_TILES = [(1 + 2 * j, 2 + 2 * j) for j in range(5)] + [(0, 11)]


def dft_constants():
    scale = 1.0 / math.sqrt(N_GRID)
    phase = ((np.arange(N_GRID)[:, None] - N_GRID // 2) * (np.arange(N_IMG)[None, :] - N_IMG // 2)) % N_GRID
    ang = phase.astype(np.float64) * (2.0 * math.pi / N_GRID)
    parts = (np.cos(ang) * scale, np.sin(ang) * scale)
    e1 = np.zeros((4, 2, Q_PAD, 2, VR))
    for dest in range(4):
        for cs in range(2):
            for half in range(2):
                part = parts[cs][half * COL_BLK:(half + 1) * COL_BLK, dest * Q_BLK:(dest + 1) * Q_BLK]
                e1[dest, cs, :Q_BLK, half, EDGE:EDGE + COL_BLK] = part.T
    e2 = np.zeros((N_CHUNK, 4, 2, TILE_U, 2, P_ALL))
    for j in range(N_CHUNK):
        for src in range(4):
            for tl in range(2):
                base = TILE_U * CHUNK_TILES[j][tl]
                rows = min(TILE_U, ROW_BLK - base)
                u0 = src * ROW_BLK + base
                for cs in range(2):
                    e2[j, src, tl, :rows, cs, :N_IMG] = parts[cs][u0:u0 + rows]
    return (jnp.asarray(e1.reshape(8 * Q_PAD, KV).astype(np.float32)).astype(BF16),
            jnp.asarray(e2.reshape(N_CHUNK * LANES, P_TWO).astype(np.float32)).astype(BF16))


def j_is_last(j):
    return isinstance(j, int) and j == LAST


def exchange_kernel(y_hbm, wy_hbm, wx_hbm, iy_hbm, ix_hbm, e2_hbm, y_ref, wy_ref, wx_ref, place_ref, e2f, *refs):
    accs = refs[:N_ACC]
    e2_ref, y_in, iy, ix, y_send, in_sem, send_sem, recv_sem = refs[N_ACC:]
    k = lax.axis_index('cols')
    r = lax.axis_index('rows')
    other = {'cols': 1 - k}
    barrier = pltpu.get_barrier_semaphore()
    pl.semaphore_signal(barrier, inc=1, device_id=other, device_id_type=MESH)
    loads = [(iy_hbm, iy), (ix_hbm, ix), (y_hbm, y_in), (wy_hbm, wy_ref.at[0]), (wx_hbm, wx_ref.at[0]), (e2_hbm, e2_ref)]
    loads = [pltpu.make_async_copy(a, b, in_sem.at[i]) for i, (a, b) in enumerate(loads)]
    for c in loads:
        c.start()

    def send(i, src, dst):
        c = pltpu.make_async_remote_copy(src_ref=src, dst_ref=dst, send_sem=send_sem.at[i], recv_sem=recv_sem.at[i],
                                         device_id=other, device_id_type=MESH)
        c.start()
        return c

    loads[3].wait()
    loads[4].wait()
    pl.semaphore_wait(barrier, 1)
    copies = [send(0, wy_ref.at[0], wy_ref.at[1]), send(1, wx_ref.at[0], wx_ref.at[1])]
    loads[0].wait()
    loads[1].wait()
    row = iy[...] - r * ROW_BLK
    tile = jnp.zeros_like(row)
    for t in range(1, N_SRC):
        tile = tile + jnp.where(row >= STRIDE_U * t, 1, 0)
    place_ref[0] = (tile * VS + (ix[...] - k * COL_BLK)) * ROWS + ((row + 14) & 15)
    loads[2].wait()
    y_re, y_im = y_in[0], y_in[1]
    low = jnp.concatenate([y_re[0:4], y_im[0:4]], axis=0)
    high = jnp.concatenate([y_re[4:8], y_im[4:8]], axis=0)
    y_ref[0] = jnp.where(k == 0, low, high)
    y_send[...] = jnp.where(k == 0, high, low)
    copies += [send(2, place_ref.at[0], place_ref.at[1]), send(3, y_send, y_ref.at[1])]

    def zero(i, _):
        for a in accs:
            a[pl.ds(pl.multiple_of(i * VS, 8), VS), :] = jnp.zeros((VS, LANES), F32)
        return 0
    lax.fori_loop(0, N_SRC, zero, 0)
    loads[-1].wait()
    for j in range(N_CHUNK):
        for h in range(2):
            v = e2_ref[LANES * j + 64 * h:LANES * j + 64 * h + 64, :]
            e2f[j, LANES * h:LANES * h + 64, :] = v
            e2f[j, LANES * h + 64:LANES * h + LANES, 0:P_ALL] = -v[:, P_ALL:P_TWO]
            e2f[j, LANES * h + 64:LANES * h + LANES, P_ALL:P_TWO] = v[:, 0:P_ALL]
    for c in copies:
        c.wait()


def split3(x):
    hi = x.astype(BF16).astype(F32)
    rest = x - hi
    mid = rest.astype(BF16).astype(F32)
    return [hi, mid, rest - mid]


def spread_kernel(place_ref, y_ref, wy_ref, wx_ref, *refs):
    accs = refs[N_ACC:4 * N_COPY]
    addr, addr_v, roff, sem, *q_refs = refs[4 * N_COPY:]
    place = place_ref[...]
    addr_v[...] = place >> 4
    roff[...] = place & 15
    to_smem = pltpu.make_async_copy(addr_v, addr, sem)
    to_smem.start()
    n = y_ref.shape[2]

    r0 = lax.broadcasted_iota(jnp.int32, (80, WIDE), 0)
    l0 = lax.broadcasted_iota(jnp.int32, (80, WIDE), 1)
    ry = (r0 < 24) & (l0 < LANES) & ((r0 & 7) == (l0 >> 4))
    rw = (r0 >= 24) & (r0 < 72) & (l0 >= LANES) & (((r0 - 24) & 15) == (l0 & 15))
    expand = jnp.where(ry | rw, 1.0, 0.0).astype(BF16)
    rr = lax.broadcasted_iota(jnp.int32, (ROWS, WIDE), 0)
    n_blk = n // WIDE

    def prep(i, slot, q_ref):
        ds = [pl.ds(pl.multiple_of((i + n_blk * h) * LANES, LANES), LANES) for h in range(2)]
        y = jnp.concatenate([y_ref[slot, :, s] for s in ds], axis=1)
        wy = jnp.concatenate([wy_ref[slot, :, s] for s in ds], axis=1)
        d = (rr - jnp.concatenate([roff[slot, pl.ds(i + n_blk * h, 1), :] for h in range(2)], axis=1)) & 15
        w16 = jnp.zeros((ROWS, WIDE), F32)
        for a in range(4):
            w16 = jnp.where(d == a, wy[a:a + 1], w16)
        lhs = jnp.concatenate(split3(y) + split3(w16) + [jnp.zeros((8, WIDE), F32)], axis=0).astype(BF16)
        o = lax.dot_general(lhs, expand, (((0,), (0,)), ((), ())), preferred_element_type=F32)
        q_ref[...] = o[:, :LANES] * o[:, LANES:]

    top = lax.broadcasted_iota(jnp.int32, (8, LANES), 0) < 4

    def scatter(i, qs):
        ds = [pl.ds(pl.multiple_of((i + n_blk * h) * LANES, LANES), LANES) for h in range(2)]
        wx = [jnp.concatenate([wx_ref[slot, :, s] for s in ds], axis=0) for slot in range(2)]
        for j in range(LANES):
            cols = [jnp.broadcast_to(wx[slot][:, j:j + 1], (8, LANES)) for slot in range(2)]
            for h in range(2):
                for slot in range(2):
                    acc = accs[slot * N_COPY + (2 * j + h) % N_COPY]
                    base = addr[slot, i + n_blk * h, j] + (0 if h else 4)
                    q = jnp.broadcast_to(qs[slot][j + LANES * h:j + LANES * h + 1, :], (8, LANES))
                    if h:
                        s = pl.ds(base, 8)
                        acc[s, :] = acc[s, :] + jnp.where(top, 0.0, cols[slot]) * q
                    else:
                        s = pl.ds(base, 4)
                        acc[s, :] = acc[s, :] + cols[slot][0:4] * q[0:4]

    qa, qb = q_refs[:2], q_refs[2:]
    for slot in range(2):
        prep(0, slot, qa[slot])
    to_smem.wait()

    def two_blocks(i, _):
        for step, now, then in ((0, qa, qb), (1, qb, qa)):
            for slot in range(2):
                prep(lax.rem(2 * i + step + 1, n_blk), slot, then[slot])
            scatter(2 * i + step, now)
        return 0
    lax.fori_loop(0, n_blk // 2, two_blocks, 0)


def transform_kernel(*refs):
    own, nbr = refs[:N_COPY], refs[N_COPY:N_ACC]
    (e1_ref, e2f, s_ref, d_ref, out_ref, st, dd, gch, raw0, f0, f11, gps, gns, msg, recv, msg_last, recv_last, gpr, gnr, img, mine, psend, precv,
     msend_sem, mrecv_sem, gsend_sem, grecv_sem, psend_sem, precv_sem) = refs[N_ACC:]
    k = lax.axis_index('cols')
    r = lax.axis_index('rows')
    chip, core = r // 2, r % 2
    dests = [2 * (1 - chip) + core, 2 * (1 - chip) + (1 - core), 2 * chip + (1 - core)]
    nxt, prv = lax.rem(r + 1, 4), lax.rem(r + 3, 4)
    barrier = pltpu.get_barrier_semaphore()
    for d in dests:
        pl.semaphore_signal(barrier, inc=1, device_id={'rows': d}, device_id_type=MESH)
    pl.semaphore_signal(barrier, inc=1, device_id={'cols': 1 - k}, device_id_type=MESH)

    slots = ((own, k), (nbr, 1 - k))
    lane16 = lax.broadcasted_iota(jnp.int32, (ROWS, LANES), 1) & 15
    sub16 = lax.broadcasted_iota(jnp.int32, (ROWS, LANES), 0)

    def merged(accs, off, targets):
        wanted = {}
        for m in targets:
            deltas = {0: 0} if m is None else {t: STRIDE_U * t - TILE_U * m - 2 for t in range(N_SRC)}
            wanted[m] = {t: d for t, d in deltas.items() if abs(d) < ROWS}
        loaded = {}
        for t in sorted({t for w in wanted.values() for t in w}):
            s = pl.ds(t * VS + off, ROWS)
            v = accs[0][s, :]
            for acc in accs[1:]:
                v = v + acc[s, :]
            loaded[t] = v
        outs = []
        for m in targets:
            out = None
            for t, d in wanted[m].items():
                lo, hi = max(0, d), min(15, 15 + d)
                v = loaded[t]
                if lo > 0 or hi < 15:
                    v = jnp.where((lane16 >= lo) & (lane16 <= hi), v, 0.0)
                out = v if out is None else out + v
            outs.append(out)
        return outs

    def merge_all(targets, put):
        def rows(i, _):
            for step in range(2):
                for accs, half in slots:
                    off = pl.multiple_of((2 * i + 1 + step) * ROWS, ROWS)
                    put(pl.multiple_of(half * VR + off, ROWS), merged(accs, off, targets))
            return 0
        lax.fori_loop(0, VR // (2 * ROWS) - 1, rows, 0)
        last = VR - ROWS
        a = [merged(accs, 0, targets) for accs, _ in slots]
        b = [merged(accs, last, targets) for accs, _ in slots]
        for i, (_, half) in enumerate(slots):
            fix_a = [x + jnp.where(sub16 == 6, y, 0.0) for x, y in zip(a[i], b[1 - i])]
            fix_b = [y + jnp.where((sub16 == 4) | (sub16 == 5), x, 0.0) for x, y in zip(a[1 - i], b[i])]
            put(pl.multiple_of(half * VR, ROWS), fix_a)
            put(pl.multiple_of(half * VR + last, ROWS), fix_b)

    def put_chunk(off, vals):
        for i, v in enumerate(vals):
            gch[pl.ds(off, ROWS), LANES * i:LANES * (i + 1)] = v.astype(BF16)

    def put_edges(off, vals):
        for ref, v in zip((raw0, f0, f11), vals):
            ref[pl.ds(off, ROWS), :] = v

    lane = lax.broadcasted_iota(jnp.int32, (Q_PAD, WIDE), 1) & 127

    def swap(sub):
        rows = pl.ds(*SUBS[sub])
        return pltpu.make_async_remote_copy(src_ref=psend.at[rows], dst_ref=precv.at[rows], send_sem=psend_sem.at[sub],
                                            recv_sem=precv_sem.at[sub], device_id={'cols': 1 - k}, device_id_type=MESH)

    def first_dft(j, g):
        ab = jnp.dot(e1_ref[...], g, preferred_element_type=F32)
        for d in range(4):
            a = ab[192 * d:192 * d + Q_PAD]
            b = ab[192 * d + Q_PAD:192 * d + 192]
            b = jnp.concatenate([pltpu.roll(b[:, :128], 64, 1), pltpu.roll(b[:, 128:], 64, 1)], axis=1)
            h = jnp.where(lane < 64, a - b, a + b).astype(BF16)
            if not j_is_last(j):
                msg[j, d] = h
                continue
            for sub, (at, _) in enumerate(SUBS_LAST):
                row0, rows = SUBS[sub]
                half = rows // 2
                upper = h[row0:row0 + half, LANES:WIDE]
                lower = pltpu.roll(h[row0 + half:row0 + rows, LANES:WIDE], 8, 1)
                msg_last[d, at:at + rows] = h[row0:row0 + rows, 0:LANES]
                msg_last[d, at + rows:at + rows + half] = jnp.where((lane[0:half, 0:LANES] & 8) == 0, upper, lower)

    def copy_of(j, sub, i, slot):
        d = dests[i]
        if j_is_last(j):
            rows = pl.ds(*SUBS_LAST[sub])
            src, dst = msg_last.at[d, rows], recv_last.at[slot, rows]
        else:
            rows = pl.ds(*SUBS[sub])
            src, dst = msg.at[j, d, rows], recv.at[j, slot, rows]
        return pltpu.make_async_remote_copy(src_ref=src, dst_ref=dst, send_sem=msend_sem.at[j, sub, i],
                                            recv_sem=mrecv_sem.at[j, sub, slot], device_id={'rows': d}, device_id_type=MESH)

    def post(chunk):
        for j, sub in POSTS[chunk]:
            for i in range(3):
                copy_of(j, sub, i, r).start()
        if chunk < LAST:
            recv[chunk, r] = msg[chunk, r]
        elif chunk == LAST:
            recv_last[r] = msg_last[r]

    merge_all(CHUNK_TILES[0], put_chunk)
    first_dft(0, gch[...])
    pl.semaphore_wait(barrier, 4)
    post(0)

    merge_all((None, 0, N_TGT - 1), put_edges)
    la = lax.broadcasted_iota(jnp.int32, (Q_PAD, LANES), 1) & 15
    lb = lax.broadcasted_iota(jnp.int32, (GN_ROWS, LANES), 1) & 15

    def shifted(v, by):
        return pltpu.roll(v, by % LANES, 1) if by else v

    gp = jnp.zeros((Q_PAD, LANES), F32)
    for c in range(8):
        gp = jnp.where((la >> 1) == c, shifted(raw0[Q_PAD * c:Q_PAD * c + Q_PAD, :], 2 * c - 14), gp)
    gps[...] = gp
    gn = jnp.zeros((GN_ROWS, LANES), F32)
    for c in range(16):
        gn = jnp.where(lb == c, shifted(f11[GN_ROWS * c:GN_ROWS * c + GN_ROWS, :], c - 8), gn)
    gns[...] = gn
    to_prv = pltpu.make_async_remote_copy(src_ref=gps, dst_ref=gpr, send_sem=gsend_sem.at[0], recv_sem=grecv_sem.at[0],
                                          device_id={'rows': prv}, device_id_type=MESH)
    to_nxt = pltpu.make_async_remote_copy(src_ref=gns, dst_ref=gnr, send_sem=gsend_sem.at[1], recv_sem=grecv_sem.at[1],
                                          device_id={'rows': nxt}, device_id_type=MESH)
    to_prv.start()
    to_nxt.start()

    for j in range(1, N_CHUNK - 1):
        merge_all(CHUNK_TILES[j], put_chunk)
        first_dft(j, gch[...])
        post(j)

    to_prv.wait()
    to_nxt.wait()
    gp, gn = gpr[...], gnr[...]
    for c in range(8):
        s = slice(Q_PAD * c, Q_PAD * c + Q_PAD)
        gch[s, LANES:WIDE] = (f11[s, :] + jnp.where((la >> 1) == 3, shifted(gp, 6 - 2 * c), 0.0)).astype(BF16)
    for c in range(16):
        s = slice(GN_ROWS * c, GN_ROWS * c + GN_ROWS)
        gch[s, 0:LANES] = (f0[s, :] + jnp.where(lb == 0, shifted(gn, -c), 0.0)).astype(BF16)
    first_dft(LAST, gch[...])
    post(LAST)

    d_all = d_ref[...].reshape(1, N_IMG)
    st[...] = jnp.zeros_like(st)
    for s in range(2):
        for c in range(4):
            st[s, c, 0:Q_BLK, 0:N_IMG] = s_ref[s, :, c, :]

    half_p = jnp.where(k == 0, d_all[:, 0:P_BLK], d_all[:, P_BLK:2 * P_BLK])
    part_q = d_all[:, 0:Q_BLK]
    for i in range(1, 4):
        part_q = jnp.where(r == i, d_all[:, Q_BLK * i:Q_BLK * (i + 1)], part_q)
    part_q = jnp.concatenate([part_q, jnp.zeros((1, LANES - Q_BLK), F32)], axis=1)
    dd[...] = jnp.broadcast_to(part_q, (8, LANES)).T[0:Q_BLK, 0:1] * half_p

    first_col = k == 0

    def second_dft(j, sub):
        row0, rows = SUBS[sub]
        for i in range(3):
            copy_of(j, sub, i, dests[i]).wait_recv()
        coil = (lax.broadcasted_iota(jnp.int32, (rows, LANES), 1) >> 4) & 3
        halves = []
        for pair in range(2):
            v = []
            for src in (2 * pair, 2 * pair + 1):
                if j_is_last(j):
                    at = SUBS_LAST[sub][0]
                    folded = recv_last[src, at + rows:at + rows + rows // 2]
                    v += [recv_last[src, at:at + rows], jnp.concatenate([folded, pltpu.roll(folded, LANES - 8, 1)], axis=0)]
                else:
                    v += [recv[j, src, pl.ds(row0, rows), LANES * t:LANES * (t + 1)] for t in range(2)]
            for bit in (1, 2):
                m = (coil & bit) == 0
                for t in range(4):
                    if t & bit:
                        continue
                    x, y = v[t], v[t | bit]
                    v[t] = jnp.where(m, x, pltpu.roll(y, ROWS * bit, 1))
                    v[t | bit] = jnp.where(m, pltpu.roll(x, LANES - ROWS * bit, 1), y)
            halves.append(v)
        lhs = jnp.concatenate([jnp.concatenate([halves[0][c], halves[1][c]], axis=1) for c in range(4)], axis=0)
        return jnp.dot(lhs, e2f[j], preferred_element_type=F32)

    img[...] = second_dft(0, FULL)
    for j in WHOLE[1:]:
        img[...] += second_dft(j, FULL)
    for sub in range(2):
        row0, rows = SUBS[sub]

        def accumulate(j, _):
            part = second_dft(j, sub)
            for c in range(4):
                img[Q_PAD * c + row0:Q_PAD * c + row0 + rows] += part[rows * c:rows * (c + 1)]
            return 0
        lax.fori_loop(N_WHOLE, N_WHOLE + 1, accumulate, 0)
        if sub == 0:
            post(N_CHUNK)
        lax.fori_loop(N_WHOLE + 1, LAST, accumulate, 0)
        accumulate(LAST, 0)

        x_re = jnp.zeros((rows, P_ALL), F32)
        x_im = jnp.zeros((rows, P_ALL), F32)
        for c in range(4):
            i_re = img[Q_PAD * c + row0:Q_PAD * c + row0 + rows, 0:P_ALL]
            i_im = img[Q_PAD * c + row0:Q_PAD * c + row0 + rows, P_ALL:P_TWO]
            s_re, s_im = st[0, c, row0:row0 + rows], st[1, c, row0:row0 + rows]
            x_re = x_re + s_re * i_re + s_im * i_im
            x_im = x_im + s_re * i_im - s_im * i_re
        lo = jnp.concatenate([x_re[:, 0:P_PAD], x_im[:, 0:P_PAD]], axis=1)
        hi = jnp.concatenate([x_re[:, P_BLK:P_BLK + P_PAD], x_im[:, P_BLK:P_BLK + P_PAD]], axis=1)
        psend[row0:row0 + rows] = jnp.where(first_col, hi, lo)
        swap(sub).start()
        mine[row0:row0 + rows] = jnp.where(first_col, lo, hi)

    for j, sub in SENT:
        for i in range(3):
            copy_of(j, sub, i, r).wait_send()
    for sub in range(2):
        swap(sub).wait()
        row0, rows = SUBS[sub]
        rows = min(rows, Q_BLK - row0)
        s = slice(row0, row0 + rows)
        total = mine[s] + precv[s]
        for i in range(2):
            out_ref[i, :, s] = (total[:, P_PAD * i:P_PAD * i + P_BLK] * dd[s]).T


def solution(mesh):
    sample_spec = ('exam', 'rows', 'cols')
    vmem = pl.BlockSpec(memory_space=pltpu.VMEM)
    hbm = pl.BlockSpec(memory_space=pltpu.HBM)
    sds = jax.ShapeDtypeStruct

    def local_fn(kspace, wts_y, wts_x, idx_y, idx_x, coil_maps, deapod):
        n = kspace.shape[2]
        e1, e2 = dft_constants()
        maps = jnp.transpose(coil_maps, (0, 3, 1, 2))
        acc_shape = [sds((N_SRC * VS, LANES), F32)] * (N_ACC)
        inputs = (kspace, wts_y, wts_x, idx_y.reshape(16, LANES), idx_x.reshape(16, LANES), e2)
        *samples, = pl.pallas_call(
            exchange_kernel,
            out_shape=[sds((2, 8, n), F32), sds((2, 4, n), F32), sds((2, 4, n), F32), sds((2, 16, LANES), jnp.int32),
                       sds((N_CHUNK, WIDE, P_TWO), BF16)] + acc_shape,
            in_specs=[hbm] * 6,
            out_specs=[vmem] * (5 + N_ACC),
            scratch_shapes=[pltpu.VMEM((KV, P_TWO), BF16), pltpu.VMEM((2, 8, n), F32), pltpu.VMEM((16, LANES), jnp.int32), pltpu.VMEM((16, LANES), jnp.int32),
                            pltpu.VMEM((8, n), F32), pltpu.SemaphoreType.DMA((6,)), pltpu.SemaphoreType.DMA((4,)),
                            pltpu.SemaphoreType.DMA((4,))],
            compiler_params=pltpu.CompilerParams(collective_id=0, has_side_effects=True, vmem_limit_bytes=8 * MIB),
            name='exchange',
        )(*[pltpu.with_memory_space_constraint(x, pltpu.HBM) for x in inputs])
        y8, wy, wx, place, e2f = samples[:5]
        accs = pl.pallas_call(
            spread_kernel,
            out_shape=acc_shape,
            in_specs=[vmem] * (4 + N_ACC),
            out_specs=[vmem] * (N_ACC),
            scratch_shapes=[pltpu.SMEM((2, 16, LANES), jnp.int32), pltpu.VMEM((2, 16, LANES), jnp.int32), pltpu.VMEM((2, 16, LANES), jnp.int32),
                            pltpu.SemaphoreType.DMA] + [pltpu.VMEM((WIDE, LANES), F32)] * 4,
            input_output_aliases={4 + i: i for i in range(N_ACC)},
            compiler_params=pltpu.CompilerParams(vmem_limit_bytes=8 * MIB),
            cost_estimate=pl.CostEstimate(flops=2 * 10**9, bytes_accessed=2 * 10**7, transcendentals=0),
            name='spread',
        )(place, y8, wy, wx, *samples[5:])
        return pl.pallas_call(
            transform_kernel,
            out_shape=sds((2, P_BLK, Q_BLK), F32),
            in_specs=[vmem] * (N_ACC + 4),
            out_specs=vmem,
            scratch_shapes=[pltpu.VMEM((2, 4, Q_PAD, P_ALL), F32), pltpu.VMEM((Q_BLK, P_BLK), F32), pltpu.VMEM((KV, WIDE), BF16)] + [pltpu.VMEM((KV, LANES), F32)] * 3 + [
                pltpu.VMEM((Q_PAD, LANES), F32),
                pltpu.VMEM((GN_ROWS, LANES), F32),
                pltpu.VMEM((LAST, 4, Q_PAD, WIDE), BF16),
                pltpu.VMEM((LAST, 4, Q_PAD, WIDE), BF16),
                pltpu.VMEM((4, 144, LANES), BF16),
                pltpu.VMEM((4, 144, LANES), BF16),
                pltpu.VMEM((Q_PAD, LANES), F32),
                pltpu.VMEM((GN_ROWS, LANES), F32),
                pltpu.VMEM((4 * Q_PAD, P_TWO), F32),
                pltpu.VMEM((Q_PAD, P_ALL), F32),
                pltpu.VMEM((Q_PAD, P_ALL), F32),
                pltpu.VMEM((Q_PAD, P_ALL), F32),
                pltpu.SemaphoreType.DMA((N_CHUNK, len(SUBS), 3)),
                pltpu.SemaphoreType.DMA((N_CHUNK, len(SUBS), 4)),
                pltpu.SemaphoreType.DMA((2,)),
                pltpu.SemaphoreType.DMA((2,)),
                pltpu.SemaphoreType.DMA((len(SUBS),)),
                pltpu.SemaphoreType.DMA((len(SUBS),)),
            ],
            compiler_params=pltpu.CompilerParams(collective_id=1, has_side_effects=True, vmem_limit_bytes=24 * MIB),
            name='transform',
        )(*accs, e1, e2f, maps, deapod)

    return jax.shard_map(
        local_fn,
        mesh=mesh,
        in_specs=(P(None, None, sample_spec), P(None, sample_spec), P(None, sample_spec), P(sample_spec), P(sample_spec), P(None, ('exam', 'cols'), None, 'rows'), P()),
        out_specs=P(None, ('exam', 'cols'), 'rows'),
        check_vma=False,
    )
```

```python
import math

import jax
import jax.numpy as jnp
import numpy as np
from jax import lax
from jax.experimental import pallas as pl
from jax.experimental.pallas import tpu as pltpu
from jax.sharding import PartitionSpec as P

F32, BF16 = jnp.float32, jnp.bfloat16
MESH = pl.DeviceIdType.MESH

N_IMG = 368
N_GRID = 736
ROW_BLK = 184
Q_BLK, Q_PAD = 92, 96
P_BLK, P_PAD, P_ALL = 184, 192, 384
N_CH = 8
TILE_U, STRIDE_U, N_SRC = 16, 13, 15
N_TGT = 12
COL_BLK = 368
VR = 384
VS = 392
KV = 2 * VR
LANES, ROWS = 128, 16
EDGE = 6
WIDE, P_TWO, GN_ROWS, MIB = 2 * LANES, 2 * P_ALL, 48, 2**20
N_CHUNK = 6
N_COPY = 3
N_ACC = 2 * N_COPY
SUBS = [(0, 64), (64, 32), (0, Q_PAD)]
FULL, N_WHOLE = 2, 2
WHOLE, SPLIT = range(N_WHOLE), range(N_WHOLE, N_CHUNK)
POSTS = [[(j, FULL)] for j in WHOLE] + [[(j, 0)] for j in SPLIT]
POSTS += [[(j, 1) for j in SPLIT]]
LAST = N_CHUNK - 1
SUBS_LAST = [(0, 96), (96, 48)]
SENT = [(j, FULL) for j in WHOLE] + [(j, sub) for j in SPLIT for sub in range(2)]
CHUNK_TILES = [(1 + 2 * j, 2 + 2 * j) for j in range(5)] + [(0, 11)]


def dft_constants():
    scale = 1.0 / math.sqrt(N_GRID)
    phase = ((np.arange(N_GRID)[:, None] - N_GRID // 2) * (np.arange(N_IMG)[None, :] - N_IMG // 2)) % N_GRID
    ang = phase.astype(np.float64) * (2.0 * math.pi / N_GRID)
    parts = (np.cos(ang) * scale, np.sin(ang) * scale)
    e1 = np.zeros((4, 2, Q_PAD, 2, VR))
    for dest in range(4):
        for cs in range(2):
            for half in range(2):
                part = parts[cs][half * COL_BLK:(half + 1) * COL_BLK, dest * Q_BLK:(dest + 1) * Q_BLK]
                e1[dest, cs, :Q_BLK, half, EDGE:EDGE + COL_BLK] = part.T
    e2 = np.zeros((N_CHUNK, 4, 2, TILE_U, 2, P_ALL))
    for j in range(N_CHUNK):
        for src in range(4):
            for tl in range(2):
                base = TILE_U * CHUNK_TILES[j][tl]
                rows = min(TILE_U, ROW_BLK - base)
                u0 = src * ROW_BLK + base
                for cs in range(2):
                    e2[j, src, tl, :rows, cs, :N_IMG] = parts[cs][u0:u0 + rows]
    return (jnp.asarray(e1.reshape(8 * Q_PAD, KV).astype(np.float32)).astype(BF16),
            jnp.asarray(e2.reshape(N_CHUNK * LANES, P_TWO).astype(np.float32)).astype(BF16))


def j_is_last(j):
    return isinstance(j, int) and j == LAST


def exchange_kernel(y_hbm, wy_hbm, wx_hbm, iy_hbm, ix_hbm, e2_hbm, y_ref, wy_ref, wx_ref, place_ref, e2f, q_own, *refs):
    accs = refs[:N_ACC]
    e2_ref, y_in, iy, ix, roff, y_send, in_sem, send_sem, recv_sem = refs[N_ACC:]
    k = lax.axis_index('cols')
    r = lax.axis_index('rows')
    other = {'cols': 1 - k}
    barrier = pltpu.get_barrier_semaphore()
    pl.semaphore_signal(barrier, inc=1, device_id=other, device_id_type=MESH)
    loads = [(iy_hbm, iy), (ix_hbm, ix), (y_hbm, y_in), (wy_hbm, wy_ref.at[0]), (wx_hbm, wx_ref.at[0]), (e2_hbm, e2_ref)]
    loads = [pltpu.make_async_copy(a, b, in_sem.at[i]) for i, (a, b) in enumerate(loads)]
    for c in loads:
        c.start()

    def send(i, src, dst):
        c = pltpu.make_async_remote_copy(src_ref=src, dst_ref=dst, send_sem=send_sem.at[i], recv_sem=recv_sem.at[i],
                                         device_id=other, device_id_type=MESH)
        c.start()
        return c

    loads[3].wait()
    loads[4].wait()
    pl.semaphore_wait(barrier, 1)
    copies = [send(0, wy_ref.at[0], wy_ref.at[1]), send(1, wx_ref.at[0], wx_ref.at[1])]
    loads[0].wait()
    loads[1].wait()
    row = iy[...] - r * ROW_BLK
    tile = jnp.zeros_like(row)
    for t in range(1, N_SRC):
        tile = tile + jnp.where(row >= STRIDE_U * t, 1, 0)
    roff[0] = (row + 14) & 15
    place_ref[0] = (tile * VS + (ix[...] - k * COL_BLK)) * ROWS + roff[0]
    loads[2].wait()
    y_re, y_im = y_in[0], y_in[1]
    low = jnp.concatenate([y_re[0:4], y_im[0:4]], axis=0)
    high = jnp.concatenate([y_re[4:8], y_im[4:8]], axis=0)
    y_ref[0] = jnp.where(k == 0, low, high)
    y_send[...] = jnp.where(k == 0, high, low)
    copies += [send(2, place_ref.at[0], place_ref.at[1]), send(3, y_send, y_ref.at[1])]

    def zero(i, _):
        for a in accs:
            a[pl.ds(pl.multiple_of(i * VS, 8), VS), :] = jnp.zeros((VS, LANES), F32)
        return 0
    lax.fori_loop(0, N_SRC, zero, 0)
    expand = expansion()

    def own_rows(i, _):
        q_own[pl.ds(pl.multiple_of(i * WIDE, WIDE), WIDE), :] = sample_rows(expand, i, 0, y_ref, wy_ref, roff)
        return 0
    lax.fori_loop(0, y_ref.shape[2] // WIDE, own_rows, 0)
    loads[-1].wait()
    for j in range(N_CHUNK):
        for h in range(2):
            v = e2_ref[LANES * j + 64 * h:LANES * j + 64 * h + 64, :]
            e2f[j, LANES * h:LANES * h + 64, :] = v
            e2f[j, LANES * h + 64:LANES * h + LANES, 0:P_ALL] = -v[:, P_ALL:P_TWO]
            e2f[j, LANES * h + 64:LANES * h + LANES, P_ALL:P_TWO] = v[:, 0:P_ALL]
    for c in copies:
        c.wait()


def split3(x):
    hi = x.astype(BF16).astype(F32)
    rest = x - hi
    mid = rest.astype(BF16).astype(F32)
    return [hi, mid, rest - mid]


def expansion():
    r0 = lax.broadcasted_iota(jnp.int32, (80, WIDE), 0)
    l0 = lax.broadcasted_iota(jnp.int32, (80, WIDE), 1)
    ry = (r0 < 24) & (l0 < LANES) & ((r0 & 7) == (l0 >> 4))
    rw = (r0 >= 24) & (r0 < 72) & (l0 >= LANES) & (((r0 - 24) & 15) == (l0 & 15))
    return jnp.where(ry | rw, 1.0, 0.0).astype(BF16)


def sample_rows(expand, i, slot, y_ref, wy_ref, roff):
    n_blk = y_ref.shape[2] // WIDE
    rr = lax.broadcasted_iota(jnp.int32, (ROWS, WIDE), 0)
    ds = [pl.ds(pl.multiple_of((i + n_blk * h) * LANES, LANES), LANES) for h in range(2)]
    y = jnp.concatenate([y_ref[slot, :, s] for s in ds], axis=1)
    wy = jnp.concatenate([wy_ref[slot, :, s] for s in ds], axis=1)
    d = (rr - jnp.concatenate([roff[slot, pl.ds(i + n_blk * h, 1), :] for h in range(2)], axis=1)) & 15
    w16 = jnp.zeros((ROWS, WIDE), F32)
    for a in range(4):
        w16 = jnp.where(d == a, wy[a:a + 1], w16)
    lhs = jnp.concatenate(split3(y) + split3(w16) + [jnp.zeros((8, WIDE), F32)], axis=0).astype(BF16)
    o = lax.dot_general(lhs, expand, (((0,), (0,)), ((), ())), preferred_element_type=F32)
    return o[:, :LANES] * o[:, LANES:]


def spread_kernel(place_ref, y_ref, wy_ref, wx_ref, q_own, *refs):
    accs = refs[N_ACC:4 * N_COPY]
    addr, addr_v, roff, sem, *q_refs = refs[4 * N_COPY:]
    place = place_ref[...]
    addr_v[...] = place >> 4
    roff[...] = place & 15
    to_smem = pltpu.make_async_copy(addr_v, addr, sem)
    to_smem.start()
    n = y_ref.shape[2]

    n_blk = n // WIDE

    expand = expansion()

    def prep(i, slot, q_ref):
        q_ref[...] = sample_rows(expand, i, slot, y_ref, wy_ref, roff)

    top = lax.broadcasted_iota(jnp.int32, (8, LANES), 0) < 4

    def scatter(i, q_nbr):
        first = pl.multiple_of(i * WIDE, WIDE)
        ds = [pl.ds(pl.multiple_of((i + n_blk * h) * LANES, LANES), LANES) for h in range(2)]
        wx = [jnp.concatenate([wx_ref[slot, :, s] for s in ds], axis=0) for slot in range(2)]
        for j in range(LANES):
            cols = [jnp.broadcast_to(wx[slot][:, j:j + 1], (8, LANES)) for slot in range(2)]
            for h in range(2):
                for slot in range(2):
                    acc = accs[slot * N_COPY + (2 * j + h) % N_COPY]
                    base = addr[slot, i + n_blk * h, j] + (0 if h else 4)
                    at = j + LANES * h
                    q = jnp.broadcast_to(q_nbr[at:at + 1, :] if slot else q_own[pl.ds(first + at, 1), :], (8, LANES))
                    if h:
                        s = pl.ds(base, 8)
                        acc[s, :] = acc[s, :] + jnp.where(top, 0.0, cols[slot]) * q
                    else:
                        s = pl.ds(base, 4)
                        acc[s, :] = acc[s, :] + cols[slot][0:4] * q[0:4]

    qa, qb = q_refs
    prep(0, 1, qa)
    to_smem.wait()

    def two_blocks(i, _):
        for step, now, then in ((0, qa, qb), (1, qb, qa)):
            prep(lax.rem(2 * i + step + 1, n_blk), 1, then)
            scatter(2 * i + step, now)
        return 0
    lax.fori_loop(0, n_blk // 2, two_blocks, 0)


def transform_kernel(*refs):
    own, nbr = refs[:N_COPY], refs[N_COPY:N_ACC]
    (e1_ref, e2f, s_ref, d_ref, out_ref, st, dd, gch, raw0, f0, f11, gps, gns, msg, recv, msg_last, recv_last, gpr, gnr, img, mine, psend, precv,
     msend_sem, mrecv_sem, gsend_sem, grecv_sem, psend_sem, precv_sem) = refs[N_ACC:]
    k = lax.axis_index('cols')
    r = lax.axis_index('rows')
    chip, core = r // 2, r % 2
    dests = [2 * (1 - chip) + core, 2 * (1 - chip) + (1 - core), 2 * chip + (1 - core)]
    nxt, prv = lax.rem(r + 1, 4), lax.rem(r + 3, 4)
    barrier = pltpu.get_barrier_semaphore()
    for d in dests:
        pl.semaphore_signal(barrier, inc=1, device_id={'rows': d}, device_id_type=MESH)
    pl.semaphore_signal(barrier, inc=1, device_id={'cols': 1 - k}, device_id_type=MESH)

    slots = ((own, k), (nbr, 1 - k))
    lane16 = lax.broadcasted_iota(jnp.int32, (ROWS, LANES), 1) & 15
    sub16 = lax.broadcasted_iota(jnp.int32, (ROWS, LANES), 0)

    def merged(accs, off, targets):
        wanted = {}
        for m in targets:
            deltas = {0: 0} if m is None else {t: STRIDE_U * t - TILE_U * m - 2 for t in range(N_SRC)}
            wanted[m] = {t: d for t, d in deltas.items() if abs(d) < ROWS}
        loaded = {}
        for t in sorted({t for w in wanted.values() for t in w}):
            s = pl.ds(t * VS + off, ROWS)
            v = accs[0][s, :]
            for acc in accs[1:]:
                v = v + acc[s, :]
            loaded[t] = v
        outs = []
        for m in targets:
            out = None
            for t, d in wanted[m].items():
                lo, hi = max(0, d), min(15, 15 + d)
                v = loaded[t]
                if lo > 0 or hi < 15:
                    v = jnp.where((lane16 >= lo) & (lane16 <= hi), v, 0.0)
                out = v if out is None else out + v
            outs.append(out)
        return outs

    def merge_all(targets, put):
        def rows(i, _):
            for step in range(2):
                for accs, half in slots:
                    off = pl.multiple_of((2 * i + 1 + step) * ROWS, ROWS)
                    put(pl.multiple_of(half * VR + off, ROWS), merged(accs, off, targets))
            return 0
        lax.fori_loop(0, VR // (2 * ROWS) - 1, rows, 0)
        last = VR - ROWS
        a = [merged(accs, 0, targets) for accs, _ in slots]
        b = [merged(accs, last, targets) for accs, _ in slots]
        for i, (_, half) in enumerate(slots):
            fix_a = [x + jnp.where(sub16 == 6, y, 0.0) for x, y in zip(a[i], b[1 - i])]
            fix_b = [y + jnp.where((sub16 == 4) | (sub16 == 5), x, 0.0) for x, y in zip(a[1 - i], b[i])]
            put(pl.multiple_of(half * VR, ROWS), fix_a)
            put(pl.multiple_of(half * VR + last, ROWS), fix_b)

    def put_chunk(off, vals):
        for i, v in enumerate(vals):
            gch[pl.ds(off, ROWS), LANES * i:LANES * (i + 1)] = v.astype(BF16)

    def put_edges(off, vals):
        for ref, v in zip((raw0, f0, f11), vals):
            ref[pl.ds(off, ROWS), :] = v

    lane = lax.broadcasted_iota(jnp.int32, (Q_PAD, WIDE), 1) & 127

    def swap(sub):
        rows = pl.ds(*SUBS[sub])
        return pltpu.make_async_remote_copy(src_ref=psend.at[rows], dst_ref=precv.at[rows], send_sem=psend_sem.at[sub],
                                            recv_sem=precv_sem.at[sub], device_id={'cols': 1 - k}, device_id_type=MESH)

    def first_dft(j, g):
        ab = jnp.dot(e1_ref[...], g, preferred_element_type=F32)
        for d in range(4):
            a = ab[192 * d:192 * d + Q_PAD]
            b = ab[192 * d + Q_PAD:192 * d + 192]
            b = jnp.concatenate([pltpu.roll(b[:, :128], 64, 1), pltpu.roll(b[:, 128:], 64, 1)], axis=1)
            h = jnp.where(lane < 64, a - b, a + b).astype(BF16)
            if not j_is_last(j):
                msg[j, d] = h
                continue
            for sub, (at, _) in enumerate(SUBS_LAST):
                row0, rows = SUBS[sub]
                half = rows // 2
                upper = h[row0:row0 + half, LANES:WIDE]
                lower = pltpu.roll(h[row0 + half:row0 + rows, LANES:WIDE], 8, 1)
                msg_last[d, at:at + rows] = h[row0:row0 + rows, 0:LANES]
                msg_last[d, at + rows:at + rows + half] = jnp.where((lane[0:half, 0:LANES] & 8) == 0, upper, lower)

    def copy_of(j, sub, i, slot):
        d = dests[i]
        if j_is_last(j):
            rows = pl.ds(*SUBS_LAST[sub])
            src, dst = msg_last.at[d, rows], recv_last.at[slot, rows]
        else:
            rows = pl.ds(*SUBS[sub])
            src, dst = msg.at[j, d, rows], recv.at[j, slot, rows]
        return pltpu.make_async_remote_copy(src_ref=src, dst_ref=dst, send_sem=msend_sem.at[j, sub, i],
                                            recv_sem=mrecv_sem.at[j, sub, slot], device_id={'rows': d}, device_id_type=MESH)

    def post(chunk):
        for j, sub in POSTS[chunk]:
            for i in range(3):
                copy_of(j, sub, i, r).start()
        if chunk < LAST:
            recv[chunk, r] = msg[chunk, r]
        elif chunk == LAST:
            recv_last[r] = msg_last[r]

    merge_all(CHUNK_TILES[0], put_chunk)
    first_dft(0, gch[...])
    pl.semaphore_wait(barrier, 4)
    post(0)

    merge_all((None, 0, N_TGT - 1), put_edges)
    la = lax.broadcasted_iota(jnp.int32, (Q_PAD, LANES), 1) & 15
    lb = lax.broadcasted_iota(jnp.int32, (GN_ROWS, LANES), 1) & 15

    def shifted(v, by):
        return pltpu.roll(v, by % LANES, 1) if by else v

    gp = jnp.zeros((Q_PAD, LANES), F32)
    for c in range(8):
        gp = jnp.where((la >> 1) == c, shifted(raw0[Q_PAD * c:Q_PAD * c + Q_PAD, :], 2 * c - 14), gp)
    gps[...] = gp
    gn = jnp.zeros((GN_ROWS, LANES), F32)
    for c in range(16):
        gn = jnp.where(lb == c, shifted(f11[GN_ROWS * c:GN_ROWS * c + GN_ROWS, :], c - 8), gn)
    gns[...] = gn
    to_prv = pltpu.make_async_remote_copy(src_ref=gps, dst_ref=gpr, send_sem=gsend_sem.at[0], recv_sem=grecv_sem.at[0],
                                          device_id={'rows': prv}, device_id_type=MESH)
    to_nxt = pltpu.make_async_remote_copy(src_ref=gns, dst_ref=gnr, send_sem=gsend_sem.at[1], recv_sem=grecv_sem.at[1],
                                          device_id={'rows': nxt}, device_id_type=MESH)
    to_prv.start()
    to_nxt.start()

    for j in range(1, N_CHUNK - 1):
        merge_all(CHUNK_TILES[j], put_chunk)
        first_dft(j, gch[...])
        post(j)

    to_prv.wait()
    to_nxt.wait()
    gp, gn = gpr[...], gnr[...]
    for c in range(8):
        s = slice(Q_PAD * c, Q_PAD * c + Q_PAD)
        gch[s, LANES:WIDE] = (f11[s, :] + jnp.where((la >> 1) == 3, shifted(gp, 6 - 2 * c), 0.0)).astype(BF16)
    for c in range(16):
        s = slice(GN_ROWS * c, GN_ROWS * c + GN_ROWS)
        gch[s, 0:LANES] = (f0[s, :] + jnp.where(lb == 0, shifted(gn, -c), 0.0)).astype(BF16)
    first_dft(LAST, gch[...])
    post(LAST)

    d_all = d_ref[...].reshape(1, N_IMG)
    st[...] = jnp.zeros_like(st)
    for s in range(2):
        for c in range(4):
            st[s, c, 0:Q_BLK, 0:N_IMG] = s_ref[s, :, c, :]

    half_p = jnp.where(k == 0, d_all[:, 0:P_BLK], d_all[:, P_BLK:2 * P_BLK])
    part_q = d_all[:, 0:Q_BLK]
    for i in range(1, 4):
        part_q = jnp.where(r == i, d_all[:, Q_BLK * i:Q_BLK * (i + 1)], part_q)
    part_q = jnp.concatenate([part_q, jnp.zeros((1, LANES - Q_BLK), F32)], axis=1)
    dd[...] = jnp.broadcast_to(part_q, (8, LANES)).T[0:Q_BLK, 0:1] * half_p

    first_col = k == 0

    def second_dft(j, sub):
        row0, rows = SUBS[sub]
        for i in range(3):
            copy_of(j, sub, i, dests[i]).wait_recv()
        coil = (lax.broadcasted_iota(jnp.int32, (rows, LANES), 1) >> 4) & 3
        halves = []
        for pair in range(2):
            v = []
            for src in (2 * pair, 2 * pair + 1):
                if j_is_last(j):
                    at = SUBS_LAST[sub][0]
                    folded = recv_last[src, at + rows:at + rows + rows // 2]
                    v += [recv_last[src, at:at + rows], jnp.concatenate([folded, pltpu.roll(folded, LANES - 8, 1)], axis=0)]
                else:
                    v += [recv[j, src, pl.ds(row0, rows), LANES * t:LANES * (t + 1)] for t in range(2)]
            for bit in (1, 2):
                m = (coil & bit) == 0
                for t in range(4):
                    if t & bit:
                        continue
                    x, y = v[t], v[t | bit]
                    v[t] = jnp.where(m, x, pltpu.roll(y, ROWS * bit, 1))
                    v[t | bit] = jnp.where(m, pltpu.roll(x, LANES - ROWS * bit, 1), y)
            halves.append(v)
        lhs = jnp.concatenate([jnp.concatenate([halves[0][c], halves[1][c]], axis=1) for c in range(4)], axis=0)
        return jnp.dot(lhs, e2f[j], preferred_element_type=F32)

    img[...] = second_dft(0, FULL)
    for j in WHOLE[1:]:
        img[...] += second_dft(j, FULL)
    for sub in range(2):
        row0, rows = SUBS[sub]

        def accumulate(j, _):
            part = second_dft(j, sub)
            for c in range(4):
                img[Q_PAD * c + row0:Q_PAD * c + row0 + rows] += part[rows * c:rows * (c + 1)]
            return 0
        lax.fori_loop(N_WHOLE, N_WHOLE + 1, accumulate, 0)
        if sub == 0:
            post(N_CHUNK)
        lax.fori_loop(N_WHOLE + 1, LAST, accumulate, 0)
        accumulate(LAST, 0)

        x_re = jnp.zeros((rows, P_ALL), F32)
        x_im = jnp.zeros((rows, P_ALL), F32)
        for c in range(4):
            i_re = img[Q_PAD * c + row0:Q_PAD * c + row0 + rows, 0:P_ALL]
            i_im = img[Q_PAD * c + row0:Q_PAD * c + row0 + rows, P_ALL:P_TWO]
            s_re, s_im = st[0, c, row0:row0 + rows], st[1, c, row0:row0 + rows]
            x_re = x_re + s_re * i_re + s_im * i_im
            x_im = x_im + s_re * i_im - s_im * i_re
        lo = jnp.concatenate([x_re[:, 0:P_PAD], x_im[:, 0:P_PAD]], axis=1)
        hi = jnp.concatenate([x_re[:, P_BLK:P_BLK + P_PAD], x_im[:, P_BLK:P_BLK + P_PAD]], axis=1)
        psend[row0:row0 + rows] = jnp.where(first_col, hi, lo)
        swap(sub).start()
        mine[row0:row0 + rows] = jnp.where(first_col, lo, hi)

    for j, sub in SENT:
        for i in range(3):
            copy_of(j, sub, i, r).wait_send()
    for sub in range(2):
        swap(sub).wait()
        row0, rows = SUBS[sub]
        rows = min(rows, Q_BLK - row0)
        s = slice(row0, row0 + rows)
        total = mine[s] + precv[s]
        for i in range(2):
            out_ref[i, :, s] = (total[:, P_PAD * i:P_PAD * i + P_BLK] * dd[s]).T


def solution(mesh):
    sample_spec = ('exam', 'rows', 'cols')
    vmem = pl.BlockSpec(memory_space=pltpu.VMEM)
    hbm = pl.BlockSpec(memory_space=pltpu.HBM)
    sds = jax.ShapeDtypeStruct

    def local_fn(kspace, wts_y, wts_x, idx_y, idx_x, coil_maps, deapod):
        n = kspace.shape[2]
        e1, e2 = dft_constants()
        maps = jnp.transpose(coil_maps, (0, 3, 1, 2))
        acc_shape = [sds((N_SRC * VS, LANES), F32)] * (N_ACC)
        inputs = (kspace, wts_y, wts_x, idx_y.reshape(16, LANES), idx_x.reshape(16, LANES), e2)
        *samples, = pl.pallas_call(
            exchange_kernel,
            out_shape=[sds((2, 8, n), F32), sds((2, 4, n), F32), sds((2, 4, n), F32), sds((2, 16, LANES), jnp.int32),
                       sds((N_CHUNK, WIDE, P_TWO), BF16), sds((n, LANES), F32)] + acc_shape,
            in_specs=[hbm] * 6,
            out_specs=[vmem] * (6 + N_ACC),
            scratch_shapes=[pltpu.VMEM((KV, P_TWO), BF16), pltpu.VMEM((2, 8, n), F32), pltpu.VMEM((16, LANES), jnp.int32), pltpu.VMEM((16, LANES), jnp.int32),
                            pltpu.VMEM((1, 16, LANES), jnp.int32),
                            pltpu.VMEM((8, n), F32), pltpu.SemaphoreType.DMA((6,)), pltpu.SemaphoreType.DMA((4,)),
                            pltpu.SemaphoreType.DMA((4,))],
            compiler_params=pltpu.CompilerParams(collective_id=0, has_side_effects=True, vmem_limit_bytes=8 * MIB),
            name='exchange',
        )(*[pltpu.with_memory_space_constraint(x, pltpu.HBM) for x in inputs])
        y8, wy, wx, place, e2f, q_own = samples[:6]
        accs = pl.pallas_call(
            spread_kernel,
            out_shape=acc_shape,
            in_specs=[vmem] * (5 + N_ACC),
            out_specs=[vmem] * (N_ACC),
            scratch_shapes=[pltpu.SMEM((2, 16, LANES), jnp.int32), pltpu.VMEM((2, 16, LANES), jnp.int32), pltpu.VMEM((2, 16, LANES), jnp.int32),
                            pltpu.SemaphoreType.DMA] + [pltpu.VMEM((WIDE, LANES), F32)] * 2,
            input_output_aliases={5 + i: i for i in range(N_ACC)},
            compiler_params=pltpu.CompilerParams(vmem_limit_bytes=8 * MIB),
            cost_estimate=pl.CostEstimate(flops=2 * 10**9, bytes_accessed=2 * 10**7, transcendentals=0),
            name='spread',
        )(place, y8, wy, wx, q_own, *samples[6:])
        return pl.pallas_call(
            transform_kernel,
            out_shape=sds((2, P_BLK, Q_BLK), F32),
            in_specs=[vmem] * (N_ACC + 4),
            out_specs=vmem,
            scratch_shapes=[pltpu.VMEM((2, 4, Q_PAD, P_ALL), F32), pltpu.VMEM((Q_BLK, P_BLK), F32), pltpu.VMEM((KV, WIDE), BF16)] + [pltpu.VMEM((KV, LANES), F32)] * 3 + [
                pltpu.VMEM((Q_PAD, LANES), F32),
                pltpu.VMEM((GN_ROWS, LANES), F32),
                pltpu.VMEM((LAST, 4, Q_PAD, WIDE), BF16),
                pltpu.VMEM((LAST, 4, Q_PAD, WIDE), BF16),
                pltpu.VMEM((4, 144, LANES), BF16),
                pltpu.VMEM((4, 144, LANES), BF16),
                pltpu.VMEM((Q_PAD, LANES), F32),
                pltpu.VMEM((GN_ROWS, LANES), F32),
                pltpu.VMEM((4 * Q_PAD, P_TWO), F32),
                pltpu.VMEM((Q_PAD, P_ALL), F32),
                pltpu.VMEM((Q_PAD, P_ALL), F32),
                pltpu.VMEM((Q_PAD, P_ALL), F32),
                pltpu.SemaphoreType.DMA((N_CHUNK, len(SUBS), 3)),
                pltpu.SemaphoreType.DMA((N_CHUNK, len(SUBS), 4)),
                pltpu.SemaphoreType.DMA((2,)),
                pltpu.SemaphoreType.DMA((2,)),
                pltpu.SemaphoreType.DMA((len(SUBS),)),
                pltpu.SemaphoreType.DMA((len(SUBS),)),
            ],
            compiler_params=pltpu.CompilerParams(collective_id=1, has_side_effects=True, vmem_limit_bytes=24 * MIB),
            name='transform',
        )(*accs, e1, e2f, maps, deapod)

    return jax.shard_map(
        local_fn,
        mesh=mesh,
        in_specs=(P(None, None, sample_spec), P(None, sample_spec), P(None, sample_spec), P(sample_spec), P(sample_spec), P(None, ('exam', 'cols'), None, 'rows'), P()),
        out_specs=P(None, ('exam', 'cols'), 'rows'),
        check_vma=False,
    )
```

```python
import math

import jax
import jax.numpy as jnp
import numpy as np
from jax import lax
from jax.experimental import pallas as pl
from jax.experimental.pallas import tpu as pltpu
from jax.sharding import PartitionSpec as P

F32, BF16 = jnp.float32, jnp.bfloat16
MESH = pl.DeviceIdType.MESH

N_IMG = 368
N_GRID = 736
ROW_BLK = 184
Q_BLK, Q_PAD = 92, 96
P_BLK, P_PAD, P_ALL = 184, 192, 384
N_CH = 8
TILE_U, STRIDE_U, N_SRC = 16, 13, 15
N_TGT = 12
COL_BLK = 368
VR = 384
VS = 392
KV = 2 * VR
LANES, ROWS = 128, 16
EDGE = 6
WIDE, P_TWO, GN_ROWS, MIB = 2 * LANES, 2 * P_ALL, 48, 2**20
N_CHUNK = 6
N_COPY = 3
N_ACC = 2 * N_COPY
SUBS = [(0, 64), (64, 32), (0, Q_PAD)]
FULL, N_WHOLE = 2, 2
WHOLE, SPLIT = range(N_WHOLE), range(N_WHOLE, N_CHUNK)
POSTS = [[(j, FULL)] for j in WHOLE] + [[(j, 0)] for j in SPLIT]
POSTS += [[(j, 1) for j in SPLIT]]
LAST = N_CHUNK - 1
SUBS_LAST = [(0, 96), (96, 48)]
SENT = [(j, FULL) for j in WHOLE] + [(j, sub) for j in SPLIT for sub in range(2)]
CHUNK_TILES = [(1 + 2 * j, 2 + 2 * j) for j in range(5)] + [(0, 11)]


def dft_constants():
    scale = 1.0 / math.sqrt(N_GRID)
    phase = ((np.arange(N_GRID)[:, None] - N_GRID // 2) * (np.arange(N_IMG)[None, :] - N_IMG // 2)) % N_GRID
    ang = phase.astype(np.float64) * (2.0 * math.pi / N_GRID)
    parts = (np.cos(ang) * scale, np.sin(ang) * scale)
    e1 = np.zeros((4, 2, Q_PAD, 2, VR))
    for dest in range(4):
        for cs in range(2):
            for half in range(2):
                part = parts[cs][half * COL_BLK:(half + 1) * COL_BLK, dest * Q_BLK:(dest + 1) * Q_BLK]
                e1[dest, cs, :Q_BLK, half, EDGE:EDGE + COL_BLK] = part.T
    e2 = np.zeros((N_CHUNK, 4, 2, TILE_U, 2, P_ALL))
    for j in range(N_CHUNK):
        for src in range(4):
            for tl in range(2):
                base = TILE_U * CHUNK_TILES[j][tl]
                rows = min(TILE_U, ROW_BLK - base)
                u0 = src * ROW_BLK + base
                for cs in range(2):
                    e2[j, src, tl, :rows, cs, :N_IMG] = parts[cs][u0:u0 + rows]
    return (jnp.asarray(e1.reshape(8 * Q_PAD, KV).astype(np.float32)).astype(BF16),
            jnp.asarray(e2.reshape(N_CHUNK * LANES, P_TWO).astype(np.float32)).astype(BF16))


def j_is_last(j):
    return isinstance(j, int) and j == LAST


def exchange_kernel(y_hbm, wy_hbm, wx_hbm, iy_hbm, ix_hbm, e2_hbm, y_ref, wy_ref, wx_ref, place_ref, e2f, q_own, *refs):
    accs = refs[:N_ACC]
    e2_ref, y_in, iy, ix, roff, y_send, in_sem, send_sem, recv_sem = refs[N_ACC:]
    k = lax.axis_index('cols')
    r = lax.axis_index('rows')
    other = {'cols': 1 - k}
    barrier = pltpu.get_barrier_semaphore()
    pl.semaphore_signal(barrier, inc=1, device_id=other, device_id_type=MESH)
    loads = [(iy_hbm, iy), (ix_hbm, ix), (y_hbm, y_in), (wy_hbm, wy_ref.at[0]), (wx_hbm, wx_ref.at[0]), (e2_hbm, e2_ref)]
    loads = [pltpu.make_async_copy(a, b, in_sem.at[i]) for i, (a, b) in enumerate(loads)]
    for c in loads:
        c.start()

    def send(i, src, dst):
        c = pltpu.make_async_remote_copy(src_ref=src, dst_ref=dst, send_sem=send_sem.at[i], recv_sem=recv_sem.at[i],
                                         device_id=other, device_id_type=MESH)
        c.start()
        return c

    loads[3].wait()
    loads[4].wait()
    pl.semaphore_wait(barrier, 1)
    copies = [send(0, wy_ref.at[0], wy_ref.at[1]), send(1, wx_ref.at[0], wx_ref.at[1])]
    loads[0].wait()
    loads[1].wait()
    row = iy[...] - r * ROW_BLK
    tile = jnp.zeros_like(row)
    for t in range(1, N_SRC):
        tile = tile + jnp.where(row >= STRIDE_U * t, 1, 0)
    roff[0] = (row + 14) & 15
    place_ref[0] = (tile * VS + (ix[...] - k * COL_BLK)) * ROWS + roff[0]
    loads[2].wait()
    y_re, y_im = y_in[0], y_in[1]
    low = jnp.concatenate([y_re[0:4], y_im[0:4]], axis=0)
    high = jnp.concatenate([y_re[4:8], y_im[4:8]], axis=0)
    y_ref[0] = jnp.where(k == 0, low, high)
    y_send[...] = jnp.where(k == 0, high, low)
    copies += [send(2, place_ref.at[0], place_ref.at[1]), send(3, y_send, y_ref.at[1])]

    def zero(i, _):
        for a in accs:
            a[pl.ds(pl.multiple_of(i * VS, 8), VS), :] = jnp.zeros((VS, LANES), F32)
        return 0
    lax.fori_loop(0, N_SRC, zero, 0)
    expand = expansion()

    def own_rows(i, _):
        q_own[pl.ds(pl.multiple_of(i * WIDE, WIDE), WIDE), :] = sample_rows(expand, i, 0, y_ref, wy_ref, roff)
        return 0
    lax.fori_loop(0, y_ref.shape[2] // WIDE, own_rows, 0)
    loads[-1].wait()
    for j in range(N_CHUNK):
        for h in range(2):
            v = e2_ref[LANES * j + 64 * h:LANES * j + 64 * h + 64, :]
            e2f[j, LANES * h:LANES * h + 64, :] = v
            e2f[j, LANES * h + 64:LANES * h + LANES, 0:P_ALL] = -v[:, P_ALL:P_TWO]
            e2f[j, LANES * h + 64:LANES * h + LANES, P_ALL:P_TWO] = v[:, 0:P_ALL]
    for c in copies:
        c.wait()


def split3(x):
    hi = x.astype(BF16).astype(F32)
    rest = x - hi
    mid = rest.astype(BF16).astype(F32)
    return [hi, mid, rest - mid]


def expansion():
    r0 = lax.broadcasted_iota(jnp.int32, (80, WIDE), 0)
    l0 = lax.broadcasted_iota(jnp.int32, (80, WIDE), 1)
    ry = (r0 < 24) & (l0 < LANES) & ((r0 & 7) == (l0 >> 4))
    rw = (r0 >= 24) & (r0 < 72) & (l0 >= LANES) & (((r0 - 24) & 15) == (l0 & 15))
    return jnp.where(ry | rw, 1.0, 0.0).astype(BF16)


def sample_rows(expand, i, slot, y_ref, wy_ref, roff):
    n_blk = y_ref.shape[2] // WIDE
    rr = lax.broadcasted_iota(jnp.int32, (ROWS, WIDE), 0)
    ds = [pl.ds(pl.multiple_of((i + n_blk * h) * LANES, LANES), LANES) for h in range(2)]
    y = jnp.concatenate([y_ref[slot, :, s] for s in ds], axis=1)
    wy = jnp.concatenate([wy_ref[slot, :, s] for s in ds], axis=1)
    d = (rr - jnp.concatenate([roff[slot, pl.ds(i + n_blk * h, 1), :] for h in range(2)], axis=1)) & 15
    w16 = jnp.zeros((ROWS, WIDE), F32)
    for a in range(4):
        w16 = jnp.where(d == a, wy[a:a + 1], w16)
    lhs = jnp.concatenate(split3(y) + split3(w16) + [jnp.zeros((8, WIDE), F32)], axis=0).astype(BF16)
    o = lax.dot_general(lhs, expand, (((0,), (0,)), ((), ())), preferred_element_type=F32)
    return o[:, :LANES] * o[:, LANES:]


def spread_kernel(place_ref, y_ref, wy_ref, wx_ref, q_own, *refs):
    accs = refs[N_ACC:4 * N_COPY]
    addr, addr_v, roff, sem, *q_refs = refs[4 * N_COPY:]
    place = place_ref[...]
    addr_v[...] = place >> 4
    roff[...] = place & 15
    to_smem = pltpu.make_async_copy(addr_v, addr, sem)
    to_smem.start()
    n = y_ref.shape[2]

    n_blk = n // WIDE

    expand = expansion()

    def prep(i, slot, q_ref):
        q_ref[...] = sample_rows(expand, i, slot, y_ref, wy_ref, roff)

    top = lax.broadcasted_iota(jnp.int32, (8, LANES), 0) < 4

    def scatter(i, q_nbr):
        first = pl.multiple_of(i * WIDE, WIDE)
        ds = [pl.ds(pl.multiple_of((i + n_blk * h) * LANES, LANES), LANES) for h in range(2)]
        wx = [jnp.concatenate([wx_ref[slot, :, s] for s in ds], axis=0) for slot in range(2)]
        for j in range(LANES):
            cols = [jnp.broadcast_to(wx[slot][:, j:j + 1], (8, LANES)) for slot in range(2)]
            for h in range(2):
                for slot in range(2):
                    acc = accs[slot * N_COPY + (2 * j + h) % N_COPY]
                    base = addr[slot, i + n_blk * h, j] + (0 if h else 4)
                    at = j + LANES * h
                    q = jnp.broadcast_to(q_nbr[at:at + 1, :] if slot else q_own[pl.ds(first + at, 1), :], (8, LANES))
                    if h:
                        s = pl.ds(base, 8)
                        acc[s, :] = acc[s, :] + jnp.where(top, 0.0, cols[slot]) * q
                    else:
                        s = pl.ds(base, 4)
                        acc[s, :] = acc[s, :] + cols[slot][0:4] * q[0:4]

    qa, qb = q_refs
    prep(0, 1, qa)
    to_smem.wait()

    def two_blocks(i, _):
        for step, now, then in ((0, qa, qb), (1, qb, qa)):
            prep(lax.rem(2 * i + step + 1, n_blk), 1, then)
            scatter(2 * i + step, now)
        return 0
    lax.fori_loop(0, n_blk // 2, two_blocks, 0)


def transform_kernel(*refs):
    own, nbr = refs[:N_COPY], refs[N_COPY:N_ACC]
    (e1_ref, e2f, s_ref, d_ref, out_ref, st, dd, gch, raw0, f0, f11, gps, gns, msg, recv, msg_last, recv_last, gpr, gnr, img, mine, psend, precv,
     msend_sem, mrecv_sem, gsend_sem, grecv_sem, psend_sem, precv_sem) = refs[N_ACC:]
    k = lax.axis_index('cols')
    r = lax.axis_index('rows')
    chip, core = r // 2, r % 2
    dests = [2 * (1 - chip) + core, 2 * (1 - chip) + (1 - core), 2 * chip + (1 - core)]
    nxt, prv = lax.rem(r + 1, 4), lax.rem(r + 3, 4)
    barrier = pltpu.get_barrier_semaphore()
    for d in dests:
        pl.semaphore_signal(barrier, inc=1, device_id={'rows': d}, device_id_type=MESH)
    pl.semaphore_signal(barrier, inc=1, device_id={'cols': 1 - k}, device_id_type=MESH)

    slots = ((own, k), (nbr, 1 - k))
    lane16 = lax.broadcasted_iota(jnp.int32, (ROWS, LANES), 1) & 15
    sub16 = lax.broadcasted_iota(jnp.int32, (ROWS, LANES), 0)

    def merged(accs, off, targets):
        wanted = {}
        for m in targets:
            deltas = {0: 0} if m is None else {t: STRIDE_U * t - TILE_U * m - 2 for t in range(N_SRC)}
            wanted[m] = {t: d for t, d in deltas.items() if abs(d) < ROWS}
        loaded = {}
        for t in sorted({t for w in wanted.values() for t in w}):
            s = pl.ds(t * VS + off, ROWS)
            v = accs[0][s, :]
            for acc in accs[1:]:
                v = v + acc[s, :]
            loaded[t] = v
        outs = []
        for m in targets:
            out = None
            for t, d in wanted[m].items():
                lo, hi = max(0, d), min(15, 15 + d)
                v = loaded[t]
                if lo > 0 or hi < 15:
                    v = jnp.where((lane16 >= lo) & (lane16 <= hi), v, 0.0)
                out = v if out is None else out + v
            outs.append(out)
        return outs

    def merge_all(targets, put):
        def rows(i, _):
            for step in range(2):
                for accs, half in slots:
                    off = pl.multiple_of((2 * i + 1 + step) * ROWS, ROWS)
                    put(pl.multiple_of(half * VR + off, ROWS), merged(accs, off, targets))
            return 0
        lax.fori_loop(0, VR // (2 * ROWS) - 1, rows, 0)
        last = VR - ROWS
        a = [merged(accs, 0, targets) for accs, _ in slots]
        b = [merged(accs, last, targets) for accs, _ in slots]
        for i, (_, half) in enumerate(slots):
            fix_a = [x + jnp.where(sub16 == 6, y, 0.0) for x, y in zip(a[i], b[1 - i])]
            fix_b = [y + jnp.where((sub16 == 4) | (sub16 == 5), x, 0.0) for x, y in zip(a[1 - i], b[i])]
            put(pl.multiple_of(half * VR, ROWS), fix_a)
            put(pl.multiple_of(half * VR + last, ROWS), fix_b)

    def put_chunk(off, vals):
        for i, v in enumerate(vals):
            gch[pl.ds(off, ROWS), LANES * i:LANES * (i + 1)] = v.astype(BF16)

    def put_edges(off, vals):
        for ref, v in zip((raw0, f0, f11), vals):
            ref[pl.ds(off, ROWS), :] = v

    lane = lax.broadcasted_iota(jnp.int32, (Q_PAD, WIDE), 1) & 127

    def swap(sub):
        rows = pl.ds(*SUBS[sub])
        return pltpu.make_async_remote_copy(src_ref=psend.at[rows], dst_ref=precv.at[rows], send_sem=psend_sem.at[sub],
                                            recv_sem=precv_sem.at[sub], device_id={'cols': 1 - k}, device_id_type=MESH)

    def first_dft_of(j, g, which):
        rows = pl.ds(pl.multiple_of(P_ALL * which, P_ALL), P_ALL)
        ab = jnp.dot(e1_ref[rows, :], g, preferred_element_type=F32)
        for d in range(2):
            a = ab[P_PAD * d:P_PAD * d + Q_PAD]
            b = ab[P_PAD * d + Q_PAD:P_PAD * (d + 1)]
            b = jnp.concatenate([pltpu.roll(b[:, :LANES], 64, 1), pltpu.roll(b[:, LANES:], 64, 1)], axis=1)
            msg[j, 2 * which + d] = jnp.where(lane < 64, a - b, a + b).astype(BF16)

    def first_dft(j, g):
        ab = jnp.dot(e1_ref[...], g, preferred_element_type=F32)
        for d in range(4):
            a = ab[192 * d:192 * d + Q_PAD]
            b = ab[192 * d + Q_PAD:192 * d + 192]
            b = jnp.concatenate([pltpu.roll(b[:, :128], 64, 1), pltpu.roll(b[:, 128:], 64, 1)], axis=1)
            h = jnp.where(lane < 64, a - b, a + b).astype(BF16)
            if not j_is_last(j):
                msg[j, d] = h
                continue
            for sub, (at, _) in enumerate(SUBS_LAST):
                row0, rows = SUBS[sub]
                half = rows // 2
                upper = h[row0:row0 + half, LANES:WIDE]
                lower = pltpu.roll(h[row0 + half:row0 + rows, LANES:WIDE], 8, 1)
                msg_last[d, at:at + rows] = h[row0:row0 + rows, 0:LANES]
                msg_last[d, at + rows:at + rows + half] = jnp.where((lane[0:half, 0:LANES] & 8) == 0, upper, lower)

    def copy_of(j, sub, i, slot):
        d = dests[i]
        if j_is_last(j):
            rows = pl.ds(*SUBS_LAST[sub])
            src, dst = msg_last.at[d, rows], recv_last.at[slot, rows]
        else:
            rows = pl.ds(*SUBS[sub])
            src, dst = msg.at[j, d, rows], recv.at[j, slot, rows]
        return pltpu.make_async_remote_copy(src_ref=src, dst_ref=dst, send_sem=msend_sem.at[j, sub, i],
                                            recv_sem=mrecv_sem.at[j, sub, slot], device_id={'rows': d}, device_id_type=MESH)

    def post(chunk):
        for j, sub in POSTS[chunk]:
            for i in range(3):
                copy_of(j, sub, i, r).start()
        if chunk < LAST:
            recv[chunk, r] = msg[chunk, r]
        elif chunk == LAST:
            recv_last[r] = msg_last[r]

    merge_all(CHUNK_TILES[0], put_chunk)
    first_dft_of(0, gch[...], 1 - chip)
    pl.semaphore_wait(barrier, 4)
    for i in range(2):
        copy_of(0, FULL, i, r).start()
    first_dft_of(0, gch[...], chip)
    copy_of(0, FULL, 2, r).start()
    recv[0, r] = msg[0, r]

    merge_all((None, 0, N_TGT - 1), put_edges)
    la = lax.broadcasted_iota(jnp.int32, (Q_PAD, LANES), 1) & 15
    lb = lax.broadcasted_iota(jnp.int32, (GN_ROWS, LANES), 1) & 15

    def shifted(v, by):
        return pltpu.roll(v, by % LANES, 1) if by else v

    gp = jnp.zeros((Q_PAD, LANES), F32)
    for c in range(8):
        gp = jnp.where((la >> 1) == c, shifted(raw0[Q_PAD * c:Q_PAD * c + Q_PAD, :], 2 * c - 14), gp)
    gps[...] = gp
    gn = jnp.zeros((GN_ROWS, LANES), F32)
    for c in range(16):
        gn = jnp.where(lb == c, shifted(f11[GN_ROWS * c:GN_ROWS * c + GN_ROWS, :], c - 8), gn)
    gns[...] = gn
    to_prv = pltpu.make_async_remote_copy(src_ref=gps, dst_ref=gpr, send_sem=gsend_sem.at[0], recv_sem=grecv_sem.at[0],
                                          device_id={'rows': prv}, device_id_type=MESH)
    to_nxt = pltpu.make_async_remote_copy(src_ref=gns, dst_ref=gnr, send_sem=gsend_sem.at[1], recv_sem=grecv_sem.at[1],
                                          device_id={'rows': nxt}, device_id_type=MESH)
    to_prv.start()
    to_nxt.start()

    for j in range(1, N_CHUNK - 1):
        merge_all(CHUNK_TILES[j], put_chunk)
        first_dft(j, gch[...])
        post(j)

    to_prv.wait()
    to_nxt.wait()
    gp, gn = gpr[...], gnr[...]
    for c in range(8):
        s = slice(Q_PAD * c, Q_PAD * c + Q_PAD)
        gch[s, LANES:WIDE] = (f11[s, :] + jnp.where((la >> 1) == 3, shifted(gp, 6 - 2 * c), 0.0)).astype(BF16)
    for c in range(16):
        s = slice(GN_ROWS * c, GN_ROWS * c + GN_ROWS)
        gch[s, 0:LANES] = (f0[s, :] + jnp.where(lb == 0, shifted(gn, -c), 0.0)).astype(BF16)
    first_dft(LAST, gch[...])
    post(LAST)

    d_all = d_ref[...].reshape(1, N_IMG)
    st[...] = jnp.zeros_like(st)
    for s in range(2):
        for c in range(4):
            st[s, c, 0:Q_BLK, 0:N_IMG] = s_ref[s, :, c, :]

    half_p = jnp.where(k == 0, d_all[:, 0:P_BLK], d_all[:, P_BLK:2 * P_BLK])
    part_q = d_all[:, 0:Q_BLK]
    for i in range(1, 4):
        part_q = jnp.where(r == i, d_all[:, Q_BLK * i:Q_BLK * (i + 1)], part_q)
    part_q = jnp.concatenate([part_q, jnp.zeros((1, LANES - Q_BLK), F32)], axis=1)
    dd[...] = jnp.broadcast_to(part_q, (8, LANES)).T[0:Q_BLK, 0:1] * half_p

    first_col = k == 0

    def second_dft(j, sub):
        row0, rows = SUBS[sub]
        for i in range(3):
            copy_of(j, sub, i, dests[i]).wait_recv()
        coil = (lax.broadcasted_iota(jnp.int32, (rows, LANES), 1) >> 4) & 3
        halves = []
        for pair in range(2):
            v = []
            for src in (2 * pair, 2 * pair + 1):
                if j_is_last(j):
                    at = SUBS_LAST[sub][0]
                    folded = recv_last[src, at + rows:at + rows + rows // 2]
                    v += [recv_last[src, at:at + rows], jnp.concatenate([folded, pltpu.roll(folded, LANES - 8, 1)], axis=0)]
                else:
                    v += [recv[j, src, pl.ds(row0, rows), LANES * t:LANES * (t + 1)] for t in range(2)]
            for bit in (1, 2):
                m = (coil & bit) == 0
                for t in range(4):
                    if t & bit:
                        continue
                    x, y = v[t], v[t | bit]
                    v[t] = jnp.where(m, x, pltpu.roll(y, ROWS * bit, 1))
                    v[t | bit] = jnp.where(m, pltpu.roll(x, LANES - ROWS * bit, 1), y)
            halves.append(v)
        lhs = jnp.concatenate([jnp.concatenate([halves[0][c], halves[1][c]], axis=1) for c in range(4)], axis=0)
        return jnp.dot(lhs, e2f[j], preferred_element_type=F32)

    img[...] = second_dft(0, FULL)
    for j in WHOLE[1:]:
        img[...] += second_dft(j, FULL)
    for sub in range(2):
        row0, rows = SUBS[sub]

        def accumulate(j, _):
            part = second_dft(j, sub)
            for c in range(4):
                img[Q_PAD * c + row0:Q_PAD * c + row0 + rows] += part[rows * c:rows * (c + 1)]
            return 0
        lax.fori_loop(N_WHOLE, N_WHOLE + 1, accumulate, 0)
        if sub == 0:
            post(N_CHUNK)
        lax.fori_loop(N_WHOLE + 1, LAST, accumulate, 0)
        accumulate(LAST, 0)

        x_re = jnp.zeros((rows, P_ALL), F32)
        x_im = jnp.zeros((rows, P_ALL), F32)
        for c in range(4):
            i_re = img[Q_PAD * c + row0:Q_PAD * c + row0 + rows, 0:P_ALL]
            i_im = img[Q_PAD * c + row0:Q_PAD * c + row0 + rows, P_ALL:P_TWO]
            s_re, s_im = st[0, c, row0:row0 + rows], st[1, c, row0:row0 + rows]
            x_re = x_re + s_re * i_re + s_im * i_im
            x_im = x_im + s_re * i_im - s_im * i_re
        lo = jnp.concatenate([x_re[:, 0:P_PAD], x_im[:, 0:P_PAD]], axis=1)
        hi = jnp.concatenate([x_re[:, P_BLK:P_BLK + P_PAD], x_im[:, P_BLK:P_BLK + P_PAD]], axis=1)
        psend[row0:row0 + rows] = jnp.where(first_col, hi, lo)
        swap(sub).start()
        mine[row0:row0 + rows] = jnp.where(first_col, lo, hi)

    for j, sub in SENT:
        for i in range(3):
            copy_of(j, sub, i, r).wait_send()
    for sub in range(2):
        swap(sub).wait()
        row0, rows = SUBS[sub]
        rows = min(rows, Q_BLK - row0)
        s = slice(row0, row0 + rows)
        total = mine[s] + precv[s]
        for i in range(2):
            out_ref[i, :, s] = (total[:, P_PAD * i:P_PAD * i + P_BLK] * dd[s]).T


def solution(mesh):
    sample_spec = ('exam', 'rows', 'cols')
    vmem = pl.BlockSpec(memory_space=pltpu.VMEM)
    hbm = pl.BlockSpec(memory_space=pltpu.HBM)
    sds = jax.ShapeDtypeStruct

    def local_fn(kspace, wts_y, wts_x, idx_y, idx_x, coil_maps, deapod):
        n = kspace.shape[2]
        e1, e2 = dft_constants()
        maps = jnp.transpose(coil_maps, (0, 3, 1, 2))
        acc_shape = [sds((N_SRC * VS, LANES), F32)] * (N_ACC)
        inputs = (kspace, wts_y, wts_x, idx_y.reshape(16, LANES), idx_x.reshape(16, LANES), e2)
        *samples, = pl.pallas_call(
            exchange_kernel,
            out_shape=[sds((2, 8, n), F32), sds((2, 4, n), F32), sds((2, 4, n), F32), sds((2, 16, LANES), jnp.int32),
                       sds((N_CHUNK, WIDE, P_TWO), BF16), sds((n, LANES), F32)] + acc_shape,
            in_specs=[hbm] * 6,
            out_specs=[vmem] * (6 + N_ACC),
            scratch_shapes=[pltpu.VMEM((KV, P_TWO), BF16), pltpu.VMEM((2, 8, n), F32), pltpu.VMEM((16, LANES), jnp.int32), pltpu.VMEM((16, LANES), jnp.int32),
                            pltpu.VMEM((1, 16, LANES), jnp.int32),
                            pltpu.VMEM((8, n), F32), pltpu.SemaphoreType.DMA((6,)), pltpu.SemaphoreType.DMA((4,)),
                            pltpu.SemaphoreType.DMA((4,))],
            compiler_params=pltpu.CompilerParams(collective_id=0, has_side_effects=True, vmem_limit_bytes=8 * MIB),
            name='exchange',
        )(*[pltpu.with_memory_space_constraint(x, pltpu.HBM) for x in inputs])
        y8, wy, wx, place, e2f, q_own = samples[:6]
        accs = pl.pallas_call(
            spread_kernel,
            out_shape=acc_shape,
            in_specs=[vmem] * (5 + N_ACC),
            out_specs=[vmem] * (N_ACC),
            scratch_shapes=[pltpu.SMEM((2, 16, LANES), jnp.int32), pltpu.VMEM((2, 16, LANES), jnp.int32), pltpu.VMEM((2, 16, LANES), jnp.int32),
                            pltpu.SemaphoreType.DMA] + [pltpu.VMEM((WIDE, LANES), F32)] * 2,
            input_output_aliases={5 + i: i for i in range(N_ACC)},
            compiler_params=pltpu.CompilerParams(vmem_limit_bytes=8 * MIB),
            cost_estimate=pl.CostEstimate(flops=2 * 10**9, bytes_accessed=2 * 10**7, transcendentals=0),
            name='spread',
        )(place, y8, wy, wx, q_own, *samples[6:])
        return pl.pallas_call(
            transform_kernel,
            out_shape=sds((2, P_BLK, Q_BLK), F32),
            in_specs=[vmem] * (N_ACC + 4),
            out_specs=vmem,
            scratch_shapes=[pltpu.VMEM((2, 4, Q_PAD, P_ALL), F32), pltpu.VMEM((Q_BLK, P_BLK), F32), pltpu.VMEM((KV, WIDE), BF16)] + [pltpu.VMEM((KV, LANES), F32)] * 3 + [
                pltpu.VMEM((Q_PAD, LANES), F32),
                pltpu.VMEM((GN_ROWS, LANES), F32),
                pltpu.VMEM((LAST, 4, Q_PAD, WIDE), BF16),
                pltpu.VMEM((LAST, 4, Q_PAD, WIDE), BF16),
                pltpu.VMEM((4, 144, LANES), BF16),
                pltpu.VMEM((4, 144, LANES), BF16),
                pltpu.VMEM((Q_PAD, LANES), F32),
                pltpu.VMEM((GN_ROWS, LANES), F32),
                pltpu.VMEM((4 * Q_PAD, P_TWO), F32),
                pltpu.VMEM((Q_PAD, P_ALL), F32),
                pltpu.VMEM((Q_PAD, P_ALL), F32),
                pltpu.VMEM((Q_PAD, P_ALL), F32),
                pltpu.SemaphoreType.DMA((N_CHUNK, len(SUBS), 3)),
                pltpu.SemaphoreType.DMA((N_CHUNK, len(SUBS), 4)),
                pltpu.SemaphoreType.DMA((2,)),
                pltpu.SemaphoreType.DMA((2,)),
                pltpu.SemaphoreType.DMA((len(SUBS),)),
                pltpu.SemaphoreType.DMA((len(SUBS),)),
            ],
            compiler_params=pltpu.CompilerParams(collective_id=1, has_side_effects=True, vmem_limit_bytes=24 * MIB),
            name='transform',
        )(*accs, e1, e2f, maps, deapod)

    return jax.shard_map(
        local_fn,
        mesh=mesh,
        in_specs=(P(None, None, sample_spec), P(None, sample_spec), P(None, sample_spec), P(sample_spec), P(sample_spec), P(None, ('exam', 'cols'), None, 'rows'), P()),
        out_specs=P(None, ('exam', 'cols'), 'rows'),
        check_vma=False,
    )
```

```python
import math

import jax
import jax.numpy as jnp
import numpy as np
from jax import lax
from jax.experimental import pallas as pl
from jax.experimental.pallas import tpu as pltpu
from jax.sharding import PartitionSpec as P

F32, BF16 = jnp.float32, jnp.bfloat16
MESH = pl.DeviceIdType.MESH

N_IMG = 368
N_GRID = 736
ROW_BLK = 184
Q_BLK, Q_PAD = 92, 96
P_BLK, P_PAD, P_ALL = 184, 192, 384
N_CH = 8
TILE_U, STRIDE_U, N_SRC = 16, 13, 15
N_TGT = 12
COL_BLK = 368
VR = 384
VS = 392
KV = 2 * VR
LANES, ROWS = 128, 16
EDGE = 6
WIDE, P_TWO, GN_ROWS, MIB = 2 * LANES, 2 * P_ALL, 48, 2**20
N_CHUNK = 6
N_COPY = 3
N_ACC = 2 * N_COPY
SUBS = [(0, 64), (64, 32), (0, Q_PAD)]
FULL, N_WHOLE = 2, 2
WHOLE, SPLIT = range(N_WHOLE), range(N_WHOLE, N_CHUNK)
POSTS = [[(j, FULL)] for j in WHOLE] + [[(j, 0)] for j in SPLIT]
POSTS += [[(j, 1) for j in SPLIT]]
LAST = N_CHUNK - 1
SUBS_LAST = [(0, 96), (96, 48)]
SENT = [(j, FULL) for j in WHOLE] + [(j, sub) for j in SPLIT for sub in range(2)]
CHUNK_TILES = [(1 + 2 * j, 2 + 2 * j) for j in range(5)] + [(0, 11)]


def dft_constants():
    scale = 1.0 / math.sqrt(N_GRID)
    phase = ((np.arange(N_GRID)[:, None] - N_GRID // 2) * (np.arange(N_IMG)[None, :] - N_IMG // 2)) % N_GRID
    ang = phase.astype(np.float64) * (2.0 * math.pi / N_GRID)
    parts = (np.cos(ang) * scale, np.sin(ang) * scale)
    e1 = np.zeros((4, 2, Q_PAD, 2, VR))
    for dest in range(4):
        for cs in range(2):
            for half in range(2):
                part = parts[cs][half * COL_BLK:(half + 1) * COL_BLK, dest * Q_BLK:(dest + 1) * Q_BLK]
                e1[dest, cs, :Q_BLK, half, EDGE:EDGE + COL_BLK] = part.T
    e2 = np.zeros((N_CHUNK, 4, 2, TILE_U, 2, P_ALL))
    for j in range(N_CHUNK):
        for src in range(4):
            for tl in range(2):
                base = TILE_U * CHUNK_TILES[j][tl]
                rows = min(TILE_U, ROW_BLK - base)
                u0 = src * ROW_BLK + base
                for cs in range(2):
                    e2[j, src, tl, :rows, cs, :N_IMG] = parts[cs][u0:u0 + rows]
    return (jnp.asarray(e1.reshape(8 * Q_PAD, KV).astype(np.float32)).astype(BF16),
            jnp.asarray(e2.reshape(N_CHUNK * LANES, P_TWO).astype(np.float32)).astype(BF16))


def j_is_last(j):
    return isinstance(j, int) and j == LAST


def exchange_kernel(y_hbm, wy_hbm, wx_hbm, iy_hbm, ix_hbm, e2_hbm, y_ref, wy_ref, wx_ref, place_ref, e2f, q_own, *refs):
    accs = refs[:N_ACC]
    e2_ref, y_in, iy, ix, roff, y_send, in_sem, send_sem, recv_sem = refs[N_ACC:]
    k = lax.axis_index('cols')
    r = lax.axis_index('rows')
    other = {'cols': 1 - k}
    barrier = pltpu.get_barrier_semaphore()
    pl.semaphore_signal(barrier, inc=1, device_id=other, device_id_type=MESH)
    loads = [(iy_hbm, iy), (ix_hbm, ix), (y_hbm, y_in), (wy_hbm, wy_ref.at[0]), (wx_hbm, wx_ref.at[0]), (e2_hbm, e2_ref)]
    loads = [pltpu.make_async_copy(a, b, in_sem.at[i]) for i, (a, b) in enumerate(loads)]
    for i in (3, 4, 0, 1, 2):
        loads[i].start()

    def send(i, src, dst):
        c = pltpu.make_async_remote_copy(src_ref=src, dst_ref=dst, send_sem=send_sem.at[i], recv_sem=recv_sem.at[i],
                                         device_id=other, device_id_type=MESH)
        c.start()
        return c

    loads[3].wait()
    loads[4].wait()
    pl.semaphore_wait(barrier, 1)
    copies = [send(0, wy_ref.at[0], wy_ref.at[1]), send(1, wx_ref.at[0], wx_ref.at[1])]
    loads[0].wait()
    loads[1].wait()
    row = iy[...] - r * ROW_BLK
    tile = jnp.zeros_like(row)
    for t in range(1, N_SRC):
        tile = tile + jnp.where(row >= STRIDE_U * t, 1, 0)
    roff[0] = (row + 14) & 15
    place_ref[0] = (tile * VS + (ix[...] - k * COL_BLK)) * ROWS + roff[0]
    loads[2].wait()
    y_re, y_im = y_in[0], y_in[1]
    low = jnp.concatenate([y_re[0:4], y_im[0:4]], axis=0)
    high = jnp.concatenate([y_re[4:8], y_im[4:8]], axis=0)
    y_ref[0] = jnp.where(k == 0, low, high)
    y_send[...] = jnp.where(k == 0, high, low)
    copies += [send(2, place_ref.at[0], place_ref.at[1]), send(3, y_send, y_ref.at[1])]
    loads[-1].start()

    def zero(i, _):
        for a in accs:
            a[pl.ds(pl.multiple_of(i * VS, 8), VS), :] = jnp.zeros((VS, LANES), F32)
        return 0
    lax.fori_loop(0, N_SRC, zero, 0)
    expand = expansion()

    def own_rows(i, _):
        q_own[pl.ds(pl.multiple_of(i * WIDE, WIDE), WIDE), :] = sample_rows(expand, i, 0, y_ref, wy_ref, roff)
        return 0
    lax.fori_loop(0, y_ref.shape[2] // WIDE, own_rows, 0)
    loads[-1].wait()
    for j in range(N_CHUNK):
        for h in range(2):
            v = e2_ref[LANES * j + 64 * h:LANES * j + 64 * h + 64, :]
            e2f[j, LANES * h:LANES * h + 64, :] = v
            e2f[j, LANES * h + 64:LANES * h + LANES, 0:P_ALL] = -v[:, P_ALL:P_TWO]
            e2f[j, LANES * h + 64:LANES * h + LANES, P_ALL:P_TWO] = v[:, 0:P_ALL]
    for c in copies:
        c.wait()


def split3(x):
    hi = x.astype(BF16).astype(F32)
    rest = x - hi
    mid = rest.astype(BF16).astype(F32)
    return [hi, mid, rest - mid]


def expansion():
    r0 = lax.broadcasted_iota(jnp.int32, (80, WIDE), 0)
    l0 = lax.broadcasted_iota(jnp.int32, (80, WIDE), 1)
    ry = (r0 < 24) & (l0 < LANES) & ((r0 & 7) == (l0 >> 4))
    rw = (r0 >= 24) & (r0 < 72) & (l0 >= LANES) & (((r0 - 24) & 15) == (l0 & 15))
    return jnp.where(ry | rw, 1.0, 0.0).astype(BF16)


def sample_rows(expand, i, slot, y_ref, wy_ref, roff):
    n_blk = y_ref.shape[2] // WIDE
    rr = lax.broadcasted_iota(jnp.int32, (ROWS, WIDE), 0)
    ds = [pl.ds(pl.multiple_of((i + n_blk * h) * LANES, LANES), LANES) for h in range(2)]
    y = jnp.concatenate([y_ref[slot, :, s] for s in ds], axis=1)
    wy = jnp.concatenate([wy_ref[slot, :, s] for s in ds], axis=1)
    d = (rr - jnp.concatenate([roff[slot, pl.ds(i + n_blk * h, 1), :] for h in range(2)], axis=1)) & 15
    w16 = jnp.zeros((ROWS, WIDE), F32)
    for a in range(4):
        w16 = jnp.where(d == a, wy[a:a + 1], w16)
    lhs = jnp.concatenate(split3(y) + split3(w16) + [jnp.zeros((8, WIDE), F32)], axis=0).astype(BF16)
    o = lax.dot_general(lhs, expand, (((0,), (0,)), ((), ())), preferred_element_type=F32)
    return o[:, :LANES] * o[:, LANES:]


def spread_kernel(place_ref, y_ref, wy_ref, wx_ref, q_own, *refs):
    accs = refs[N_ACC:4 * N_COPY]
    addr, addr_v, roff, sem, *q_refs = refs[4 * N_COPY:]
    place = place_ref[...]
    addr_v[...] = place >> 4
    roff[...] = place & 15
    to_smem = pltpu.make_async_copy(addr_v, addr, sem)
    to_smem.start()
    n = y_ref.shape[2]

    n_blk = n // WIDE

    expand = expansion()

    def prep(i, slot, q_ref):
        q_ref[...] = sample_rows(expand, i, slot, y_ref, wy_ref, roff)

    top = lax.broadcasted_iota(jnp.int32, (8, LANES), 0) < 4

    def scatter(i, q_nbr):
        first = pl.multiple_of(i * WIDE, WIDE)
        ds = [pl.ds(pl.multiple_of((i + n_blk * h) * LANES, LANES), LANES) for h in range(2)]
        wx = [jnp.concatenate([wx_ref[slot, :, s] for s in ds], axis=0) for slot in range(2)]
        for j in range(LANES):
            cols = [jnp.broadcast_to(wx[slot][:, j:j + 1], (8, LANES)) for slot in range(2)]
            for h in range(2):
                for slot in range(2):
                    acc = accs[slot * N_COPY + (2 * j + h) % N_COPY]
                    base = addr[slot, i + n_blk * h, j] + (0 if h else 4)
                    at = j + LANES * h
                    q = jnp.broadcast_to(q_nbr[at:at + 1, :] if slot else q_own[pl.ds(first + at, 1), :], (8, LANES))
                    if h:
                        s = pl.ds(base, 8)
                        acc[s, :] = acc[s, :] + jnp.where(top, 0.0, cols[slot]) * q
                    else:
                        s = pl.ds(base, 4)
                        acc[s, :] = acc[s, :] + cols[slot][0:4] * q[0:4]

    qa, qb = q_refs
    prep(0, 1, qa)
    to_smem.wait()

    def two_blocks(i, _):
        for step, now, then in ((0, qa, qb), (1, qb, qa)):
            prep(lax.rem(2 * i + step + 1, n_blk), 1, then)
            scatter(2 * i + step, now)
        return 0
    lax.fori_loop(0, n_blk // 2, two_blocks, 0)


def transform_kernel(*refs):
    own, nbr = refs[:N_COPY], refs[N_COPY:N_ACC]
    (e1_ref, e2f, s_ref, d_ref, out_ref, st, dd, gch, raw0, f0, f11, gps, gns, msg, recv, msg_last, recv_last, gpr, gnr, img, mine, psend, precv,
     msend_sem, mrecv_sem, gsend_sem, grecv_sem, psend_sem, precv_sem) = refs[N_ACC:]
    k = lax.axis_index('cols')
    r = lax.axis_index('rows')
    chip, core = r // 2, r % 2
    dests = [2 * (1 - chip) + core, 2 * (1 - chip) + (1 - core), 2 * chip + (1 - core)]
    nxt, prv = lax.rem(r + 1, 4), lax.rem(r + 3, 4)
    barrier = pltpu.get_barrier_semaphore()
    for d in dests:
        pl.semaphore_signal(barrier, inc=1, device_id={'rows': d}, device_id_type=MESH)
    pl.semaphore_signal(barrier, inc=1, device_id={'cols': 1 - k}, device_id_type=MESH)

    slots = ((own, k), (nbr, 1 - k))
    lane16 = lax.broadcasted_iota(jnp.int32, (ROWS, LANES), 1) & 15
    sub16 = lax.broadcasted_iota(jnp.int32, (ROWS, LANES), 0)

    def merged(accs, off, targets):
        wanted = {}
        for m in targets:
            deltas = {0: 0} if m is None else {t: STRIDE_U * t - TILE_U * m - 2 for t in range(N_SRC)}
            wanted[m] = {t: d for t, d in deltas.items() if abs(d) < ROWS}
        loaded = {}
        for t in sorted({t for w in wanted.values() for t in w}):
            s = pl.ds(t * VS + off, ROWS)
            v = accs[0][s, :]
            for acc in accs[1:]:
                v = v + acc[s, :]
            loaded[t] = v
        outs = []
        for m in targets:
            out = None
            for t, d in wanted[m].items():
                lo, hi = max(0, d), min(15, 15 + d)
                v = loaded[t]
                if lo > 0 or hi < 15:
                    v = jnp.where((lane16 >= lo) & (lane16 <= hi), v, 0.0)
                out = v if out is None else out + v
            outs.append(out)
        return outs

    def merge_all(targets, put):
        def rows(i, _):
            for step in range(2):
                for accs, half in slots:
                    off = pl.multiple_of((2 * i + 1 + step) * ROWS, ROWS)
                    put(pl.multiple_of(half * VR + off, ROWS), merged(accs, off, targets))
            return 0
        lax.fori_loop(0, VR // (2 * ROWS) - 1, rows, 0)
        last = VR - ROWS
        a = [merged(accs, 0, targets) for accs, _ in slots]
        b = [merged(accs, last, targets) for accs, _ in slots]
        for i, (_, half) in enumerate(slots):
            fix_a = [x + jnp.where(sub16 == 6, y, 0.0) for x, y in zip(a[i], b[1 - i])]
            fix_b = [y + jnp.where((sub16 == 4) | (sub16 == 5), x, 0.0) for x, y in zip(a[1 - i], b[i])]
            put(pl.multiple_of(half * VR, ROWS), fix_a)
            put(pl.multiple_of(half * VR + last, ROWS), fix_b)

    def put_chunk(off, vals):
        for i, v in enumerate(vals):
            gch[pl.ds(off, ROWS), LANES * i:LANES * (i + 1)] = v.astype(BF16)

    def put_edges(off, vals):
        for ref, v in zip((raw0, f0, f11), vals):
            ref[pl.ds(off, ROWS), :] = v

    lane = lax.broadcasted_iota(jnp.int32, (Q_PAD, WIDE), 1) & 127

    def swap(sub):
        rows = pl.ds(*SUBS[sub])
        return pltpu.make_async_remote_copy(src_ref=psend.at[rows], dst_ref=precv.at[rows], send_sem=psend_sem.at[sub],
                                            recv_sem=precv_sem.at[sub], device_id={'cols': 1 - k}, device_id_type=MESH)

    def first_dft(j, g):
        ab = jnp.dot(e1_ref[...], g, preferred_element_type=F32)
        for d in range(4):
            a = ab[192 * d:192 * d + Q_PAD]
            b = ab[192 * d + Q_PAD:192 * d + 192]
            b = jnp.concatenate([pltpu.roll(b[:, :128], 64, 1), pltpu.roll(b[:, 128:], 64, 1)], axis=1)
            h = jnp.where(lane < 64, a - b, a + b).astype(BF16)
            if not j_is_last(j):
                msg[j, d] = h
                continue
            for sub, (at, _) in enumerate(SUBS_LAST):
                row0, rows = SUBS[sub]
                half = rows // 2
                upper = h[row0:row0 + half, LANES:WIDE]
                lower = pltpu.roll(h[row0 + half:row0 + rows, LANES:WIDE], 8, 1)
                msg_last[d, at:at + rows] = h[row0:row0 + rows, 0:LANES]
                msg_last[d, at + rows:at + rows + half] = jnp.where((lane[0:half, 0:LANES] & 8) == 0, upper, lower)

    def copy_of(j, sub, i, slot):
        d = dests[i]
        if j_is_last(j):
            rows = pl.ds(*SUBS_LAST[sub])
            src, dst = msg_last.at[d, rows], recv_last.at[slot, rows]
        else:
            rows = pl.ds(*SUBS[sub])
            src, dst = msg.at[j, d, rows], recv.at[j, slot, rows]
        return pltpu.make_async_remote_copy(src_ref=src, dst_ref=dst, send_sem=msend_sem.at[j, sub, i],
                                            recv_sem=mrecv_sem.at[j, sub, slot], device_id={'rows': d}, device_id_type=MESH)

    def post(chunk):
        for j, sub in POSTS[chunk]:
            for i in range(3):
                copy_of(j, sub, i, r).start()
        if chunk < LAST:
            recv[chunk, r] = msg[chunk, r]
        elif chunk == LAST:
            recv_last[r] = msg_last[r]

    merge_all(CHUNK_TILES[0], put_chunk)
    first_dft(0, gch[...])
    pl.semaphore_wait(barrier, 4)
    post(0)

    merge_all((None, 0, N_TGT - 1), put_edges)
    la = lax.broadcasted_iota(jnp.int32, (Q_PAD, LANES), 1) & 15
    lb = lax.broadcasted_iota(jnp.int32, (GN_ROWS, LANES), 1) & 15

    def shifted(v, by):
        return pltpu.roll(v, by % LANES, 1) if by else v

    gp = jnp.zeros((Q_PAD, LANES), F32)
    for c in range(8):
        gp = jnp.where((la >> 1) == c, shifted(raw0[Q_PAD * c:Q_PAD * c + Q_PAD, :], 2 * c - 14), gp)
    gps[...] = gp
    gn = jnp.zeros((GN_ROWS, LANES), F32)
    for c in range(16):
        gn = jnp.where(lb == c, shifted(f11[GN_ROWS * c:GN_ROWS * c + GN_ROWS, :], c - 8), gn)
    gns[...] = gn
    to_prv = pltpu.make_async_remote_copy(src_ref=gps, dst_ref=gpr, send_sem=gsend_sem.at[0], recv_sem=grecv_sem.at[0],
                                          device_id={'rows': prv}, device_id_type=MESH)
    to_nxt = pltpu.make_async_remote_copy(src_ref=gns, dst_ref=gnr, send_sem=gsend_sem.at[1], recv_sem=grecv_sem.at[1],
                                          device_id={'rows': nxt}, device_id_type=MESH)
    to_prv.start()
    to_nxt.start()

    for j in range(1, N_CHUNK - 1):
        merge_all(CHUNK_TILES[j], put_chunk)
        first_dft(j, gch[...])
        post(j)

    to_prv.wait()
    to_nxt.wait()
    gp, gn = gpr[...], gnr[...]
    for c in range(8):
        s = slice(Q_PAD * c, Q_PAD * c + Q_PAD)
        gch[s, LANES:WIDE] = (f11[s, :] + jnp.where((la >> 1) == 3, shifted(gp, 6 - 2 * c), 0.0)).astype(BF16)
    for c in range(16):
        s = slice(GN_ROWS * c, GN_ROWS * c + GN_ROWS)
        gch[s, 0:LANES] = (f0[s, :] + jnp.where(lb == 0, shifted(gn, -c), 0.0)).astype(BF16)
    first_dft(LAST, gch[...])
    post(LAST)

    d_all = d_ref[...].reshape(1, N_IMG)
    st[...] = jnp.zeros_like(st)
    for s in range(2):
        for c in range(4):
            st[s, c, 0:Q_BLK, 0:N_IMG] = s_ref[s, :, c, :]

    half_p = jnp.where(k == 0, d_all[:, 0:P_BLK], d_all[:, P_BLK:2 * P_BLK])
    part_q = d_all[:, 0:Q_BLK]
    for i in range(1, 4):
        part_q = jnp.where(r == i, d_all[:, Q_BLK * i:Q_BLK * (i + 1)], part_q)
    part_q = jnp.concatenate([part_q, jnp.zeros((1, LANES - Q_BLK), F32)], axis=1)
    dd[...] = jnp.broadcast_to(part_q, (8, LANES)).T[0:Q_BLK, 0:1] * half_p

    first_col = k == 0

    def second_dft(j, sub):
        row0, rows = SUBS[sub]
        for i in range(3):
            copy_of(j, sub, i, dests[i]).wait_recv()
        coil = (lax.broadcasted_iota(jnp.int32, (rows, LANES), 1) >> 4) & 3
        halves = []
        for pair in range(2):
            v = []
            for src in (2 * pair, 2 * pair + 1):
                if j_is_last(j):
                    at = SUBS_LAST[sub][0]
                    folded = recv_last[src, at + rows:at + rows + rows // 2]
                    v += [recv_last[src, at:at + rows], jnp.concatenate([folded, pltpu.roll(folded, LANES - 8, 1)], axis=0)]
                else:
                    v += [recv[j, src, pl.ds(row0, rows), LANES * t:LANES * (t + 1)] for t in range(2)]
            for bit in (1, 2):
                m = (coil & bit) == 0
                for t in range(4):
                    if t & bit:
                        continue
                    x, y = v[t], v[t | bit]
                    v[t] = jnp.where(m, x, pltpu.roll(y, ROWS * bit, 1))
                    v[t | bit] = jnp.where(m, pltpu.roll(x, LANES - ROWS * bit, 1), y)
            halves.append(v)
        lhs = jnp.concatenate([jnp.concatenate([halves[0][c], halves[1][c]], axis=1) for c in range(4)], axis=0)
        return jnp.dot(lhs, e2f[j], preferred_element_type=F32)

    img[...] = second_dft(0, FULL)
    for j in WHOLE[1:]:
        img[...] += second_dft(j, FULL)
    for sub in range(2):
        row0, rows = SUBS[sub]

        def accumulate(j, _):
            part = second_dft(j, sub)
            for c in range(4):
                img[Q_PAD * c + row0:Q_PAD * c + row0 + rows] += part[rows * c:rows * (c + 1)]
            return 0
        lax.fori_loop(N_WHOLE, N_WHOLE + 1, accumulate, 0)
        if sub == 0:
            post(N_CHUNK)
        lax.fori_loop(N_WHOLE + 1, LAST, accumulate, 0)
        accumulate(LAST, 0)

        x_re = jnp.zeros((rows, P_ALL), F32)
        x_im = jnp.zeros((rows, P_ALL), F32)
        for c in range(4):
            i_re = img[Q_PAD * c + row0:Q_PAD * c + row0 + rows, 0:P_ALL]
            i_im = img[Q_PAD * c + row0:Q_PAD * c + row0 + rows, P_ALL:P_TWO]
            s_re, s_im = st[0, c, row0:row0 + rows], st[1, c, row0:row0 + rows]
            x_re = x_re + s_re * i_re + s_im * i_im
            x_im = x_im + s_re * i_im - s_im * i_re
        lo = jnp.concatenate([x_re[:, 0:P_PAD], x_im[:, 0:P_PAD]], axis=1)
        hi = jnp.concatenate([x_re[:, P_BLK:P_BLK + P_PAD], x_im[:, P_BLK:P_BLK + P_PAD]], axis=1)
        psend[row0:row0 + rows] = jnp.where(first_col, hi, lo)
        swap(sub).start()
        mine[row0:row0 + rows] = jnp.where(first_col, lo, hi)

    for j, sub in SENT:
        for i in range(3):
            copy_of(j, sub, i, r).wait_send()
    for sub in range(2):
        swap(sub).wait()
        row0, rows = SUBS[sub]
        rows = min(rows, Q_BLK - row0)
        s = slice(row0, row0 + rows)
        total = mine[s] + precv[s]
        for i in range(2):
            out_ref[i, :, s] = (total[:, P_PAD * i:P_PAD * i + P_BLK] * dd[s]).T


def solution(mesh):
    sample_spec = ('exam', 'rows', 'cols')
    vmem = pl.BlockSpec(memory_space=pltpu.VMEM)
    hbm = pl.BlockSpec(memory_space=pltpu.HBM)
    sds = jax.ShapeDtypeStruct

    def local_fn(kspace, wts_y, wts_x, idx_y, idx_x, coil_maps, deapod):
        n = kspace.shape[2]
        e1, e2 = dft_constants()
        maps = jnp.transpose(coil_maps, (0, 3, 1, 2))
        acc_shape = [sds((N_SRC * VS, LANES), F32)] * (N_ACC)
        inputs = (kspace, wts_y, wts_x, idx_y.reshape(16, LANES), idx_x.reshape(16, LANES), e2)
        *samples, = pl.pallas_call(
            exchange_kernel,
            out_shape=[sds((2, 8, n), F32), sds((2, 4, n), F32), sds((2, 4, n), F32), sds((2, 16, LANES), jnp.int32),
                       sds((N_CHUNK, WIDE, P_TWO), BF16), sds((n, LANES), F32)] + acc_shape,
            in_specs=[hbm] * 6,
            out_specs=[vmem] * (6 + N_ACC),
            scratch_shapes=[pltpu.VMEM((KV, P_TWO), BF16), pltpu.VMEM((2, 8, n), F32), pltpu.VMEM((16, LANES), jnp.int32), pltpu.VMEM((16, LANES), jnp.int32),
                            pltpu.VMEM((1, 16, LANES), jnp.int32),
                            pltpu.VMEM((8, n), F32), pltpu.SemaphoreType.DMA((6,)), pltpu.SemaphoreType.DMA((4,)),
                            pltpu.SemaphoreType.DMA((4,))],
            compiler_params=pltpu.CompilerParams(collective_id=0, has_side_effects=True, vmem_limit_bytes=8 * MIB),
            name='exchange',
        )(*[pltpu.with_memory_space_constraint(x, pltpu.HBM) for x in inputs])
        y8, wy, wx, place, e2f, q_own = samples[:6]
        accs = pl.pallas_call(
            spread_kernel,
            out_shape=acc_shape,
            in_specs=[vmem] * (5 + N_ACC),
            out_specs=[vmem] * (N_ACC),
            scratch_shapes=[pltpu.SMEM((2, 16, LANES), jnp.int32), pltpu.VMEM((2, 16, LANES), jnp.int32), pltpu.VMEM((2, 16, LANES), jnp.int32),
                            pltpu.SemaphoreType.DMA] + [pltpu.VMEM((WIDE, LANES), F32)] * 2,
            input_output_aliases={5 + i: i for i in range(N_ACC)},
            compiler_params=pltpu.CompilerParams(vmem_limit_bytes=8 * MIB),
            cost_estimate=pl.CostEstimate(flops=2 * 10**9, bytes_accessed=2 * 10**7, transcendentals=0),
            name='spread',
        )(place, y8, wy, wx, q_own, *samples[6:])
        return pl.pallas_call(
            transform_kernel,
            out_shape=sds((2, P_BLK, Q_BLK), F32),
            in_specs=[vmem] * (N_ACC + 4),
            out_specs=vmem,
            scratch_shapes=[pltpu.VMEM((2, 4, Q_PAD, P_ALL), F32), pltpu.VMEM((Q_BLK, P_BLK), F32), pltpu.VMEM((KV, WIDE), BF16)] + [pltpu.VMEM((KV, LANES), F32)] * 3 + [
                pltpu.VMEM((Q_PAD, LANES), F32),
                pltpu.VMEM((GN_ROWS, LANES), F32),
                pltpu.VMEM((LAST, 4, Q_PAD, WIDE), BF16),
                pltpu.VMEM((LAST, 4, Q_PAD, WIDE), BF16),
                pltpu.VMEM((4, 144, LANES), BF16),
                pltpu.VMEM((4, 144, LANES), BF16),
                pltpu.VMEM((Q_PAD, LANES), F32),
                pltpu.VMEM((GN_ROWS, LANES), F32),
                pltpu.VMEM((4 * Q_PAD, P_TWO), F32),
                pltpu.VMEM((Q_PAD, P_ALL), F32),
                pltpu.VMEM((Q_PAD, P_ALL), F32),
                pltpu.VMEM((Q_PAD, P_ALL), F32),
                pltpu.SemaphoreType.DMA((N_CHUNK, len(SUBS), 3)),
                pltpu.SemaphoreType.DMA((N_CHUNK, len(SUBS), 4)),
                pltpu.SemaphoreType.DMA((2,)),
                pltpu.SemaphoreType.DMA((2,)),
                pltpu.SemaphoreType.DMA((len(SUBS),)),
                pltpu.SemaphoreType.DMA((len(SUBS),)),
            ],
            compiler_params=pltpu.CompilerParams(collective_id=1, has_side_effects=True, vmem_limit_bytes=24 * MIB),
            name='transform',
        )(*accs, e1, e2f, maps, deapod)

    return jax.shard_map(
        local_fn,
        mesh=mesh,
        in_specs=(P(None, None, sample_spec), P(None, sample_spec), P(None, sample_spec), P(sample_spec), P(sample_spec), P(None, ('exam', 'cols'), None, 'rows'), P()),
        out_specs=P(None, ('exam', 'cols'), 'rows'),
        check_vma=False,
    )
```

```python
import math

import jax
import jax.numpy as jnp
import numpy as np
from jax import lax
from jax.experimental import pallas as pl
from jax.experimental.pallas import tpu as pltpu
from jax.sharding import PartitionSpec as P

F32, BF16 = jnp.float32, jnp.bfloat16
MESH = pl.DeviceIdType.MESH

N_IMG = 368
N_GRID = 736
ROW_BLK = 184
Q_BLK, Q_PAD = 92, 96
P_BLK, P_PAD, P_ALL = 184, 192, 384
N_CH = 8
TILE_U, STRIDE_U, N_SRC = 16, 13, 15
N_TGT = 12
COL_BLK = 368
VR = 384
VS = 392
KV = 2 * VR
LANES, ROWS = 128, 16
EDGE = 6
WIDE, P_TWO, GN_ROWS, MIB = 2 * LANES, 2 * P_ALL, 48, 2**20
N_CHUNK = 6
N_COPY = 3
N_ACC = 2 * N_COPY
SUBS = [(0, 64), (64, 32), (0, Q_PAD)]
FULL, N_WHOLE = 2, 2
WHOLE, SPLIT = range(N_WHOLE), range(N_WHOLE, N_CHUNK)
POSTS = [[(j, FULL)] for j in WHOLE] + [[(j, 0)] for j in SPLIT]
POSTS += [[(j, 1) for j in SPLIT]]
LAST = N_CHUNK - 1
SUBS_LAST = [(0, 96), (96, 48)]
SENT = [(j, FULL) for j in WHOLE] + [(j, sub) for j in SPLIT for sub in range(2)]
CHUNK_TILES = [(1 + 2 * j, 2 + 2 * j) for j in range(5)] + [(0, 11)]


def dft_constants():
    scale = 1.0 / math.sqrt(N_GRID)
    phase = ((np.arange(N_GRID)[:, None] - N_GRID // 2) * (np.arange(N_IMG)[None, :] - N_IMG // 2)) % N_GRID
    ang = phase.astype(np.float64) * (2.0 * math.pi / N_GRID)
    parts = (np.cos(ang) * scale, np.sin(ang) * scale)
    e1 = np.zeros((4, 2, Q_PAD, 2, VR))
    for dest in range(4):
        for cs in range(2):
            for half in range(2):
                part = parts[cs][half * COL_BLK:(half + 1) * COL_BLK, dest * Q_BLK:(dest + 1) * Q_BLK]
                e1[dest, cs, :Q_BLK, half, EDGE:EDGE + COL_BLK] = part.T
    e2 = np.zeros((N_CHUNK, 4, 2, TILE_U, 2, P_ALL))
    for j in range(N_CHUNK):
        for src in range(4):
            for tl in range(2):
                base = TILE_U * CHUNK_TILES[j][tl]
                rows = min(TILE_U, ROW_BLK - base)
                u0 = src * ROW_BLK + base
                for cs in range(2):
                    e2[j, src, tl, :rows, cs, :N_IMG] = parts[cs][u0:u0 + rows]
    return (jnp.asarray(e1.reshape(8 * Q_PAD, KV).astype(np.float32)).astype(BF16),
            jnp.asarray(e2.reshape(N_CHUNK * LANES, P_TWO).astype(np.float32)).astype(BF16))


def j_is_last(j):
    return isinstance(j, int) and j == LAST


def exchange_kernel(y_hbm, wy_hbm, wx_hbm, iy_hbm, ix_hbm, e2_hbm, y_ref, wy_ref, wx_ref, place_ref, e2f, q_own, *refs):
    accs = refs[:N_ACC]
    e2_ref, y_in, iy, ix, roff, y_send, in_sem, send_sem, recv_sem = refs[N_ACC:]
    k = lax.axis_index('cols')
    r = lax.axis_index('rows')
    other = {'cols': 1 - k}
    barrier = pltpu.get_barrier_semaphore()
    pl.semaphore_signal(barrier, inc=1, device_id=other, device_id_type=MESH)
    loads = [(iy_hbm, iy), (ix_hbm, ix), (y_hbm, y_in), (wy_hbm, wy_ref.at[0]), (wx_hbm, wx_ref.at[0]), (e2_hbm, e2_ref)]
    loads = [pltpu.make_async_copy(a, b, in_sem.at[i]) for i, (a, b) in enumerate(loads)]
    for i in (3, 4, 0, 1, 2):
        loads[i].start()

    def send(i, src, dst):
        c = pltpu.make_async_remote_copy(src_ref=src, dst_ref=dst, send_sem=send_sem.at[i], recv_sem=recv_sem.at[i],
                                         device_id=other, device_id_type=MESH)
        c.start()
        return c

    loads[3].wait()
    loads[4].wait()
    pl.semaphore_wait(barrier, 1)
    copies = [send(0, wy_ref.at[0], wy_ref.at[1]), send(1, wx_ref.at[0], wx_ref.at[1])]
    loads[0].wait()
    loads[1].wait()
    row = iy[...] - r * ROW_BLK
    tile = jnp.zeros_like(row)
    for t in range(1, N_SRC):
        tile = tile + jnp.where(row >= STRIDE_U * t, 1, 0)
    roff[0] = (row + 14) & 15
    place_ref[0] = (tile * VS + (ix[...] - k * COL_BLK)) * ROWS + roff[0]
    loads[2].wait()
    y_re, y_im = y_in[0], y_in[1]
    low = jnp.concatenate([y_re[0:4], y_im[0:4]], axis=0)
    high = jnp.concatenate([y_re[4:8], y_im[4:8]], axis=0)
    y_ref[0] = jnp.where(k == 0, low, high)
    y_send[...] = jnp.where(k == 0, high, low)
    copies += [send(2, place_ref.at[0], place_ref.at[1]), send(3, y_send, y_ref.at[1])]
    loads[-1].start()

    def zero(i, _):
        for a in accs:
            a[pl.ds(pl.multiple_of(i * VS, 8), VS), :] = jnp.zeros((VS, LANES), F32)
        return 0
    lax.fori_loop(0, N_SRC, zero, 0)
    expand = expansion()

    def own_rows(i, _):
        q_own[pl.ds(pl.multiple_of(i * WIDE, WIDE), WIDE), :] = sample_rows(expand, i, 0, y_ref, wy_ref, roff)
        return 0
    lax.fori_loop(0, y_ref.shape[2] // WIDE, own_rows, 0)
    loads[-1].wait()
    for j in range(N_CHUNK):
        for h in range(2):
            v = e2_ref[LANES * j + 64 * h:LANES * j + 64 * h + 64, :]
            e2f[j, LANES * h:LANES * h + 64, :] = v
            e2f[j, LANES * h + 64:LANES * h + LANES, 0:P_ALL] = -v[:, P_ALL:P_TWO]
            e2f[j, LANES * h + 64:LANES * h + LANES, P_ALL:P_TWO] = v[:, 0:P_ALL]
    for c in copies:
        c.wait()


def split3(x):
    hi = x.astype(BF16).astype(F32)
    rest = x - hi
    mid = rest.astype(BF16).astype(F32)
    return [hi, mid, rest - mid]


def expansion():
    r0 = lax.broadcasted_iota(jnp.int32, (80, WIDE), 0)
    l0 = lax.broadcasted_iota(jnp.int32, (80, WIDE), 1)
    ry = (r0 < 24) & (l0 < LANES) & ((r0 & 7) == (l0 >> 4))
    rw = (r0 >= 24) & (r0 < 72) & (l0 >= LANES) & (((r0 - 24) & 15) == (l0 & 15))
    return jnp.where(ry | rw, 1.0, 0.0).astype(BF16)


def sample_rows(expand, i, slot, y_ref, wy_ref, roff):
    n_blk = y_ref.shape[2] // WIDE
    rr = lax.broadcasted_iota(jnp.int32, (ROWS, WIDE), 0)
    ds = [pl.ds(pl.multiple_of((i + n_blk * h) * LANES, LANES), LANES) for h in range(2)]
    y = jnp.concatenate([y_ref[slot, :, s] for s in ds], axis=1)
    wy = jnp.concatenate([wy_ref[slot, :, s] for s in ds], axis=1)
    d = (rr - jnp.concatenate([roff[slot, pl.ds(i + n_blk * h, 1), :] for h in range(2)], axis=1)) & 15
    w16 = jnp.zeros((ROWS, WIDE), F32)
    for a in range(4):
        w16 = jnp.where(d == a, wy[a:a + 1], w16)
    lhs = jnp.concatenate(split3(y) + split3(w16) + [jnp.zeros((8, WIDE), F32)], axis=0).astype(BF16)
    o = lax.dot_general(lhs, expand, (((0,), (0,)), ((), ())), preferred_element_type=F32)
    return o[:, :LANES] * o[:, LANES:]


def spread_kernel(place_ref, y_ref, wy_ref, wx_ref, q_own, *refs):
    accs = refs[N_ACC:4 * N_COPY]
    addr, addr_v, roff, sem, *q_refs = refs[4 * N_COPY:]
    place = place_ref[...]
    addr_v[...] = place >> 4
    roff[...] = place & 15
    to_smem = pltpu.make_async_copy(addr_v, addr, sem)
    to_smem.start()
    n = y_ref.shape[2]

    n_blk = n // WIDE

    expand = expansion()

    def prep(i, slot, q_ref):
        q_ref[...] = sample_rows(expand, i, slot, y_ref, wy_ref, roff)

    top = lax.broadcasted_iota(jnp.int32, (8, LANES), 0) < 4

    def scatter(i, q_nbr):
        first = pl.multiple_of(i * WIDE, WIDE)
        ds = [pl.ds(pl.multiple_of((i + n_blk * h) * LANES, LANES), LANES) for h in range(2)]
        wx = [jnp.concatenate([wx_ref[slot, :, s] for s in ds], axis=0) for slot in range(2)]
        for j in range(LANES):
            cols = [jnp.broadcast_to(wx[slot][:, j:j + 1], (8, LANES)) for slot in range(2)]
            for h in range(2):
                for slot in range(2):
                    acc = accs[slot * N_COPY + (2 * j + h) % N_COPY]
                    base = addr[slot, i + n_blk * h, j] + (0 if h else 4)
                    at = j + LANES * h
                    q = jnp.broadcast_to(q_nbr[at:at + 1, :] if slot else q_own[pl.ds(first + at, 1), :], (8, LANES))
                    if h:
                        s = pl.ds(base, 8)
                        acc[s, :] = acc[s, :] + jnp.where(top, 0.0, cols[slot]) * q
                    else:
                        s = pl.ds(base, 4)
                        acc[s, :] = acc[s, :] + cols[slot][0:4] * q[0:4]

    qa, qb = q_refs
    prep(0, 1, qa)
    to_smem.wait()

    def two_blocks(i, _):
        for step, now, then in ((0, qa, qb), (1, qb, qa)):
            prep(lax.rem(2 * i + step + 1, n_blk), 1, then)
            scatter(2 * i + step, now)
        return 0
    lax.fori_loop(0, n_blk // 2, two_blocks, 0)


def transform_kernel(*refs):
    own, nbr = refs[:N_COPY], refs[N_COPY:N_ACC]
    (e1_ref, e2f, s_ref, d_ref, out_ref, st, dd, gch, raw0, f0, f11, gps, gns, msg, recv, msg_last, recv_last, gpr, gnr, img, mine, psend, precv,
     msend_sem, mrecv_sem, gsend_sem, grecv_sem, psend_sem, precv_sem) = refs[N_ACC:]
    k = lax.axis_index('cols')
    r = lax.axis_index('rows')
    chip, core = r // 2, r % 2
    dests = [2 * (1 - chip) + (1 - core), 2 * (1 - chip) + core, 2 * chip + (1 - core)]
    nxt, prv = lax.rem(r + 1, 4), lax.rem(r + 3, 4)
    barrier = pltpu.get_barrier_semaphore()
    for d in dests:
        pl.semaphore_signal(barrier, inc=1, device_id={'rows': d}, device_id_type=MESH)
    pl.semaphore_signal(barrier, inc=1, device_id={'cols': 1 - k}, device_id_type=MESH)

    slots = ((own, k), (nbr, 1 - k))
    lane16 = lax.broadcasted_iota(jnp.int32, (ROWS, LANES), 1) & 15
    sub16 = lax.broadcasted_iota(jnp.int32, (ROWS, LANES), 0)

    def merged(accs, off, targets):
        wanted = {}
        for m in targets:
            deltas = {0: 0} if m is None else {t: STRIDE_U * t - TILE_U * m - 2 for t in range(N_SRC)}
            wanted[m] = {t: d for t, d in deltas.items() if abs(d) < ROWS}
        loaded = {}
        for t in sorted({t for w in wanted.values() for t in w}):
            s = pl.ds(t * VS + off, ROWS)
            v = accs[0][s, :]
            for acc in accs[1:]:
                v = v + acc[s, :]
            loaded[t] = v
        outs = []
        for m in targets:
            out = None
            for t, d in wanted[m].items():
                lo, hi = max(0, d), min(15, 15 + d)
                v = loaded[t]
                if lo > 0 or hi < 15:
                    v = jnp.where((lane16 >= lo) & (lane16 <= hi), v, 0.0)
                out = v if out is None else out + v
            outs.append(out)
        return outs

    def merge_all(targets, put):
        def rows(i, _):
            for step in range(2):
                for accs, half in slots:
                    off = pl.multiple_of((2 * i + 1 + step) * ROWS, ROWS)
                    put(pl.multiple_of(half * VR + off, ROWS), merged(accs, off, targets))
            return 0
        lax.fori_loop(0, VR // (2 * ROWS) - 1, rows, 0)
        last = VR - ROWS
        a = [merged(accs, 0, targets) for accs, _ in slots]
        b = [merged(accs, last, targets) for accs, _ in slots]
        for i, (_, half) in enumerate(slots):
            fix_a = [x + jnp.where(sub16 == 6, y, 0.0) for x, y in zip(a[i], b[1 - i])]
            fix_b = [y + jnp.where((sub16 == 4) | (sub16 == 5), x, 0.0) for x, y in zip(a[1 - i], b[i])]
            put(pl.multiple_of(half * VR, ROWS), fix_a)
            put(pl.multiple_of(half * VR + last, ROWS), fix_b)

    def put_chunk(off, vals):
        for i, v in enumerate(vals):
            gch[pl.ds(off, ROWS), LANES * i:LANES * (i + 1)] = v.astype(BF16)

    def put_edges(off, vals):
        for ref, v in zip((raw0, f0, f11), vals):
            ref[pl.ds(off, ROWS), :] = v

    lane = lax.broadcasted_iota(jnp.int32, (Q_PAD, WIDE), 1) & 127

    def swap(sub):
        rows = pl.ds(*SUBS[sub])
        return pltpu.make_async_remote_copy(src_ref=psend.at[rows], dst_ref=precv.at[rows], send_sem=psend_sem.at[sub],
                                            recv_sem=precv_sem.at[sub], device_id={'cols': 1 - k}, device_id_type=MESH)

    def first_dft(j, g):
        ab = jnp.dot(e1_ref[...], g, preferred_element_type=F32)
        for d in range(4):
            a = ab[192 * d:192 * d + Q_PAD]
            b = ab[192 * d + Q_PAD:192 * d + 192]
            b = jnp.concatenate([pltpu.roll(b[:, :128], 64, 1), pltpu.roll(b[:, 128:], 64, 1)], axis=1)
            h = jnp.where(lane < 64, a - b, a + b).astype(BF16)
            if not j_is_last(j):
                msg[j, d] = h
                continue
            for sub, (at, _) in enumerate(SUBS_LAST):
                row0, rows = SUBS[sub]
                half = rows // 2
                upper = h[row0:row0 + half, LANES:WIDE]
                lower = pltpu.roll(h[row0 + half:row0 + rows, LANES:WIDE], 8, 1)
                msg_last[d, at:at + rows] = h[row0:row0 + rows, 0:LANES]
                msg_last[d, at + rows:at + rows + half] = jnp.where((lane[0:half, 0:LANES] & 8) == 0, upper, lower)

    def copy_of(j, sub, i, slot):
        d = dests[i]
        if j_is_last(j):
            rows = pl.ds(*SUBS_LAST[sub])
            src, dst = msg_last.at[d, rows], recv_last.at[slot, rows]
        else:
            rows = pl.ds(*SUBS[sub])
            src, dst = msg.at[j, d, rows], recv.at[j, slot, rows]
        return pltpu.make_async_remote_copy(src_ref=src, dst_ref=dst, send_sem=msend_sem.at[j, sub, i],
                                            recv_sem=mrecv_sem.at[j, sub, slot], device_id={'rows': d}, device_id_type=MESH)

    def post(chunk):
        for j, sub in POSTS[chunk]:
            for i in range(3):
                copy_of(j, sub, i, r).start()
        if chunk < LAST:
            recv[chunk, r] = msg[chunk, r]
        elif chunk == LAST:
            recv_last[r] = msg_last[r]

    merge_all(CHUNK_TILES[0], put_chunk)
    first_dft(0, gch[...])
    pl.semaphore_wait(barrier, 4)
    post(0)

    merge_all((None, 0, N_TGT - 1), put_edges)
    la = lax.broadcasted_iota(jnp.int32, (Q_PAD, LANES), 1) & 15
    lb = lax.broadcasted_iota(jnp.int32, (GN_ROWS, LANES), 1) & 15

    def shifted(v, by):
        return pltpu.roll(v, by % LANES, 1) if by else v

    gp = jnp.zeros((Q_PAD, LANES), F32)
    for c in range(8):
        gp = jnp.where((la >> 1) == c, shifted(raw0[Q_PAD * c:Q_PAD * c + Q_PAD, :], 2 * c - 14), gp)
    gps[...] = gp
    gn = jnp.zeros((GN_ROWS, LANES), F32)
    for c in range(16):
        gn = jnp.where(lb == c, shifted(f11[GN_ROWS * c:GN_ROWS * c + GN_ROWS, :], c - 8), gn)
    gns[...] = gn
    to_prv = pltpu.make_async_remote_copy(src_ref=gps, dst_ref=gpr, send_sem=gsend_sem.at[0], recv_sem=grecv_sem.at[0],
                                          device_id={'rows': prv}, device_id_type=MESH)
    to_nxt = pltpu.make_async_remote_copy(src_ref=gns, dst_ref=gnr, send_sem=gsend_sem.at[1], recv_sem=grecv_sem.at[1],
                                          device_id={'rows': nxt}, device_id_type=MESH)
    to_prv.start()
    to_nxt.start()

    for j in range(1, N_CHUNK - 1):
        merge_all(CHUNK_TILES[j], put_chunk)
        first_dft(j, gch[...])
        post(j)

    to_prv.wait()
    to_nxt.wait()
    gp, gn = gpr[...], gnr[...]
    for c in range(8):
        s = slice(Q_PAD * c, Q_PAD * c + Q_PAD)
        gch[s, LANES:WIDE] = (f11[s, :] + jnp.where((la >> 1) == 3, shifted(gp, 6 - 2 * c), 0.0)).astype(BF16)
    for c in range(16):
        s = slice(GN_ROWS * c, GN_ROWS * c + GN_ROWS)
        gch[s, 0:LANES] = (f0[s, :] + jnp.where(lb == 0, shifted(gn, -c), 0.0)).astype(BF16)
    first_dft(LAST, gch[...])
    post(LAST)

    d_all = d_ref[...].reshape(1, N_IMG)
    st[...] = jnp.zeros_like(st)
    for s in range(2):
        for c in range(4):
            st[s, c, 0:Q_BLK, 0:N_IMG] = s_ref[s, :, c, :]

    half_p = jnp.where(k == 0, d_all[:, 0:P_BLK], d_all[:, P_BLK:2 * P_BLK])
    part_q = d_all[:, 0:Q_BLK]
    for i in range(1, 4):
        part_q = jnp.where(r == i, d_all[:, Q_BLK * i:Q_BLK * (i + 1)], part_q)
    part_q = jnp.concatenate([part_q, jnp.zeros((1, LANES - Q_BLK), F32)], axis=1)
    dd[...] = jnp.broadcast_to(part_q, (8, LANES)).T[0:Q_BLK, 0:1] * half_p

    first_col = k == 0

    def second_dft(j, sub):
        row0, rows = SUBS[sub]
        for i in range(3):
            copy_of(j, sub, i, dests[i]).wait_recv()
        coil = (lax.broadcasted_iota(jnp.int32, (rows, LANES), 1) >> 4) & 3
        halves = []
        for pair in range(2):
            v = []
            for src in (2 * pair, 2 * pair + 1):
                if j_is_last(j):
                    at = SUBS_LAST[sub][0]
                    folded = recv_last[src, at + rows:at + rows + rows // 2]
                    v += [recv_last[src, at:at + rows], jnp.concatenate([folded, pltpu.roll(folded, LANES - 8, 1)], axis=0)]
                else:
                    v += [recv[j, src, pl.ds(row0, rows), LANES * t:LANES * (t + 1)] for t in range(2)]
            for bit in (1, 2):
                m = (coil & bit) == 0
                for t in range(4):
                    if t & bit:
                        continue
                    x, y = v[t], v[t | bit]
                    v[t] = jnp.where(m, x, pltpu.roll(y, ROWS * bit, 1))
                    v[t | bit] = jnp.where(m, pltpu.roll(x, LANES - ROWS * bit, 1), y)
            halves.append(v)
        lhs = jnp.concatenate([jnp.concatenate([halves[0][c], halves[1][c]], axis=1) for c in range(4)], axis=0)
        return jnp.dot(lhs, e2f[j], preferred_element_type=F32)

    img[...] = second_dft(0, FULL)
    for j in WHOLE[1:]:
        img[...] += second_dft(j, FULL)
    for sub in range(2):
        row0, rows = SUBS[sub]

        def accumulate(j, _):
            part = second_dft(j, sub)
            for c in range(4):
                img[Q_PAD * c + row0:Q_PAD * c + row0 + rows] += part[rows * c:rows * (c + 1)]
            return 0
        lax.fori_loop(N_WHOLE, N_WHOLE + 1, accumulate, 0)
        if sub == 0:
            post(N_CHUNK)
        lax.fori_loop(N_WHOLE + 1, LAST, accumulate, 0)
        accumulate(LAST, 0)

        x_re = jnp.zeros((rows, P_ALL), F32)
        x_im = jnp.zeros((rows, P_ALL), F32)
        for c in range(4):
            i_re = img[Q_PAD * c + row0:Q_PAD * c + row0 + rows, 0:P_ALL]
            i_im = img[Q_PAD * c + row0:Q_PAD * c + row0 + rows, P_ALL:P_TWO]
            s_re, s_im = st[0, c, row0:row0 + rows], st[1, c, row0:row0 + rows]
            x_re = x_re + s_re * i_re + s_im * i_im
            x_im = x_im + s_re * i_im - s_im * i_re
        lo = jnp.concatenate([x_re[:, 0:P_PAD], x_im[:, 0:P_PAD]], axis=1)
        hi = jnp.concatenate([x_re[:, P_BLK:P_BLK + P_PAD], x_im[:, P_BLK:P_BLK + P_PAD]], axis=1)
        psend[row0:row0 + rows] = jnp.where(first_col, hi, lo)
        swap(sub).start()
        mine[row0:row0 + rows] = jnp.where(first_col, lo, hi)

    for j, sub in SENT:
        for i in range(3):
            copy_of(j, sub, i, r).wait_send()
    for sub in range(2):
        swap(sub).wait()
        row0, rows = SUBS[sub]
        rows = min(rows, Q_BLK - row0)
        s = slice(row0, row0 + rows)
        total = mine[s] + precv[s]
        for i in range(2):
            out_ref[i, :, s] = (total[:, P_PAD * i:P_PAD * i + P_BLK] * dd[s]).T


def solution(mesh):
    sample_spec = ('exam', 'rows', 'cols')
    vmem = pl.BlockSpec(memory_space=pltpu.VMEM)
    hbm = pl.BlockSpec(memory_space=pltpu.HBM)
    sds = jax.ShapeDtypeStruct

    def local_fn(kspace, wts_y, wts_x, idx_y, idx_x, coil_maps, deapod):
        n = kspace.shape[2]
        e1, e2 = dft_constants()
        maps = jnp.transpose(coil_maps, (0, 3, 1, 2))
        acc_shape = [sds((N_SRC * VS, LANES), F32)] * (N_ACC)
        inputs = (kspace, wts_y, wts_x, idx_y.reshape(16, LANES), idx_x.reshape(16, LANES), e2)
        *samples, = pl.pallas_call(
            exchange_kernel,
            out_shape=[sds((2, 8, n), F32), sds((2, 4, n), F32), sds((2, 4, n), F32), sds((2, 16, LANES), jnp.int32),
                       sds((N_CHUNK, WIDE, P_TWO), BF16), sds((n, LANES), F32)] + acc_shape,
            in_specs=[hbm] * 6,
            out_specs=[vmem] * (6 + N_ACC),
            scratch_shapes=[pltpu.VMEM((KV, P_TWO), BF16), pltpu.VMEM((2, 8, n), F32), pltpu.VMEM((16, LANES), jnp.int32), pltpu.VMEM((16, LANES), jnp.int32),
                            pltpu.VMEM((1, 16, LANES), jnp.int32),
                            pltpu.VMEM((8, n), F32), pltpu.SemaphoreType.DMA((6,)), pltpu.SemaphoreType.DMA((4,)),
                            pltpu.SemaphoreType.DMA((4,))],
            compiler_params=pltpu.CompilerParams(collective_id=0, has_side_effects=True, vmem_limit_bytes=8 * MIB),
            name='exchange',
        )(*[pltpu.with_memory_space_constraint(x, pltpu.HBM) for x in inputs])
        y8, wy, wx, place, e2f, q_own = samples[:6]
        accs = pl.pallas_call(
            spread_kernel,
            out_shape=acc_shape,
            in_specs=[vmem] * (5 + N_ACC),
            out_specs=[vmem] * (N_ACC),
            scratch_shapes=[pltpu.SMEM((2, 16, LANES), jnp.int32), pltpu.VMEM((2, 16, LANES), jnp.int32), pltpu.VMEM((2, 16, LANES), jnp.int32),
                            pltpu.SemaphoreType.DMA] + [pltpu.VMEM((WIDE, LANES), F32)] * 2,
            input_output_aliases={5 + i: i for i in range(N_ACC)},
            compiler_params=pltpu.CompilerParams(vmem_limit_bytes=8 * MIB),
            cost_estimate=pl.CostEstimate(flops=2 * 10**9, bytes_accessed=2 * 10**7, transcendentals=0),
            name='spread',
        )(place, y8, wy, wx, q_own, *samples[6:])
        return pl.pallas_call(
            transform_kernel,
            out_shape=sds((2, P_BLK, Q_BLK), F32),
            in_specs=[vmem] * (N_ACC + 4),
            out_specs=vmem,
            scratch_shapes=[pltpu.VMEM((2, 4, Q_PAD, P_ALL), F32), pltpu.VMEM((Q_BLK, P_BLK), F32), pltpu.VMEM((KV, WIDE), BF16)] + [pltpu.VMEM((KV, LANES), F32)] * 3 + [
                pltpu.VMEM((Q_PAD, LANES), F32),
                pltpu.VMEM((GN_ROWS, LANES), F32),
                pltpu.VMEM((LAST, 4, Q_PAD, WIDE), BF16),
                pltpu.VMEM((LAST, 4, Q_PAD, WIDE), BF16),
                pltpu.VMEM((4, 144, LANES), BF16),
                pltpu.VMEM((4, 144, LANES), BF16),
                pltpu.VMEM((Q_PAD, LANES), F32),
                pltpu.VMEM((GN_ROWS, LANES), F32),
                pltpu.VMEM((4 * Q_PAD, P_TWO), F32),
                pltpu.VMEM((Q_PAD, P_ALL), F32),
                pltpu.VMEM((Q_PAD, P_ALL), F32),
                pltpu.VMEM((Q_PAD, P_ALL), F32),
                pltpu.SemaphoreType.DMA((N_CHUNK, len(SUBS), 3)),
                pltpu.SemaphoreType.DMA((N_CHUNK, len(SUBS), 4)),
                pltpu.SemaphoreType.DMA((2,)),
                pltpu.SemaphoreType.DMA((2,)),
                pltpu.SemaphoreType.DMA((len(SUBS),)),
                pltpu.SemaphoreType.DMA((len(SUBS),)),
            ],
            compiler_params=pltpu.CompilerParams(collective_id=1, has_side_effects=True, vmem_limit_bytes=24 * MIB),
            name='transform',
        )(*accs, e1, e2f, maps, deapod)

    return jax.shard_map(
        local_fn,
        mesh=mesh,
        in_specs=(P(None, None, sample_spec), P(None, sample_spec), P(None, sample_spec), P(sample_spec), P(sample_spec), P(None, ('exam', 'cols'), None, 'rows'), P()),
        out_specs=P(None, ('exam', 'cols'), 'rows'),
        check_vma=False,
    )
```
